32 devices in a mesh: batch: 1 (over z), col: 4 (over y), row: 8 (over x, core).
Axes of the slice: x: 4, y: 4, z: 1, core: 2. Of those that a mesh axis runs over, the one named last changes fastest.
The devices are a block of a 4x4x8 slice.
Arguments:
- pair_rep: bfloat16 [768, 768, 128], P(('batch', 'row'), 'col')
- pair_mask: int32 [768, 768], P(('batch', 'row'), 'col')
- ln_in_scale: bfloat16 [128], replicated
- w_left: bfloat16 [128, 128], replicated
- w_left_gate: bfloat16 [128, 128], replicated
- w_right: bfloat16 [128, 128], replicated
- w_right_gate: bfloat16 [128, 128], replicated
- w_out_gate: bfloat16 [128, 128], replicated
- ln_out_scale: bfloat16 [128], replicated
- w_out: bfloat16 [128, 128], replicated
Outputs:
- output: bfloat16 [768, 768, 128], P(('batch', 'row'), 'col')
All inputs are finite; a program needn't handle non-finite values.
Results may differ from the reference program's by a relative error of at most 0.00117811.
Values are sent between devices in bfloat16 or wider.
A program may use at most 768 MiB of HBM per device.

```python
import math
import jax
import jax.numpy as jnp
from jax import lax

RESIDUES = 768
PAIR_DIM = 128
TRI_DIM = 128
ROW_BLK = math.gcd(RESIDUES, 64)
NUM_BLK = RESIDUES // ROW_BLK
LN_EPS = 0.00001


def layer_norm(values, gain_vec):
    mean_val = jnp.mean(values, axis=-1, keepdims=True)
    centered = values - mean_val
    variance = jnp.mean(centered * centered, axis=-1, keepdims=True)
    return centered * lax.rsqrt(variance + LN_EPS) * gain_vec.astype(jnp.float32)


def setup_inputs(seed: int = 0, part: int = 0) -> dict:
    part_keys = jax.random.split(jax.random.fold_in(jax.random.key(seed), part), 3)
    weight_keys = jax.random.split(jax.random.key(seed + 1), 8)
    pair_rep = jax.random.normal(part_keys[0], (RESIDUES, RESIDUES, PAIR_DIM), jnp.float32).astype(jnp.bfloat16)
    residue_ok = jax.random.randint(part_keys[1], (RESIDUES,), 0, 16) != 0
    pair_ok = jax.random.randint(part_keys[2], (RESIDUES, RESIDUES), 0, 8) != 0
    pair_mask = (residue_ok[:, None] & residue_ok[None, :] & pair_ok).astype(jnp.int32)

    def matrix(key_val, fan_in, fan_out):
        return (jax.random.normal(key_val, (fan_in, fan_out), jnp.float32) * fan_in ** -0.5).astype(jnp.bfloat16)

    def gain_vector(key_val, num_chan):
        return (1.0 + 0.5 * jax.random.normal(key_val, (num_chan,), jnp.float32)).astype(jnp.bfloat16)

    return {
        'pair_rep': pair_rep,
        'pair_mask': pair_mask,
        'ln_in_scale': gain_vector(weight_keys[0], PAIR_DIM),
        'w_left': matrix(weight_keys[1], PAIR_DIM, TRI_DIM),
        'w_left_gate': matrix(weight_keys[2], PAIR_DIM, TRI_DIM),
        'w_right': matrix(weight_keys[3], PAIR_DIM, TRI_DIM),
        'w_right_gate': matrix(weight_keys[4], PAIR_DIM, TRI_DIM),
        'w_out_gate': matrix(weight_keys[5], PAIR_DIM, PAIR_DIM),
        'ln_out_scale': gain_vector(weight_keys[6], TRI_DIM),
        'w_out': matrix(weight_keys[7], TRI_DIM, PAIR_DIM),
    }


def reference(pair_rep, pair_mask, ln_in_scale, w_left, w_left_gate, w_right, w_right_gate, w_out_gate, ln_out_scale, w_out):
    pair_blocks = pair_rep.reshape(NUM_BLK, ROW_BLK, RESIDUES, PAIR_DIM)
    mask_blocks = pair_mask.reshape(NUM_BLK, ROW_BLK * RESIDUES, 1).astype(jnp.float32)

    def project(block_args):
        pair_rows, keep_rows = block_args
        normed = layer_norm(pair_rows.astype(jnp.float32), ln_in_scale).astype(jnp.bfloat16).reshape(ROW_BLK * RESIDUES, PAIR_DIM)
        left_act = keep_rows * jax.nn.sigmoid(jnp.dot(normed, w_left_gate, preferred_element_type=jnp.float32)) * jnp.dot(normed, w_left, preferred_element_type=jnp.float32)
        right_act = keep_rows * jax.nn.sigmoid(jnp.dot(normed, w_right_gate, preferred_element_type=jnp.float32)) * jnp.dot(normed, w_right, preferred_element_type=jnp.float32)
        return left_act.astype(jnp.bfloat16), right_act.astype(jnp.bfloat16)

    left_all, right_all = lax.map(project, (pair_blocks, mask_blocks))
    right_t = right_all.reshape(RESIDUES, RESIDUES, TRI_DIM).astype(jnp.float32).transpose(2, 0, 1)
    left_blocks = left_all.reshape(RESIDUES, NUM_BLK, ROW_BLK, TRI_DIM).transpose(1, 3, 0, 2)

    def finish(block_args):
        left_cols, pair_rows = block_args
        summed = jnp.einsum('hki,hkj->ijh', left_cols.astype(jnp.float32), right_t)
        normed_out = layer_norm(summed, ln_out_scale).astype(jnp.bfloat16).reshape(ROW_BLK * RESIDUES, TRI_DIM)
        update = jnp.dot(normed_out, w_out, preferred_element_type=jnp.float32)
        pair_flat = pair_rows.astype(jnp.float32).reshape(ROW_BLK * RESIDUES, PAIR_DIM)
        normed_in = layer_norm(pair_flat, ln_in_scale).astype(jnp.bfloat16)
        gate_act = jax.nn.sigmoid(jnp.dot(normed_in, w_out_gate, preferred_element_type=jnp.float32))
        return (pair_flat + gate_act * update).astype(jnp.bfloat16).reshape(ROW_BLK, RESIDUES, PAIR_DIM)

    return lax.map(finish, (left_blocks, pair_blocks)).reshape(RESIDUES, RESIDUES, PAIR_DIM)
```

```python
import functools

import jax
import jax.numpy as jnp
from jax import lax
from jax.experimental import pallas as pl
from jax.experimental.pallas import tpu as pltpu
from jax.sharding import PartitionSpec as P

LN_EPS = 0.00001
LANES = 128
HALF = 64
GROUP = 16
PITCH = 24
F32 = jnp.float32
BF16 = jnp.bfloat16


def dot(lhs, rhs, dims):
    return lax.dot_general(lhs, rhs, (dims, ((), ())), preferred_element_type=F32)


def layer_norm(values, gain):
    mean = jnp.mean(values, axis=-1, keepdims=True)
    centered = values - mean
    variance = jnp.mean(centered * centered, axis=-1, keepdims=True)
    return centered * lax.rsqrt(variance + LN_EPS) * gain


def project_kernel(z_ref, m_ref, g_ref, w_ref, x_ref, a_ref, b_ref, scr):
    heads = a_ref.shape[0]
    gain = g_ref[...].astype(F32)
    flat = scr.reshape(6 * heads * PITCH, LANES)

    def row(t, carry):
        lo = layer_norm(z_ref[0, t].astype(F32), gain).astype(BF16)
        hi = layer_norm(z_ref[1, t].astype(F32), gain).astype(BF16)
        x_ref[0, t] = lo
        x_ref[1, t] = hi
        parts = (lo[:LANES], hi[:LANES], jnp.concatenate([lo[LANES:], hi[LANES:]], axis=0))
        mask = m_ref[0, t].astype(F32)
        for seg in range(3):
            keep = mask[seg:seg + 1]
            for side in range(2):
                both = dot(w_ref[2 * side * heads:2 * (side + 1) * heads], parts[seg], ((1,), (1,)))
                act = keep * jax.nn.sigmoid(both[heads:]) * both[:heads]
                flat[pl.ds((2 * seg + side) * heads * PITCH + t, heads, stride=PITCH), :] = act
        return carry

    lax.fori_loop(0, GROUP, row, 0)

    def pack(h, carry):
        for seg in range(3):
            a_ref[h, seg] = scr[2 * seg * heads + h, 0:GROUP].astype(BF16)
            b_ref[h, seg] = scr[(2 * seg + 1) * heads + h, 0:GROUP].astype(BF16)
        return carry

    lax.fori_loop(0, heads, pack, 0)


def project(pair, mask, gain, weights):
    rows, cols, chan = pair.shape
    half = rows // 2
    heads = weights.shape[0] // 4
    steps = half // GROUP
    m = mask.reshape(2, half, cols)
    tail = jnp.concatenate([m[0, :, LANES:], m[1, :, LANES:]], axis=-1)
    m = jnp.stack([m[0, :, :LANES], m[1, :, :LANES], tail], axis=1)
    m = jnp.pad(m, ((0, 0), (0, 5), (0, 0))).reshape(steps, GROUP, 8, LANES)
    wire = jax.ShapeDtypeStruct((heads, 3, half, LANES), BF16)
    wire_spec = pl.BlockSpec((heads, 3, GROUP, LANES), lambda t: (0, 0, t, 0))
    tile_spec = pl.BlockSpec((2, GROUP, cols, chan), lambda t: (0, t, 0, 0))
    return pl.pallas_call(
        project_kernel,
        grid=(steps,),
        in_specs=[
            tile_spec,
            pl.BlockSpec((1, GROUP, 8, LANES), lambda t: (t, 0, 0, 0)),
            pl.BlockSpec((1, chan), lambda t: (0, 0)),
            pl.BlockSpec(weights.shape, lambda t: (0, 0)),
        ],
        out_specs=[tile_spec, wire_spec, wire_spec],
        out_shape=[jax.ShapeDtypeStruct((2, half, cols, chan), BF16), wire, wire],
        scratch_shapes=[pltpu.VMEM((6 * heads, PITCH, LANES), F32)],
        compiler_params=pltpu.CompilerParams(vmem_limit_bytes=60 * 2**20),
        cost_estimate=pl.CostEstimate(flops=2 * rows * cols * chan * 4 * heads, bytes_accessed=rows * cols * chan * 8, transcendentals=0),
    )(pair.reshape(2, half, cols, chan), m, gain.reshape(1, chan), weights)


def finish_kernel(y_ref, x_ref, z_ref, wg_ref, wo_ref, out_ref):
    srcs, _, _, per, _ = y_ref.shape
    heads = srcs * per

    def update(pos):
        return dot(y_ref[:, 0, pos].reshape(heads, LANES), wo_ref[...], ((0,), (0,)))

    def gated(x, z, upd):
        gate = jax.nn.sigmoid(dot(x, wg_ref[...], ((1,), (0,))))
        return (z.astype(F32) + gate * upd).astype(BF16)

    def wide(t, carry):
        out_ref[t, :LANES] = gated(x_ref[t, :LANES], z_ref[t, :LANES], update(t))
        return carry

    def narrow(t, carry):
        x = jnp.concatenate([x_ref[t, LANES:], x_ref[t + 16, LANES:]], axis=0)
        z = jnp.concatenate([z_ref[t, LANES:], z_ref[t + 16, LANES:]], axis=0)
        res = gated(x, z, update(t + 32))
        out_ref[t, LANES:] = res[:HALF]
        out_ref[t + 16, LANES:] = res[HALF:]
        return carry

    lax.fori_loop(0, 32, wide, 0, unroll=2)
    lax.fori_loop(0, 16, narrow, 0, unroll=2)


def finish(y, x, z, w_gate, w_out):
    rows, cols, chan = z.shape
    srcs, groups, places, per, _ = y.shape
    tile_spec = pl.BlockSpec((32, cols, chan), lambda t: (t, 0, 0))
    return pl.pallas_call(
        finish_kernel,
        grid=(groups,),
        in_specs=[
            pl.BlockSpec((srcs, 1, places, per, LANES), lambda t: (0, t, 0, 0, 0)),
            tile_spec,
            tile_spec,
            pl.BlockSpec(w_gate.shape, lambda t: (0, 0)),
            pl.BlockSpec(w_out.shape, lambda t: (0, 0)),
        ],
        out_specs=tile_spec,
        out_shape=jax.ShapeDtypeStruct(z.shape, BF16),
        compiler_params=pltpu.CompilerParams(vmem_limit_bytes=60 * 2**20),
        cost_estimate=pl.CostEstimate(flops=4 * rows * cols * chan * chan, bytes_accessed=rows * cols * chan * 8, transcendentals=0),
    )(y, x.reshape(z.shape), z, w_gate, w_out)


def exchange(a, b, gain, row_count, col_count):
    heads, _, half, _ = a.shape
    per = heads // row_count
    wire = (row_count, per, 3, half, LANES)
    got_a = lax.all_to_all(a.reshape(wire), 'row', 0, 0, tiled=True)
    all_a = lax.all_gather(got_a, 'col', axis=0)
    got_b = lax.all_to_all(b.reshape(wire), 'row', 0, 0, tiled=True)

    def unpack(w):
        w = jnp.moveaxis(w, -3, 0)
        tail = jnp.stack([w[2, ..., :HALF], w[2, ..., HALF:]])
        return jnp.concatenate([w[:2], tail], axis=-1)

    left, right = unpack(all_a), unpack(got_b)
    o = jnp.einsum('pyshki,pshkj->yhij', left, right, preferred_element_type=F32)
    cols = o.shape[-1]
    o = jnp.moveaxis(o, 1, 0).reshape(per, col_count * cols, cols)
    mean_p = jnp.mean(o, axis=0)
    m2_p = jnp.sum((o - mean_p) ** 2, axis=0)
    mean = lax.pmean(mean_p, 'row')
    m2 = lax.psum(m2_p + per * (mean_p - mean) ** 2, 'row')
    g = lax.dynamic_slice_in_dim(gain, lax.axis_index('row') * per, per).astype(F32)
    y = ((o - mean) * lax.rsqrt(m2 / heads + LN_EPS) * g[:, None, None]).astype(BF16)
    y = jnp.transpose(y.reshape(per, row_count, 2 * half // 32, 32, cols), (1, 2, 3, 0, 4))
    wide = y[..., :LANES]
    narrow = jnp.concatenate([y[:, :, :16, :, LANES:], y[:, :, 16:, :, LANES:]], axis=-1)
    packed = jnp.concatenate([wide, narrow], axis=2)
    return lax.all_to_all(packed, 'row', 0, 0, tiled=True)


def solution(mesh):
    row_count = mesh.shape['row']
    col_count = mesh.shape['col']
    tile_spec = P(('batch', 'row'), 'col', None)
    mask_spec = P(('batch', 'row'), 'col')

    def local_step(z, mask, g_in, w_a, w_ag, w_b, w_bg, w_g, g_out, w_o):
        weights = jnp.concatenate([w_a, w_ag, w_b, w_bg], axis=1).T
        x, a, b = project(z, mask, g_in, weights)
        y = exchange(a, b, g_out, row_count, col_count)
        return finish(y, x, z, w_g, w_o)

    return jax.shard_map(local_step, mesh=mesh, in_specs=(tile_spec, mask_spec) + (P(),) * 8, out_specs=tile_spec, check_vma=False)
```

```python
import functools

import jax
import jax.numpy as jnp
from jax import lax
from jax.experimental import pallas as pl
from jax.experimental.pallas import tpu as pltpu
from jax.sharding import PartitionSpec as P

LN_EPS = 0.00001
LANES = 128
HALF = 64
GROUP = 16
PITCH = 24
F32 = jnp.float32
BF16 = jnp.bfloat16


def dot(lhs, rhs, dims):
    return lax.dot_general(lhs, rhs, (dims, ((), ())), preferred_element_type=F32)


def layer_norm(values, gain):
    mean = jnp.mean(values, axis=-1, keepdims=True)
    centered = values - mean
    variance = jnp.mean(centered * centered, axis=-1, keepdims=True)
    return centered * lax.rsqrt(variance + LN_EPS) * gain


def project_kernel(z_ref, m_ref, g_ref, w_ref, x_ref, a_ref, b_ref, scr):
    heads = a_ref.shape[0]
    gain = g_ref[...].astype(F32)
    flat = scr.reshape(6 * heads * PITCH, LANES)

    def row(t, carry):
        lo = layer_norm(z_ref[0, t].astype(F32), gain).astype(BF16)
        hi = layer_norm(z_ref[1, t].astype(F32), gain).astype(BF16)
        x_ref[0, t] = lo
        x_ref[1, t] = hi
        parts = (lo[:LANES], hi[:LANES], jnp.concatenate([lo[LANES:], hi[LANES:]], axis=0))
        mask = m_ref[0, t].astype(F32)
        for seg in range(3):
            keep = mask[seg:seg + 1]
            for side in range(2):
                both = dot(w_ref[2 * side * heads:2 * (side + 1) * heads], parts[seg], ((1,), (1,)))
                act = keep * jax.nn.sigmoid(both[heads:]) * both[:heads]
                flat[pl.ds((2 * seg + side) * heads * PITCH + t, heads, stride=PITCH), :] = act
        return carry

    lax.fori_loop(0, GROUP, row, 0)

    def pack(h, carry):
        for seg in range(3):
            a_ref[h, seg] = scr[2 * seg * heads + h, 0:GROUP].astype(BF16)
            b_ref[h, seg] = scr[(2 * seg + 1) * heads + h, 0:GROUP].astype(BF16)
        return carry

    lax.fori_loop(0, heads, pack, 0)


def project(pair, mask, gain, weights):
    rows, cols, chan = pair.shape
    half = rows // 2
    heads = weights.shape[0] // 4
    steps = half // GROUP
    m = mask.reshape(2, half, cols)
    tail = jnp.concatenate([m[0, :, LANES:], m[1, :, LANES:]], axis=-1)
    m = jnp.stack([m[0, :, :LANES], m[1, :, :LANES], tail], axis=1)
    m = jnp.pad(m, ((0, 0), (0, 5), (0, 0))).reshape(steps, GROUP, 8, LANES)
    wire = jax.ShapeDtypeStruct((heads, 3, half, LANES), BF16)
    wire_spec = pl.BlockSpec((heads, 3, GROUP, LANES), lambda t: (0, 0, t, 0))
    tile_spec = pl.BlockSpec((2, GROUP, cols, chan), lambda t: (0, t, 0, 0))
    return pl.pallas_call(
        project_kernel,
        grid=(steps,),
        in_specs=[
            tile_spec,
            pl.BlockSpec((1, GROUP, 8, LANES), lambda t: (t, 0, 0, 0)),
            pl.BlockSpec((1, chan), lambda t: (0, 0)),
            pl.BlockSpec(weights.shape, lambda t: (0, 0)),
        ],
        out_specs=[tile_spec, wire_spec, wire_spec],
        out_shape=[jax.ShapeDtypeStruct((2, half, cols, chan), BF16), wire, wire],
        scratch_shapes=[pltpu.VMEM((6 * heads, PITCH, LANES), F32)],
        compiler_params=pltpu.CompilerParams(vmem_limit_bytes=60 * 2**20),
        cost_estimate=pl.CostEstimate(flops=2 * rows * cols * chan * 4 * heads, bytes_accessed=rows * cols * chan * 8, transcendentals=0),
    )(pair.reshape(2, half, cols, chan), m, gain.reshape(1, chan), weights)


def finish_kernel(y_ref, x_ref, z_ref, wg_ref, wo_ref, out_ref):
    srcs, _, _, per, _ = y_ref.shape
    heads = srcs * per

    def update(pos):
        return dot(y_ref[:, 0, pos].reshape(heads, LANES), wo_ref[...], ((0,), (0,)))

    def gated(x, z, upd):
        gate = jax.nn.sigmoid(dot(x, wg_ref[...], ((1,), (0,))))
        return (z.astype(F32) + gate * upd).astype(BF16)

    def wide(t, carry):
        out_ref[t, :LANES] = gated(x_ref[t, :LANES], z_ref[t, :LANES], update(t))
        return carry

    def narrow(t, carry):
        x = jnp.concatenate([x_ref[t, LANES:], x_ref[t + 16, LANES:]], axis=0)
        z = jnp.concatenate([z_ref[t, LANES:], z_ref[t + 16, LANES:]], axis=0)
        res = gated(x, z, update(t + 32))
        out_ref[t, LANES:] = res[:HALF]
        out_ref[t + 16, LANES:] = res[HALF:]
        return carry

    lax.fori_loop(0, 32, wide, 0, unroll=2)
    lax.fori_loop(0, 16, narrow, 0, unroll=2)


def finish(y, x, z, w_gate, w_out):
    rows, cols, chan = z.shape
    srcs, groups, places, per, _ = y.shape
    tile_spec = pl.BlockSpec((32, cols, chan), lambda t: (t, 0, 0))
    return pl.pallas_call(
        finish_kernel,
        grid=(groups,),
        in_specs=[
            pl.BlockSpec((srcs, 1, places, per, LANES), lambda t: (0, t, 0, 0, 0)),
            tile_spec,
            tile_spec,
            pl.BlockSpec(w_gate.shape, lambda t: (0, 0)),
            pl.BlockSpec(w_out.shape, lambda t: (0, 0)),
        ],
        out_specs=tile_spec,
        out_shape=jax.ShapeDtypeStruct(z.shape, BF16),
        compiler_params=pltpu.CompilerParams(vmem_limit_bytes=60 * 2**20),
        cost_estimate=pl.CostEstimate(flops=4 * rows * cols * chan * chan, bytes_accessed=rows * cols * chan * 8, transcendentals=0),
    )(y, x.reshape(z.shape), z, w_gate, w_out)


def remote(src, dst, send_sem, recv_sem, **place):
    return pltpu.make_async_remote_copy(
        src_ref=src, dst_ref=dst, send_sem=send_sem, recv_sem=recv_sem, device_id=place, device_id_type=pl.DeviceIdType.MESH
    )


def exchange_kernel(
    row_count, col_count, a_hbm, b_hbm, g_ref, y_hbm, all_a, got_b, rhs, o_wide, o_tail, st_part, st_got, st_tot, y_out,
    xa_s, xa_r, xb_s, xb_r, dir_s, dir_r, fwd_s, fwd_r, rs_s, rs_r, ag_s, ag_r, ys_s, ys_r, loc,
):
    me, col = lax.axis_index('row'), lax.axis_index('col')
    per, _, half, _ = a_hbm.shape[1:]
    heads = per * row_count
    depth = row_count * half
    cols = LANES + HALF
    chip, core = me // 2, me % 2
    chips = row_count // 2
    steps = [(0, 0), (0, 1)]
    for d in range(1, chips // 2 + 1):
        steps += [(d, 0), (-d, 0), (d, 1), (-d, 1)] if 2 * d < chips else [(d, 0), (d, 1)]
    peers = [lax.rem(chip + d + chips, chips) * 2 + lax.rem(core + f, 2) for d, f in steps]
    up, down = lax.rem(col + 1, col_count), lax.rem(col + col_count - 1, col_count)
    far = lax.rem(col + 2, col_count)

    barrier = pltpu.get_barrier_semaphore()
    for p in peers[1:]:
        pl.semaphore_signal(barrier, inc=1, device_id={'row': p}, device_id_type=pl.DeviceIdType.MESH)
    for p in (up, down):
        pl.semaphore_signal(barrier, inc=1, device_id={'col': p}, device_id_type=pl.DeviceIdType.MESH)
    pl.semaphore_wait(barrier, row_count + 1)

    own_a = pltpu.make_async_copy(a_hbm.at[me], all_a.at[col, me], loc.at[0])
    own_b = pltpu.make_async_copy(b_hbm.at[me], got_b.at[me], loc.at[1])
    sends = []

    def send(*args, **place):
        copy = remote(*args, **place)
        copy.start()
        sends.append(copy)

    def direct(q):
        src = all_a.at[col, peers[q]]
        send(src, src, dir_s.at[0, q], dir_r.at[0, peers[q]], col=up)
        send(src, src, dir_s.at[1, q], dir_r.at[1, peers[q]], col=down)

    own_a.start()
    for q in range(1, row_count):
        send(a_hbm.at[peers[q]], all_a.at[col, me], xa_s.at[q], xa_r.at[me], row=peers[q])
    own_b.start()
    for q in range(1, row_count):
        send(b_hbm.at[peers[q]], got_b.at[me], xb_s.at[q], xb_r.at[me], row=peers[q])

    own_a.wait()
    direct(0)
    for q in range(1, row_count):
        remote(a_hbm.at[me], all_a.at[col, peers[q]], xa_s.at[q], xa_r.at[peers[q]], row=peers[q]).wait_recv()
        direct(q)

    def forward(q, part):
        away, block = (up, down) if q % 2 == 0 else (down, up)
        src = all_a.at[block, peers[q], :, pl.ds(2 * part, 2 - part)]
        send(src, src, fwd_s.at[part, q], fwd_r.at[part, peers[q]], col=away)

    for q in range(row_count):
        for way, block in ((0, down), (1, up)):
            ref = all_a.at[block, peers[q]]
            remote(ref, ref, dir_s.at[way, q], dir_r.at[way, peers[q]], col=up).wait_recv()
        forward(q, 0)
    for q in range(row_count):
        forward(q, 1)

    own_b.wait()
    for q in range(1, row_count):
        remote(b_hbm.at[me], got_b.at[peers[q]], xb_s.at[q], xb_r.at[peers[q]], row=peers[q]).wait_recv()

    def spread(h, carry):
        tail = got_b[:, h, 2].reshape(depth, LANES)
        for s in range(2):
            rhs[h, s, :, :LANES] = got_b[:, h, s].reshape(depth, LANES)
        rhs[h, 0, :, LANES:] = tail
        rhs[h, 1, :, LANES:] = jnp.concatenate([tail[:, HALF:], tail[:, :HALF]], axis=1)
        return carry

    lax.fori_loop(0, per, spread, 0)

    lane = lax.broadcasted_iota(jnp.int32, (8, LANES), 1)
    pitch = o_wide.shape[2]
    flat_wide = o_wide.reshape(col_count * per * pitch, LANES)
    flat_tail = o_tail.reshape(col_count * per * pitch, LANES)

    def swap(v):
        return pltpu.roll(v, HALF, v.ndim - 1)

    def product(block, row0, rows):
        def channel(h, carry):
            if row0 == 0:
                res = dot(all_a[block, :, h, 0].reshape(depth, LANES), rhs[h, 0], ((0,), (0,)))
                res += dot(all_a[block, :, h, 1].reshape(depth, LANES), rhs[h, 1], ((0,), (0,)))
                o_wide[block, h, 0:LANES] = res[:, :LANES]
                o_tail[block, h, 0:LANES] = res[:, LANES:]
            if row0 + rows == cols:
                turned = all_a[block, :, h, 2].reshape(depth, LANES).T
                res = dot(turned[:HALF], rhs[h, 0], ((1,), (0,)))
                res += dot(turned[HALF:], rhs[h, 1], ((1,), (0,)))
                o_wide[block, h, LANES:cols] = res[:, :LANES]
                o_tail[block, h, LANES:cols] = res[:, LANES:]
            return carry

        lax.fori_loop(0, per, channel, 0)

    def partial(u, block, row0, rows):
        def tile(t, carry):
            at = pl.ds(pl.multiple_of(row0 + 8 * t, 8), 8)
            out = []
            for ref in (o_wide, o_tail):
                v = ref[block, :, at]
                mean = jnp.sum(v, axis=0) * (1.0 / per)
                out += [mean, jnp.sum((v - mean) ** 2, axis=0)]
            st_part[block, 0, at] = out[0]
            st_part[block, 1, at] = out[1]
            st_part[block, 2, at] = jnp.where(lane < HALF, out[2], swap(out[3]))
            return carry

        lax.fori_loop(0, rows // 8, tile, 0)
        own = rows // row_count
        for q in range(1, row_count):
            at = pl.ds(pl.multiple_of(row0 + own * peers[q], 8), own)
            send(st_part.at[block, :, at], st_got.at[u, me, :, 0:own], rs_s.at[u, q], rs_r.at[u, me], row=peers[q])

    def combine(u, block, row0, rows):
        own = rows // row_count
        first = pl.multiple_of(row0 + own * me, 8)
        st_got[u, me, :, 0:own] = st_part[block, :, pl.ds(first, own)]
        for q in range(1, row_count):
            ref = st_got.at[u, peers[q], :, 0:own]
            remote(ref, ref, rs_s.at[u, q], rs_r.at[u, peers[q]], row=peers[q]).wait_recv()
        for t in range(own // 8):
            at = slice(8 * t, 8 * t + 8)
            to = pl.ds(pl.multiple_of(first + 8 * t, 8), 8)
            means, squares, both = st_got[u, :, 0, at], st_got[u, :, 1, at], st_got[u, :, 2, at]
            mean = jnp.sum(means, axis=0) * (1.0 / row_count)
            square = jnp.sum(squares, axis=0) + per * jnp.sum((means - mean) ** 2, axis=0)
            st_tot[block, 0, to] = mean
            st_tot[block, 1, to] = lax.rsqrt(square * (1.0 / heads) + LN_EPS)
            total = jnp.sum(both, axis=0)
            mean = total * (1.0 / row_count)
            square = total + swap(per * jnp.sum((both - mean) ** 2, axis=0))
            st_tot[block, 2, to] = jnp.where(lane < HALF, mean, lax.rsqrt(square * (1.0 / heads) + LN_EPS))
        for q in range(1, row_count):
            ref = st_tot.at[block, :, pl.ds(first, own)]
            send(ref, ref, ag_s.at[u, q], ag_r.at[u, me], row=peers[q])

    gain = g_ref[pl.ds(pl.multiple_of(me * per, 8), per), :]
    wide_lane = lax.broadcasted_iota(jnp.int32, (per, LANES), 1)

    def normalize(u, block, row0, rows):
        own = rows // row_count
        for q in range(1, row_count):
            ref = st_tot.at[block, :, pl.ds(pl.multiple_of(row0 + own * peers[q], 8), own)]
            remote(ref, ref, ag_s.at[u, q], ag_r.at[u, peers[q]], row=peers[q]).wait_recv()
        base = block * (per * pitch)

        def wide(t, carry):
            for s in range(8):
                i = row0 + 8 * t + s
                v = flat_wide[pl.ds(base + i, per, stride=pitch), :]
                v = (v - st_tot[block, 0, pl.ds(i, 1)]) * st_tot[block, 1, pl.ds(i, 1)] * gain
                y_out[block, i // 32, i % 32] = v.astype(BF16)
            return carry

        def tail(t, carry):
            for s in range(8):
                i = row0 + 32 * (t // 2) + 8 * (t % 2) + s
                lo = flat_tail[pl.ds(base + i, per, stride=pitch), :]
                hi = flat_tail[pl.ds(base + i + 16, per, stride=pitch), :]
                first, second = st_tot[block, 2, pl.ds(i, 1)], st_tot[block, 2, pl.ds(i + 16, 1)]
                v = jnp.where(wide_lane < HALF, lo, swap(hi))
                mean = jnp.where(wide_lane[:1] < HALF, first, swap(second))
                rstd = jnp.where(wide_lane[:1] < HALF, swap(first), second)
                y_out[block, i // 32, 32 + i % 32] = ((v - mean) * rstd * gain).astype(BF16)
            return carry

        lax.fori_loop(0, rows // 8, wide, 0)
        lax.fori_loop(0, rows // 16, tail, 0)

    def back(block, slot, pieces):
        for c, p in pieces:
            dest = block * 2 + c
            src = y_out.at[block, pl.ds(3 * c + p, 1 + p)]
            dst = y_hbm.at[me, pl.ds(p, 1 + p)]

            @pl.when(dest != me)
            def _():
                remote(src, dst, ys_s.at[slot, c, p], ys_r.at[me, p], row=dest).start()

            @pl.when(dest == me)
            def _():
                pltpu.make_async_copy(src, dst, loc.at[2 + p]).start()

    def back_done(block, slot):
        for c in range(2):
            for p in range(2):
                dest = block * 2 + c
                src = y_out.at[block, pl.ds(3 * c + p, 1 + p)]
                dst = y_hbm.at[me, pl.ds(p, 1 + p)]

                @pl.when(dest != me)
                def _():
                    remote(src, dst, ys_s.at[slot, c, p], ys_r.at[me, p], row=dest).wait_send()

                @pl.when(dest == me)
                def _():
                    pltpu.make_async_copy(src, dst, loc.at[2 + p]).wait()

    def arrived(part):
        for q in range(row_count):
            block = far
            ref = all_a.at[block, peers[q], :, pl.ds(2 * part, 2 - part)]
            remote(ref, ref, fwd_s.at[part, q], fwd_r.at[part, peers[q]], col=up).wait_recv()

    wide_rows, all_rows = (0, LANES), (0, cols)
    every = ((0, 0), (0, 1), (1, 0), (1, 1))
    units = [(0, col) + all_rows, (1, down) + all_rows, (2, up) + all_rows, (3, far) + wide_rows, (4, far, LANES, HALF)]

    def start(u):
        product(*units[u][1:])
        partial(*units[u])

    start(0)
    start(1)
    combine(*units[0])
    start(2)
    combine(*units[1])
    normalize(*units[0])
    back(col, 0, every)
    combine(*units[2])
    normalize(*units[1])
    back(down, 1, every)
    normalize(*units[2])
    back(up, 2, every)
    arrived(0)
    start(3)
    combine(*units[3])
    arrived(1)
    start(4)
    normalize(*units[3])
    back(far, 3, ((0, 0), (0, 1), (1, 0)))
    combine(*units[4])
    normalize(*units[4])
    back(far, 3, ((1, 1),))

    for copy in sends:
        copy.wait_send()
    for slot, block in enumerate((col, down, up, far)):
        back_done(block, slot)
    for q in range(1, row_count):
        for p in range(2):
            ref = y_hbm.at[peers[q], pl.ds(p, 1 + p)]
            remote(y_out.at[0, pl.ds(p, 1 + p)], ref, ys_s.at[0, 0, p], ys_r.at[peers[q], p], row=peers[q]).wait_recv()


def exchange(a, b, gain, row_count, col_count):
    heads, _, half, _ = a.shape
    per = heads // row_count
    cols = 2 * half * row_count // col_count
    depth = row_count * half
    groups = 2 * half // 32
    wire = (row_count, per, 3, half, LANES)
    dma = pltpu.SemaphoreType.DMA
    pitch = cols + 8
    gains = jnp.broadcast_to(gain.astype(F32)[:, None], (heads, LANES))
    hbm = pl.BlockSpec(memory_space=pl.ANY)
    return pl.pallas_call(
        functools.partial(exchange_kernel, row_count, col_count),
        in_specs=[hbm, hbm, pl.BlockSpec(memory_space=pltpu.VMEM)],
        out_specs=hbm,
        out_shape=jax.ShapeDtypeStruct((row_count, groups, 48, per, LANES), BF16),
        scratch_shapes=[
            pltpu.VMEM((col_count,) + wire, BF16),
            pltpu.VMEM(wire, BF16),
            pltpu.VMEM((per, 2, depth, 2 * LANES), BF16),
            pltpu.VMEM((col_count, per, pitch, LANES), F32),
            pltpu.VMEM((col_count, per, pitch, LANES), F32),
            pltpu.VMEM((col_count, 3, cols, LANES), F32),
            pltpu.VMEM((5, row_count, 3, cols // row_count, LANES), F32),
            pltpu.VMEM((col_count, 3, cols, LANES), F32),
            pltpu.VMEM((col_count, 2 * groups, 48, per, LANES), BF16),
            dma((row_count,)), dma((row_count,)), dma((row_count,)), dma((row_count,)),
            dma((2, row_count)), dma((2, row_count)), dma((2, row_count)), dma((2, row_count)),
            dma((5, row_count)), dma((5, row_count)), dma((5, row_count)), dma((5, row_count)),
            dma((col_count, 2, 2)), dma((row_count, 2)), dma((4,)),
        ],
        compiler_params=pltpu.CompilerParams(collective_id=0, has_side_effects=True, vmem_limit_bytes=62 * 2**20),
        cost_estimate=pl.CostEstimate(flops=2 * per * depth * 2 * cols * col_count * cols, bytes_accessed=a.size * 8, transcendentals=0),
    )(a.reshape(wire), b.reshape(wire), gains)


def solution(mesh):
    row_count = mesh.shape['row']
    col_count = mesh.shape['col']
    tile_spec = P(('batch', 'row'), 'col', None)
    mask_spec = P(('batch', 'row'), 'col')

    def local_step(z, mask, g_in, w_a, w_ag, w_b, w_bg, w_g, g_out, w_o):
        weights = jnp.concatenate([w_a, w_ag, w_b, w_bg], axis=1).T
        x, a, b = project(z, mask, g_in, weights)
        y = exchange(a, b, g_out, row_count, col_count)
        return finish(y, x, z, w_g, w_o)

    return jax.shard_map(local_step, mesh=mesh, in_specs=(tile_spec, mask_spec) + (P(),) * 8, out_specs=tile_spec, check_vma=False)
```

```python
import functools

import jax
import jax.numpy as jnp
from jax import lax
from jax.experimental import pallas as pl
from jax.experimental.pallas import tpu as pltpu
from jax.sharding import PartitionSpec as P

LN_EPS = 0.00001
LANES = 128
HALF = 64
GROUP = 16
PITCH = 24
F32 = jnp.float32
BF16 = jnp.bfloat16


def dot(lhs, rhs, dims):
    return lax.dot_general(lhs, rhs, (dims, ((), ())), preferred_element_type=F32)


def layer_norm(values, gain):
    mean = jnp.mean(values, axis=-1, keepdims=True)
    centered = values - mean
    variance = jnp.mean(centered * centered, axis=-1, keepdims=True)
    return centered * lax.rsqrt(variance + LN_EPS) * gain


def project_kernel(z_ref, m_ref, g_ref, w_ref, x_ref, a_ref, b_ref, scr):
    heads = a_ref.shape[0]
    gain = g_ref[...].astype(F32)
    flat = scr.reshape(6 * heads * PITCH, LANES)

    def row(t, carry):
        lo = layer_norm(z_ref[0, t].astype(F32), gain).astype(BF16)
        hi = layer_norm(z_ref[1, t].astype(F32), gain).astype(BF16)
        x_ref[0, t] = lo
        x_ref[1, t] = hi
        parts = [v[HALF * s:HALF * (s + 1)] for s in range(3) for v in (lo, hi)]
        tall = jnp.concatenate(parts, axis=0)
        keep = m_ref[0, t].astype(F32)
        for side in range(2):
            both = dot(w_ref[2 * side * heads:2 * (side + 1) * heads], tall, ((1,), (1,)))
            for seg in range(3):
                at = slice(seg * LANES, (seg + 1) * LANES)
                act = keep[seg:seg + 1] * jax.nn.sigmoid(both[heads:, at]) * both[:heads, at]
                flat[pl.ds((2 * seg + side) * heads * PITCH + t, heads, stride=PITCH), :] = act
        return carry

    lax.fori_loop(0, GROUP, row, 0)

    def pack(h, carry):
        for seg in range(3):
            a_ref[h, seg] = scr[2 * seg * heads + h, 0:GROUP].astype(BF16)
            b_ref[h, seg] = scr[(2 * seg + 1) * heads + h, 0:GROUP].astype(BF16)
        return carry

    lax.fori_loop(0, heads, pack, 0)


def project(pair, mask, gain, weights):
    rows, cols, chan = pair.shape
    half = rows // 2
    heads = weights.shape[0] // 4
    steps = half // GROUP
    m = mask.reshape(2, half, 3, HALF).transpose(1, 2, 0, 3).reshape(half, 3, LANES)
    m = jnp.pad(m, ((0, 0), (0, 5), (0, 0))).reshape(steps, GROUP, 8, LANES)
    wire = jax.ShapeDtypeStruct((heads, 3, half, LANES), BF16)
    wire_spec = pl.BlockSpec((heads, 3, GROUP, LANES), lambda t: (0, 0, t, 0))
    tile_spec = pl.BlockSpec((2, GROUP, cols, chan), lambda t: (0, t, 0, 0))
    return pl.pallas_call(
        project_kernel,
        grid=(steps,),
        in_specs=[
            tile_spec,
            pl.BlockSpec((1, GROUP, 8, LANES), lambda t: (t, 0, 0, 0)),
            pl.BlockSpec((1, chan), lambda t: (0, 0)),
            pl.BlockSpec(weights.shape, lambda t: (0, 0)),
        ],
        out_specs=[tile_spec, wire_spec, wire_spec],
        out_shape=[jax.ShapeDtypeStruct((2, half, cols, chan), BF16), wire, wire],
        scratch_shapes=[pltpu.VMEM((6 * heads, PITCH, LANES), F32)],
        compiler_params=pltpu.CompilerParams(vmem_limit_bytes=60 * 2**20),
        cost_estimate=pl.CostEstimate(flops=2 * rows * cols * chan * 4 * heads, bytes_accessed=rows * cols * chan * 8, transcendentals=0),
    )(pair.reshape(2, half, cols, chan), m, gain.reshape(1, chan), weights)


def finish_kernel(y_ref, x_ref, z_ref, wg_ref, wo_ref, out_ref):
    srcs, _, _, per, _ = y_ref.shape
    heads = srcs * per

    def update(pos):
        return dot(y_ref[:, 0, pos].reshape(heads, LANES), wo_ref[...], ((0,), (0,)))

    def gated(x, z, upd):
        gate = jax.nn.sigmoid(dot(x, wg_ref[...], ((1,), (0,))))
        return (z.astype(F32) + gate * upd).astype(BF16)

    def wide(t, carry):
        out_ref[t, :LANES] = gated(x_ref[t, :LANES], z_ref[t, :LANES], update(t))
        return carry

    def narrow(t, carry):
        x = jnp.concatenate([x_ref[t, LANES:], x_ref[t + 16, LANES:]], axis=0)
        z = jnp.concatenate([z_ref[t, LANES:], z_ref[t + 16, LANES:]], axis=0)
        res = gated(x, z, update(t + 32))
        out_ref[t, LANES:] = res[:HALF]
        out_ref[t + 16, LANES:] = res[HALF:]
        return carry

    lax.fori_loop(0, 32, wide, 0, unroll=2)
    lax.fori_loop(0, 16, narrow, 0, unroll=2)


def finish(y, x, z, w_gate, w_out):
    rows, cols, chan = z.shape
    srcs, groups, places, per, _ = y.shape
    tile_spec = pl.BlockSpec((32, cols, chan), lambda t: (t, 0, 0))
    return pl.pallas_call(
        finish_kernel,
        grid=(groups,),
        in_specs=[
            pl.BlockSpec((srcs, 1, places, per, LANES), lambda t: (0, t, 0, 0, 0)),
            tile_spec,
            tile_spec,
            pl.BlockSpec(w_gate.shape, lambda t: (0, 0)),
            pl.BlockSpec(w_out.shape, lambda t: (0, 0)),
        ],
        out_specs=tile_spec,
        out_shape=jax.ShapeDtypeStruct(z.shape, BF16),
        compiler_params=pltpu.CompilerParams(vmem_limit_bytes=60 * 2**20),
        cost_estimate=pl.CostEstimate(flops=4 * rows * cols * chan * chan, bytes_accessed=rows * cols * chan * 8, transcendentals=0),
    )(y, x.reshape(z.shape), z, w_gate, w_out)


def remote(src, dst, send_sem, recv_sem, **place):
    return pltpu.make_async_remote_copy(
        src_ref=src, dst_ref=dst, send_sem=send_sem, recv_sem=recv_sem, device_id=place, device_id_type=pl.DeviceIdType.MESH
    )


MESSAGES = (((0, 0, 2, 0, 0),), ((0, 2, 1, 2, 1), (1, 3, 1, 0, 0)), ((1, 4, 2, 1, 1),))
ARRIVALS = (((0, 2), (2, 1)), ((0, 1), (1, 2)))


def exchange_kernel(
    row_count, col_count, a_hbm, b_hbm, g_ref, y_hbm, all_a, got_b, rhs, o_wide, o_tail, st_part, st_got, st_tot, y_out,
    xa_s, xa_r, xb_s, xb_r, dir_s, dir_r, fwd_s, fwd_r, rs_s, rs_r, ag_s, ag_r, ys_s, ys_r, loc,
):
    me, col = lax.axis_index('row'), lax.axis_index('col')
    per, _, half, _ = a_hbm.shape[1:]
    heads = per * row_count
    depth = row_count * half
    chip, core = me // 2, me % 2
    chips = row_count // 2
    steps = [(0, 0), (0, 1)]
    for d in range(1, chips // 2 + 1):
        steps += [(d, 0), (-d, 0), (d, 1), (-d, 1)] if 2 * d < chips else [(d, 0), (d, 1)]
    peers = [lax.rem(chip + d + chips, chips) * 2 + lax.rem(core + f, 2) for d, f in steps]
    blocks = [lax.rem(chip + d, chips) for d in (1, 3, 2, 0)]
    up, down = lax.rem(col + 1, col_count), lax.rem(col + col_count - 1, col_count)
    far = lax.rem(col + 2, col_count)

    barrier = pltpu.get_barrier_semaphore()
    for p in peers[1:]:
        pl.semaphore_signal(barrier, inc=1, device_id={'row': p}, device_id_type=pl.DeviceIdType.MESH)
    for p in (up, down):
        pl.semaphore_signal(barrier, inc=1, device_id={'col': p}, device_id_type=pl.DeviceIdType.MESH)
    pl.semaphore_wait(barrier, row_count + 1)

    sends = []

    def send(*args, **place):
        copy = remote(*args, **place)
        copy.start()
        sends.append(copy)

    own_a = [pltpu.make_async_copy(a_hbm.at[me, :, s], all_a.at[s, col, me], loc.at[s]) for s in range(3)]
    own_b = pltpu.make_async_copy(b_hbm.at[me], got_b.at[me], loc.at[3])

    def scatter_a(s):
        own_a[s].start()
        for q in range(1, row_count):
            send(a_hbm.at[peers[q], :, s], all_a.at[s, col, me], xa_s.at[s, q], xa_r.at[s, me], row=peers[q])

    def scatter_b():
        own_b.start()
        for q in range(1, row_count):
            send(b_hbm.at[peers[q]], got_b.at[me], xb_s.at[q], xb_r.at[me], row=peers[q])

    def direct(s):
        own_a[s].wait()
        for q in range(row_count):
            src = all_a.at[s, col, peers[q]]
            if q:
                remote(src, src, xa_s.at[s, q], xa_r.at[s, peers[q]], row=peers[q]).wait_recv()
            send(src, src, dir_s.at[s, 0, q], dir_r.at[s, 0, peers[q]], col=up)
            send(src, src, dir_s.at[s, 1, q], dir_r.at[s, 1, peers[q]], col=down)

    def forward(s, first, last):
        for q in range(first, last):
            for way, block in ((0, down), (1, up)):
                ref = all_a.at[s, block, peers[q]]
                remote(ref, ref, dir_s.at[s, way, q], dir_r.at[s, way, peers[q]], col=up).wait_recv()
            away, block = (up, down) if q % 2 == 0 else (down, up)
            src = all_a.at[s, block, peers[q]]
            send(src, src, fwd_s.at[s, q], fwd_r.at[s, peers[q]], col=away)

    def arrived(s):
        for q in range(row_count):
            ref = all_a.at[s, far, peers[q]]
            remote(ref, ref, fwd_s.at[s, q], fwd_r.at[s, peers[q]], col=up).wait_recv()

    lane = lax.broadcasted_iota(jnp.int32, (8, LANES), 1)
    pitch = o_wide.shape[2]
    rows = col_count * HALF
    own = rows // row_count
    flat_wide = o_wide.reshape(3 * per * pitch, LANES)
    flat_tail = o_tail.reshape(3 * per * pitch, LANES)

    def swap(v):
        return pltpu.roll(v, HALF, v.ndim - 1)

    def spread():
        own_b.wait()
        for q in range(1, row_count):
            ref = got_b.at[peers[q]]
            remote(ref, ref, xb_s.at[q], xb_r.at[peers[q]], row=peers[q]).wait_recv()

        def channel(h, carry):
            w = [got_b[:, h, s].reshape(depth, LANES) for s in range(3)]
            rhs[h, 0, :, :LANES] = jnp.concatenate([w[0][:, :HALF], w[1][:, :HALF]], axis=1)
            rhs[h, 1, :, :LANES] = jnp.concatenate([w[0][:, HALF:], w[1][:, HALF:]], axis=1)
            rhs[h, 0, :, LANES:] = w[2]
            rhs[h, 1, :, LANES:] = jnp.concatenate([w[2][:, HALF:], w[2][:, :HALF]], axis=1)
            return carry

        lax.fori_loop(0, per, channel, 0)

    def product(u):
        def channel(h, carry):
            turned = [all_a[u, c, :, h].reshape(depth, LANES).T for c in range(col_count)]
            res = dot(jnp.concatenate([t[:HALF] for t in turned], axis=0), rhs[h, 0], ((1,), (0,)))
            res += dot(jnp.concatenate([t[HALF:] for t in turned], axis=0), rhs[h, 1], ((1,), (0,)))
            o_wide[u, h, 0:rows] = res[:, :LANES]
            o_tail[u, h, 0:rows] = res[:, LANES:]
            return carry

        lax.fori_loop(0, per, channel, 0)

    def partial(u):
        def tile(t, carry):
            at = pl.ds(pl.multiple_of(8 * t, 8), 8)
            out = []
            for ref in (o_wide, o_tail):
                v = ref[u, :, at]
                mean = jnp.sum(v, axis=0) * (1.0 / per)
                out += [mean, jnp.sum((v - mean) ** 2, axis=0)]
            st_part[u, 0, at] = out[0]
            st_part[u, 1, at] = out[1]
            st_part[u, 2, at] = jnp.where(lane < HALF, out[2], swap(out[3]))
            return carry

        lax.fori_loop(0, rows // 8, tile, 0, unroll=2)
        for q in range(1, row_count):
            at = pl.ds(pl.multiple_of(own * peers[q], 8), own)
            send(st_part.at[u, :, at], st_got.at[u, me], rs_s.at[u, q], rs_r.at[u, me], row=peers[q])

    def combine(u):
        first = pl.multiple_of(own * me, 8)
        st_got[u, me] = st_part[u, :, pl.ds(first, own)]
        for q in range(1, row_count):
            ref = st_got.at[u, peers[q]]
            remote(ref, ref, rs_s.at[u, q], rs_r.at[u, peers[q]], row=peers[q]).wait_recv()
        for t in range(own // 8):
            at = slice(8 * t, 8 * t + 8)
            to = pl.ds(pl.multiple_of(first + 8 * t, 8), 8)
            means, squares, both = st_got[u, :, 0, at], st_got[u, :, 1, at], st_got[u, :, 2, at]
            mean = jnp.sum(means, axis=0) * (1.0 / row_count)
            square = jnp.sum(squares, axis=0) + per * jnp.sum((means - mean) ** 2, axis=0)
            st_tot[u, 0, to] = mean
            st_tot[u, 1, to] = lax.rsqrt(square * (1.0 / heads) + LN_EPS)
            total = jnp.sum(both, axis=0)
            mean = total * (1.0 / row_count)
            square = total + swap(per * jnp.sum((both - mean) ** 2, axis=0))
            st_tot[u, 2, to] = jnp.where(lane < HALF, mean, lax.rsqrt(square * (1.0 / heads) + LN_EPS))
        for q in range(1, row_count):
            ref = st_tot.at[u, :, pl.ds(first, own)]
            send(ref, ref, ag_s.at[u, q], ag_r.at[u, me], row=peers[q])

    gain = g_ref[pl.ds(pl.multiple_of(me * per, 8), per), :]
    low = lax.broadcasted_iota(jnp.int32, (per, LANES), 1) < HALF

    def normalize(u):
        for q in range(1, row_count):
            ref = st_tot.at[u, :, pl.ds(pl.multiple_of(own * peers[q], 8), own)]
            remote(ref, ref, ag_s.at[u, q], ag_r.at[u, peers[q]], row=peers[q]).wait_recv()
        base = u * (per * pitch)

        def wide(t, carry):
            for s in range(8):
                i = 8 * t + s
                v = flat_wide[pl.ds(base + i, per, stride=pitch), :]
                v = (v - st_tot[u, 0, pl.ds(i, 1)]) * st_tot[u, 1, pl.ds(i, 1)] * gain
                y_out[t // 8, 2 * u + (t // 4) % 2, 8 * (t % 4) + s] = v.astype(BF16)
            return carry

        def tail(t, carry):
            for s in range(8):
                i = 32 * (t // 2) + 8 * (t % 2) + s
                lo = flat_tail[pl.ds(base + i, per, stride=pitch), :]
                hi = flat_tail[pl.ds(base + i + 16, per, stride=pitch), :]
                first, second = st_tot[u, 2, pl.ds(i, 1)], st_tot[u, 2, pl.ds(i + 16, 1)]
                v = jnp.where(low, lo, swap(hi))
                mean = jnp.where(low[:1], first, swap(second))
                rstd = jnp.where(low[:1], swap(first), second)
                y_out[t // 4, 2 * u + (t // 2) % 2, 32 + 8 * (t % 2) + s] = ((v - mean) * rstd * gain).astype(BF16)
            return carry

        lax.fori_loop(0, rows // 8, wide, 0)
        lax.fori_loop(0, rows // 16, tail, 0)

    def back(u, begin):
        for block in blocks:
            for c, group, count, place, tag in MESSAGES[u]:
                dest = block * 2 + c
                src = y_out.at[block, pl.ds(group, count)]
                dst = y_hbm.at[me, pl.ds(place, count)]

                @pl.when(dest != me)
                def _():
                    copy = remote(src, dst, ys_s.at[block, c, tag], ys_r.at[me, tag], row=dest)
                    copy.start() if begin else copy.wait_send()

                @pl.when(dest == me)
                def _():
                    copy = pltpu.make_async_copy(src, dst, loc.at[4 + tag])
                    copy.start() if begin else copy.wait()

    scatter_a(0)
    scatter_a(1)
    scatter_b()
    scatter_a(2)
    direct(0)
    forward(0, 0, row_count)
    direct(1)
    forward(1, 0, row_count)
    spread()
    arrived(0)
    product(0)
    partial(0)
    direct(2)
    combine(0)
    arrived(1)
    product(1)
    partial(1)
    normalize(0)
    combine(1)
    back(0, True)
    forward(2, 0, row_count // 2)
    normalize(1)
    back(1, True)
    forward(2, row_count // 2, row_count)
    arrived(2)
    product(2)
    partial(2)
    combine(2)
    normalize(2)
    back(2, True)

    for copy in sends:
        copy.wait_send()
    for u in range(3):
        back(u, False)
    for c in range(2):
        @pl.when(core == c)
        def _():
            for q in range(1, row_count):
                for tag, (place, count) in enumerate(ARRIVALS[c]):
                    ref = y_hbm.at[peers[q], pl.ds(place, count)]
                    remote(y_out.at[0, pl.ds(0, count)], ref, ys_s.at[0, 0, tag], ys_r.at[peers[q], tag], row=peers[q]).wait_recv()


def exchange(a, b, gain, row_count, col_count):
    heads, _, half, _ = a.shape
    per = heads // row_count
    depth = row_count * half
    rows = col_count * HALF
    groups = 2 * half // 32
    wire = (row_count, per, 3, half, LANES)
    dma = pltpu.SemaphoreType.DMA
    gains = jnp.broadcast_to(gain.astype(F32)[:, None], (heads, LANES))
    hbm = pl.BlockSpec(memory_space=pl.ANY)
    return pl.pallas_call(
        functools.partial(exchange_kernel, row_count, col_count),
        in_specs=[hbm, hbm, pl.BlockSpec(memory_space=pltpu.VMEM)],
        out_specs=hbm,
        out_shape=jax.ShapeDtypeStruct((row_count, groups, 48, per, LANES), BF16),
        scratch_shapes=[
            pltpu.VMEM((3, col_count, row_count, per, half, LANES), BF16),
            pltpu.VMEM(wire, BF16),
            pltpu.VMEM((per, 2, depth, 2 * LANES), BF16),
            pltpu.VMEM((3, per, rows + 8, LANES), F32),
            pltpu.VMEM((3, per, rows + 8, LANES), F32),
            pltpu.VMEM((3, 3, rows, LANES), F32),
            pltpu.VMEM((3, row_count, 3, rows // row_count, LANES), F32),
            pltpu.VMEM((3, 3, rows, LANES), F32),
            pltpu.VMEM((col_count, 2 * groups, 48, per, LANES), BF16),
            dma((3, row_count)), dma((3, row_count)), dma((row_count,)), dma((row_count,)),
            dma((3, 2, row_count)), dma((3, 2, row_count)), dma((3, row_count)), dma((3, row_count)),
            dma((3, row_count)), dma((3, row_count)), dma((3, row_count)), dma((3, row_count)),
            dma((col_count, 2, 2)), dma((row_count, 2)), dma((6,)),
        ],
        compiler_params=pltpu.CompilerParams(collective_id=0, has_side_effects=True, vmem_limit_bytes=62 * 2**20),
        cost_estimate=pl.CostEstimate(flops=12 * per * depth * 2 * LANES * rows, bytes_accessed=a.size * 8, transcendentals=0),
    )(a.reshape(wire), b.reshape(wire), gains)


def solution(mesh):
    row_count = mesh.shape['row']
    col_count = mesh.shape['col']
    tile_spec = P(('batch', 'row'), 'col', None)
    mask_spec = P(('batch', 'row'), 'col')

    def local_step(z, mask, g_in, w_a, w_ag, w_b, w_bg, w_g, g_out, w_o):
        weights = jnp.concatenate([w_a, w_ag, w_b, w_bg], axis=1).T
        x, a, b = project(z, mask, g_in, weights)
        y = exchange(a, b, g_out, row_count, col_count)
        return finish(y, x, z, w_g, w_o)

    return jax.shard_map(local_step, mesh=mesh, in_specs=(tile_spec, mask_spec) + (P(),) * 8, out_specs=tile_spec, check_vma=False)
```

```python
import functools

import jax
import jax.numpy as jnp
from jax import lax
from jax.experimental import pallas as pl
from jax.experimental.pallas import tpu as pltpu
from jax.sharding import PartitionSpec as P

LN_EPS = 0.00001
LANES = 128
HALF = 64
GROUP = 16
PITCH = 24
F32 = jnp.float32
BF16 = jnp.bfloat16


def dot(lhs, rhs, dims):
    return lax.dot_general(lhs, rhs, (dims, ((), ())), preferred_element_type=F32)


def layer_norm(values, gain):
    mean = jnp.mean(values, axis=-1, keepdims=True)
    centered = values - mean
    variance = jnp.mean(centered * centered, axis=-1, keepdims=True)
    return centered * lax.rsqrt(variance + LN_EPS) * gain


def finish_kernel(y_ref, x_ref, z_ref, wg_ref, wo_ref, out_ref):
    srcs, _, _, per, _ = y_ref.shape
    heads = srcs * per

    def update(pos):
        return dot(y_ref[:, 0, pos].reshape(heads, LANES), wo_ref[...], ((0,), (0,)))

    def gated(x, z, upd):
        gate = jax.nn.sigmoid(dot(x, wg_ref[...], ((1,), (0,))))
        return (z.astype(F32) + gate * upd).astype(BF16)

    def wide(t, carry):
        out_ref[t, :LANES] = gated(x_ref[t, :LANES], z_ref[t, :LANES], update(t))
        return carry

    def narrow(t, carry):
        x = jnp.concatenate([x_ref[t, LANES:], x_ref[t + 16, LANES:]], axis=0)
        z = jnp.concatenate([z_ref[t, LANES:], z_ref[t + 16, LANES:]], axis=0)
        res = gated(x, z, update(t + 32))
        out_ref[t, LANES:] = res[:HALF]
        out_ref[t + 16, LANES:] = res[HALF:]
        return carry

    lax.fori_loop(0, 32, wide, 0, unroll=2)
    lax.fori_loop(0, 16, narrow, 0, unroll=2)


def finish(y, x, z, w_gate, w_out):
    rows, cols, chan = z.shape
    srcs, groups, places, per, _ = y.shape
    tile_spec = pl.BlockSpec((32, cols, chan), lambda t: (t, 0, 0))
    return pl.pallas_call(
        finish_kernel,
        grid=(groups,),
        in_specs=[
            pl.BlockSpec((srcs, 1, places, per, LANES), lambda t: (0, t, 0, 0, 0)),
            tile_spec,
            tile_spec,
            pl.BlockSpec(w_gate.shape, lambda t: (0, 0)),
            pl.BlockSpec(w_out.shape, lambda t: (0, 0)),
        ],
        out_specs=tile_spec,
        out_shape=jax.ShapeDtypeStruct(z.shape, BF16),
        compiler_params=pltpu.CompilerParams(vmem_limit_bytes=60 * 2**20),
        cost_estimate=pl.CostEstimate(flops=4 * rows * cols * chan * chan, bytes_accessed=rows * cols * chan * 8, transcendentals=0),
    )(y, x.reshape(z.shape), z, w_gate, w_out)


def remote(src, dst, send_sem, recv_sem, **place):
    return pltpu.make_async_remote_copy(
        src_ref=src, dst_ref=dst, send_sem=send_sem, recv_sem=recv_sem, device_id=place, device_id_type=pl.DeviceIdType.MESH
    )


MESSAGES = (((0, 0, 2, 0, 0),), ((0, 2, 1, 2, 1), (1, 3, 1, 0, 0)), ((1, 4, 2, 1, 1),))
ARRIVALS = (((0, 2), (2, 1)), ((0, 1), (1, 2)))


def exchange_kernel(
    row_count, col_count, z_hbm, m_ref, gi_ref, wa_ref, wag_ref, wb_ref, wbg_ref, go_ref, y_hbm, x_hbm,
    zx, weights, keep, gains, turn, a_out, b_out, all_a, got_b, rhs, o_wide, o_tail, st_part, st_got, st_tot, y_out,
    xa_s, xa_r, xb_s, xb_r, dir_s, dir_r, fwd_s, fwd_r, rs_s, rs_r, ag_s, ag_r, ys_s, ys_r, loc,
):
    me, col = lax.axis_index('row'), lax.axis_index('col')
    per, _, half, _ = a_out.shape[1:]
    heads = per * row_count
    depth = row_count * half
    chip, core = me // 2, me % 2
    chips = row_count // 2
    steps = [(0, 0), (0, 1)]
    for d in range(1, chips // 2 + 1):
        steps += [(d, 0), (-d, 0), (d, 1), (-d, 1)] if 2 * d < chips else [(d, 0), (d, 1)]
    peers = [lax.rem(chip + d + chips, chips) * 2 + lax.rem(core + f, 2) for d, f in steps]
    up, down = lax.rem(col + 1, col_count), lax.rem(col + col_count - 1, col_count)
    far = lax.rem(col + 2, col_count)
    order = (col, down, up, far)

    loads = [pltpu.make_async_copy(z_hbm.at[:, :, pl.ds(HALF * s, HALF)], zx.at[s], loc.at[s]) for s in range(3)]
    saves = [pltpu.make_async_copy(zx.at[s], x_hbm.at[:, :, pl.ds(HALF * s, HALF)], loc.at[3 + s]) for s in range(3)]
    for copy in loads:
        copy.start()
    barrier = pltpu.get_barrier_semaphore()
    for p in peers[1:]:
        pl.semaphore_signal(barrier, inc=1, device_id={'row': p}, device_id_type=pl.DeviceIdType.MESH)
    for p in (up, down):
        pl.semaphore_signal(barrier, inc=1, device_id={'col': p}, device_id_type=pl.DeviceIdType.MESH)

    for n, ref in enumerate((wa_ref, wag_ref, wb_ref, wbg_ref)):
        weights[n * heads:(n + 1) * heads] = ref[...].T
    gains[...] = jnp.broadcast_to(go_ref[...].astype(F32), (heads, heads)).T
    gain_in = gi_ref[...].astype(F32)
    mask = m_ref[...].astype(F32)
    low_mask, high_mask = mask[:half], mask[half:]
    for s in range(3):
        at = slice(HALF * s, HALF * (s + 1))
        keep[s] = jnp.concatenate([low_mask[:, at], high_mask[:, at]], axis=1)

    flat_turn = turn.reshape(2 * heads * PITCH, LANES)
    flat_out = [ref.reshape(heads, 3, half, LANES) for ref in (a_out, b_out)]

    def project(s, sides, fresh):
        def group(g, carry):
            def row(t, carry):
                k = g * GROUP + t
                tall = jnp.concatenate([zx[s, 0, k], zx[s, 1, k]], axis=0)
                if fresh:
                    tall = layer_norm(tall.astype(F32), gain_in).astype(BF16)
                    zx[s, 0, k] = tall[:HALF]
                    zx[s, 1, k] = tall[HALF:]
                for side in sides:
                    both = dot(weights[2 * side * heads:2 * (side + 1) * heads], tall, ((1,), (1,)))
                    act = keep[s, pl.ds(k, 1)] * jax.nn.sigmoid(both[heads:]) * both[:heads]
                    flat_turn[pl.ds(side * heads * PITCH + t, heads, stride=PITCH), :] = act
                return carry

            lax.fori_loop(0, GROUP, row, 0, unroll=2)

            def pack(h, carry):
                for side in sides:
                    flat_out[side][h, s, pl.ds(pl.multiple_of(g * GROUP, GROUP), GROUP)] = turn[side * heads + h, 0:GROUP].astype(BF16)
                return carry

            lax.fori_loop(0, heads, pack, 0, unroll=4)
            return carry

        lax.fori_loop(0, half // GROUP, group, 0)

    sends = []

    def send(*args, **place):
        copy = remote(*args, **place)
        copy.start()
        sends.append(copy)

    def scatter_a(s):
        for q in range(1, row_count):
            send(a_out.at[peers[q], :, s], all_a.at[s, col, me], xa_s.at[s, q], xa_r.at[s, me], row=peers[q])
        all_a[s, col, me] = a_out[me, :, s]

    def scatter_b():
        for q in range(1, row_count):
            send(b_out.at[peers[q]], got_b.at[me], xb_s.at[q], xb_r.at[me], row=peers[q])
        got_b[me] = b_out[me]

    def direct(s, first, last):
        for q in range(first, last):
            src = all_a.at[s, col, peers[q]]
            if q:
                remote(src, src, xa_s.at[s, q], xa_r.at[s, peers[q]], row=peers[q]).wait_recv()
            send(src, src, dir_s.at[s, 0, q], dir_r.at[s, 0, peers[q]], col=up)
            send(src, src, dir_s.at[s, 1, q], dir_r.at[s, 1, peers[q]], col=down)

    def forward(s, first, last):
        for q in range(first, last):
            for way, block in ((0, down), (1, up)):
                ref = all_a.at[s, block, peers[q]]
                remote(ref, ref, dir_s.at[s, way, q], dir_r.at[s, way, peers[q]], col=up).wait_recv()
            away, block = (up, down) if q % 2 == 0 else (down, up)
            src = all_a.at[s, block, peers[q]]
            send(src, src, fwd_s.at[s, q], fwd_r.at[s, peers[q]], col=away)

    def arrived(s):
        for q in range(row_count):
            ref = all_a.at[s, far, peers[q]]
            remote(ref, ref, fwd_s.at[s, q], fwd_r.at[s, peers[q]], col=up).wait_recv()

    lane = lax.broadcasted_iota(jnp.int32, (8, LANES), 1)
    pitch = o_wide.shape[2]
    flat_wide = o_wide.reshape(2 * per * pitch, LANES)
    flat_tail = o_tail.reshape(2 * per * pitch, LANES)

    def swap(v):
        return pltpu.roll(v, HALF, v.ndim - 1)

    def spread():
        for q in range(1, row_count):
            ref = got_b.at[peers[q]]
            remote(ref, ref, xb_s.at[q], xb_r.at[peers[q]], row=peers[q]).wait_recv()

        def channel(h, carry):
            w = [got_b[:, h, s].reshape(depth, LANES) for s in range(3)]
            rhs[h, 0, :, :LANES] = jnp.concatenate([w[0][:, :HALF], w[1][:, :HALF]], axis=1)
            rhs[h, 1, :, :LANES] = jnp.concatenate([w[0][:, HALF:], w[1][:, HALF:]], axis=1)
            rhs[h, 0, :, LANES:] = w[2]
            rhs[h, 1, :, LANES:] = jnp.concatenate([w[2][:, HALF:], w[2][:, :HALF]], axis=1)
            return carry

        lax.fori_loop(0, per, channel, 0)

    def product(u, s, first, count):
        at = slice(first * HALF, (first + count) * HALF)

        def channel(h, carry):
            turned = [all_a[s, c, :, h].reshape(depth, LANES).T for c in order[first:first + count]]
            res = dot(jnp.concatenate([t[:HALF] for t in turned], axis=0), rhs[h, 0], ((1,), (0,)))
            res += dot(jnp.concatenate([t[HALF:] for t in turned], axis=0), rhs[h, 1], ((1,), (0,)))
            o_wide[s % 2, h, at] = res[:, :LANES]
            o_tail[s % 2, h, at] = res[:, LANES:]
            return carry

        lax.fori_loop(0, per, channel, 0)

    def partial(u, s, first, count):
        def tile(t, carry):
            at = pl.ds(pl.multiple_of(first * HALF + 8 * t, 8), 8)
            out = []
            for ref in (o_wide, o_tail):
                v = ref[s % 2, :, at]
                mean = jnp.sum(v, axis=0) * (1.0 / per)
                out += [mean, jnp.sum((v - mean) ** 2, axis=0)]
            st_part[s, 0, at] = out[0]
            st_part[s, 1, at] = out[1]
            st_part[s, 2, at] = jnp.where(lane < HALF, out[2], swap(out[3]))
            return carry

        lax.fori_loop(0, count * HALF // 8, tile, 0, unroll=2)
        own = count * HALF // row_count
        for q in range(1, row_count):
            at = pl.ds(pl.multiple_of(first * HALF + own * peers[q], 8), own)
            send(st_part.at[s, :, at], st_got.at[u, me, :, 0:own], rs_s.at[u, q], rs_r.at[u, me], row=peers[q])

    def combine(u, s, first, count):
        own = count * HALF // row_count
        base = pl.multiple_of(first * HALF + own * me, 8)
        st_got[u, me, :, 0:own] = st_part[s, :, pl.ds(base, own)]
        for q in range(1, row_count):
            ref = st_got.at[u, peers[q], :, 0:own]
            remote(ref, ref, rs_s.at[u, q], rs_r.at[u, peers[q]], row=peers[q]).wait_recv()
        for t in range(own // 8):
            at = slice(8 * t, 8 * t + 8)
            to = pl.ds(pl.multiple_of(base + 8 * t, 8), 8)
            means, squares, both = st_got[u, :, 0, at], st_got[u, :, 1, at], st_got[u, :, 2, at]
            mean = jnp.sum(means, axis=0) * (1.0 / row_count)
            square = jnp.sum(squares, axis=0) + per * jnp.sum((means - mean) ** 2, axis=0)
            st_tot[s, 0, to] = mean
            st_tot[s, 1, to] = lax.rsqrt(square * (1.0 / heads) + LN_EPS)
            total = jnp.sum(both, axis=0)
            mean = total * (1.0 / row_count)
            square = total + swap(per * jnp.sum((both - mean) ** 2, axis=0))
            st_tot[s, 2, to] = jnp.where(lane < HALF, mean, lax.rsqrt(square * (1.0 / heads) + LN_EPS))
        for q in range(1, row_count):
            ref = st_tot.at[s, :, pl.ds(base, own)]
            send(ref, ref, ag_s.at[u, q], ag_r.at[u, me], row=peers[q])

    gain_out = gains[pl.ds(pl.multiple_of(me * per, 8), per), :]
    low = lax.broadcasted_iota(jnp.int32, (per, LANES), 1) < HALF

    def normalize(u, s, first, count):
        own = count * HALF // row_count
        for q in range(1, row_count):
            ref = st_tot.at[s, :, pl.ds(pl.multiple_of(first * HALF + own * peers[q], 8), own)]
            remote(ref, ref, ag_s.at[u, q], ag_r.at[u, peers[q]], row=peers[q]).wait_recv()
        base = (s % 2) * (per * pitch)

        def wide(t, carry):
            for r in range(8):
                i = 8 * t + r
                v = flat_wide[pl.ds(base + i, per, stride=pitch), :]
                v = (v - st_tot[s, 0, pl.ds(i, 1)]) * st_tot[s, 1, pl.ds(i, 1)] * gain_out
                y_out[t // 8, 2 * s + (t // 4) % 2, 8 * (t % 4) + r] = v.astype(BF16)
            return carry

        def tail(t, carry):
            for r in range(8):
                i = 32 * (t // 2) + 8 * (t % 2) + r
                lo = flat_tail[pl.ds(base + i, per, stride=pitch), :]
                hi = flat_tail[pl.ds(base + i + 16, per, stride=pitch), :]
                one, two = st_tot[s, 2, pl.ds(i, 1)], st_tot[s, 2, pl.ds(i + 16, 1)]
                v = jnp.where(low, lo, swap(hi))
                mean = jnp.where(low[:1], one, swap(two))
                rstd = jnp.where(low[:1], swap(one), two)
                y_out[t // 4, 2 * s + (t // 2) % 2, 32 + 8 * (t % 2) + r] = ((v - mean) * rstd * gain_out).astype(BF16)
            return carry

        lax.fori_loop(8 * first, 8 * (first + count), wide, 0)
        lax.fori_loop(4 * first, 4 * (first + count), tail, 0)

    def back(u, s, first, count, begin=True):
        for n in range(first, first + count):
            for c, group, size, place, tag in MESSAGES[s]:
                dest = order[n] * 2 + c
                src = y_out.at[n, pl.ds(group, size)]
                dst = y_hbm.at[me, pl.ds(place, size)]

                @pl.when(dest != me)
                def _():
                    copy = remote(src, dst, ys_s.at[n, c, tag], ys_r.at[me, tag], row=dest)
                    copy.start() if begin else copy.wait_send()

                @pl.when(dest == me)
                def _():
                    copy = pltpu.make_async_copy(src, dst, loc.at[6 + tag])
                    copy.start() if begin else copy.wait()

    units = [(0, 0, 0, col_count), (1, 1, 0, col_count), (2, 2, 0, col_count - 1), (3, 2, col_count - 1, 1)]

    loads[0].wait()
    project(0, (0,), True)
    pl.semaphore_wait(barrier, row_count + 1)
    scatter_a(0)
    direct(0, 0, 1)
    loads[1].wait()
    project(1, (0,), True)
    scatter_a(1)
    direct(0, 1, 4)
    project(0, (1,), False)
    project(1, (1,), False)
    direct(0, 4, 6)
    loads[2].wait()
    project(2, (0, 1), True)
    scatter_b()
    scatter_a(2)
    for copy in saves:
        copy.start()
    direct(0, 6, row_count)
    forward(0, 0, row_count)
    direct(1, 0, row_count)
    forward(1, 0, row_count)
    spread()
    arrived(0)
    product(*units[0])
    partial(*units[0])
    direct(2, 0, row_count)
    combine(*units[0])
    arrived(1)
    product(*units[1])
    partial(*units[1])
    normalize(*units[0])
    combine(*units[1])
    back(*units[0])
    forward(2, 0, row_count // 2)
    normalize(*units[1])
    back(*units[1])
    forward(2, row_count // 2, row_count)
    product(*units[2])
    partial(*units[2])
    combine(*units[2])
    arrived(2)
    product(*units[3])
    partial(*units[3])
    normalize(*units[2])
    combine(*units[3])
    back(*units[2])
    normalize(*units[3])
    back(*units[3])

    for copy in saves:
        copy.wait()
    for copy in sends:
        copy.wait_send()
    for unit in units:
        back(*unit, begin=False)
    for c in range(2):
        @pl.when(core == c)
        def _():
            for q in range(1, row_count):
                for tag, (place, size) in enumerate(ARRIVALS[c]):
                    ref = y_hbm.at[peers[q], pl.ds(place, size)]
                    remote(y_out.at[0, pl.ds(0, size)], ref, ys_s.at[0, 0, tag], ys_r.at[peers[q], tag], row=peers[q]).wait_recv()


def exchange(z, mask, g_in, w_a, w_ag, w_b, w_bg, g_out, row_count, col_count):
    tile_rows, cols, chan = z.shape
    heads = w_a.shape[1]
    half = tile_rows // 2
    per = heads // row_count
    depth = row_count * half
    rows = col_count * HALF
    groups = tile_rows // 32
    wire = (row_count, per, 3, half, LANES)
    dma = pltpu.SemaphoreType.DMA
    hbm = pl.BlockSpec(memory_space=pl.ANY)
    vmem = pl.BlockSpec(memory_space=pltpu.VMEM)
    return pl.pallas_call(
        functools.partial(exchange_kernel, row_count, col_count),
        in_specs=[hbm] + [vmem] * 7,
        out_specs=[hbm, hbm],
        out_shape=[
            jax.ShapeDtypeStruct((row_count, groups, 48, per, LANES), BF16),
            jax.ShapeDtypeStruct((2, half, cols, chan), BF16),
        ],
        scratch_shapes=[
            pltpu.VMEM((3, 2, half, HALF, chan), BF16),
            pltpu.VMEM((4 * heads, chan), BF16),
            pltpu.VMEM((3, half, LANES), F32),
            pltpu.VMEM((heads, LANES), F32),
            pltpu.VMEM((2 * heads, PITCH, LANES), F32),
            pltpu.VMEM(wire, BF16),
            pltpu.VMEM(wire, BF16),
            pltpu.VMEM((3, col_count, row_count, per, half, LANES), BF16),
            pltpu.VMEM(wire, BF16),
            pltpu.VMEM((per, 2, depth, 2 * LANES), BF16),
            pltpu.VMEM((2, per, rows + 8, LANES), F32),
            pltpu.VMEM((2, per, rows + 8, LANES), F32),
            pltpu.VMEM((3, 3, rows, LANES), F32),
            pltpu.VMEM((4, row_count, 3, rows // row_count, LANES), F32),
            pltpu.VMEM((3, 3, rows, LANES), F32),
            pltpu.VMEM((col_count, 2 * groups, 48, per, LANES), BF16),
            dma((3, row_count)), dma((3, row_count)), dma((row_count,)), dma((row_count,)),
            dma((3, 2, row_count)), dma((3, 2, row_count)), dma((3, row_count)), dma((3, row_count)),
            dma((4, row_count)), dma((4, row_count)), dma((4, row_count)), dma((4, row_count)),
            dma((col_count, 2, 2)), dma((row_count, 2)), dma((8,)),
        ],
        compiler_params=pltpu.CompilerParams(collective_id=0, has_side_effects=True, vmem_limit_bytes=67000000),
        cost_estimate=pl.CostEstimate(flops=12 * per * depth * 2 * LANES * rows, bytes_accessed=z.size * 8, transcendentals=0),
    )(z.reshape(2, half, cols, chan), mask, g_in.reshape(1, chan), w_a, w_ag, w_b, w_bg, g_out.reshape(1, heads))


def solution(mesh):
    row_count = mesh.shape['row']
    col_count = mesh.shape['col']
    tile_spec = P(('batch', 'row'), 'col', None)
    mask_spec = P(('batch', 'row'), 'col')

    def local_step(z, mask, g_in, w_a, w_ag, w_b, w_bg, w_g, g_out, w_o):
        y, x = exchange(z, mask, g_in, w_a, w_ag, w_b, w_bg, g_out, row_count, col_count)
        return finish(y, x, z, w_g, w_o)

    return jax.shard_map(local_step, mesh=mesh, in_specs=(tile_spec, mask_spec) + (P(),) * 8, out_specs=tile_spec, check_vma=False)
```

```python
import functools

import jax
import jax.numpy as jnp
from jax import lax
from jax.experimental import pallas as pl
from jax.experimental.pallas import tpu as pltpu
from jax.sharding import PartitionSpec as P

LN_EPS = 0.00001
LANES = 128
HALF = 64
GROUP = 16
PITCH = 24
BATCH = 16
QUART = 32
PAIR = 2
UNROLL = 4
F32 = jnp.float32
BF16 = jnp.bfloat16


def dot(lhs, rhs, dims):
    return lax.dot_general(lhs, rhs, (dims, ((), ())), preferred_element_type=F32)


def layer_norm(values, gain):
    mean = jnp.mean(values, axis=-1, keepdims=True)
    centered = values - mean
    variance = jnp.mean(centered * centered, axis=-1, keepdims=True)
    return centered * lax.rsqrt(variance + LN_EPS) * gain


def finish_kernel(y_ref, x_ref, z_ref, wg_ref, wo_ref, out_ref):
    srcs, _, _, per, _ = y_ref.shape
    heads = srcs * per

    def gated(x, z, upd):
        gate = jax.nn.sigmoid(dot(x, wg_ref[...], ((1,), (0,))))
        return (z.astype(F32) + gate * upd).astype(BF16)

    def wide(i, carry):
        t = BATCH * i
        at = pl.ds(t, BATCH)
        turned = jnp.concatenate([y_ref[:, 0, t + r].reshape(heads, LANES) for r in range(BATCH)], axis=1)
        upd = dot(turned, wo_ref[...], ((0,), (0,)))
        x = jnp.concatenate([x_ref[s, at] for s in range(2)], axis=1).reshape(BATCH * LANES, LANES)
        parts = [slice(QUART * n, QUART * (n + 1)) for n in (0, 3, 1, 4)]
        z = jnp.concatenate([z_ref[at, part] for part in parts], axis=1).reshape(BATCH * LANES, LANES)
        res = gated(x, z, upd).reshape(BATCH, LANES, LANES)
        for e, part in enumerate(parts):
            out_ref[at, part] = res[:, QUART * e:QUART * (e + 1)]
        return carry

    lax.fori_loop(0, 32 // BATCH, wide, 0)
    turned = jnp.concatenate([y_ref[:, 0, 32 + r].reshape(heads, LANES) for r in range(16)], axis=1)
    upd = dot(turned, wo_ref[...], ((0,), (0,)))
    rows = [r + 16 * h for r in range(16) for h in range(2)]
    x = jnp.concatenate([x_ref[2, p] for p in rows], axis=0)
    z = jnp.concatenate([z_ref[p, QUART * n:QUART * (n + 1)] for p in rows for n in (2, 5)], axis=0)
    res = gated(x, z, upd)
    for e, p in enumerate(rows):
        for n in range(2):
            out_ref[p, QUART * (2 + 3 * n):QUART * (3 + 3 * n)] = res[HALF * e + QUART * n:HALF * e + QUART * (n + 1)]


def finish(y, x, z, w_gate, w_out):
    rows, cols, chan = z.shape
    srcs, groups, places, per, _ = y.shape
    tile_spec = pl.BlockSpec((32, cols, chan), lambda t: (t, 0, 0))
    return pl.pallas_call(
        finish_kernel,
        grid=(groups,),
        in_specs=[
            pl.BlockSpec((srcs, 1, places, per, LANES), lambda t: (0, t, 0, 0, 0)),
            pl.BlockSpec((3, 32, HALF, chan), lambda t: (0, t, 0, 0)),
            tile_spec,
            pl.BlockSpec(w_gate.shape, lambda t: (0, 0)),
            pl.BlockSpec(w_out.shape, lambda t: (0, 0)),
        ],
        out_specs=tile_spec,
        out_shape=jax.ShapeDtypeStruct(z.shape, BF16),
        compiler_params=pltpu.CompilerParams(vmem_limit_bytes=60 * 2**20),
        cost_estimate=pl.CostEstimate(flops=4 * rows * cols * chan * chan, bytes_accessed=rows * cols * chan * 8, transcendentals=0),
    )(y, x.reshape(3, rows, HALF, chan), z, w_gate, w_out)


def remote(src, dst, send_sem, recv_sem, **place):
    return pltpu.make_async_remote_copy(
        src_ref=src, dst_ref=dst, send_sem=send_sem, recv_sem=recv_sem, device_id=place, device_id_type=pl.DeviceIdType.MESH
    )


def exchange_kernel(
    row_count, col_count, z_hbm, m_ref, gi_ref, wa_ref, wag_ref, wb_ref, wbg_ref, go_ref, y_hbm, x_hbm,
    zx, weights, keep, gains, turn, a_out, b_out, all_a, got_b, rhs, o_wide, o_tail, st_part, st_got, st_tot, y_out,
    xa_s, xa_r, xb_s, xb_r, dir_s, dir_r, fwd_s, fwd_r, rs_s, rs_r, ag_s, ag_r, ys_s, ys_r, loc,
):
    me, col = lax.axis_index('row'), lax.axis_index('col')
    per, _, half, _ = a_out.shape[1:]
    heads = per * row_count
    depth = row_count * half
    chip, core = me // 2, me % 2
    chips = row_count // 2
    steps = [(0, 0), (0, 1)]
    for d in range(1, chips // 2 + 1):
        steps += [(d, 0), (-d, 0), (d, 1), (-d, 1)] if 2 * d < chips else [(d, 0), (d, 1)]
    peers = [lax.rem(chip + d + chips, chips) * 2 + lax.rem(core + f, 2) for d, f in steps]
    up, down = lax.rem(col + 1, col_count), lax.rem(col + col_count - 1, col_count)
    far = lax.rem(col + 2, col_count)
    order = (col, down, up, far)

    loads = [
        [
            pltpu.make_async_copy(z_hbm.at[:, :, pl.ds(QUART * (s + 3 * e), QUART)], zx.at[s, :, :, pl.ds(QUART * e, QUART)], loc.at[s, e])
            for e in range(2)
        ]
        for s in range(3)
    ]
    saves = [pltpu.make_async_copy(zx.at[s], x_hbm.at[s], loc.at[s, 2]) for s in range(3)]
    for pair in loads:
        for copy in pair:
            copy.start()

    def loaded(s):
        for copy in loads[s]:
            copy.wait()

    barrier = pltpu.get_barrier_semaphore()
    for p in peers[1:]:
        pl.semaphore_signal(barrier, inc=1, device_id={'row': p}, device_id_type=pl.DeviceIdType.MESH)
    for p in (up, down):
        pl.semaphore_signal(barrier, inc=1, device_id={'col': p}, device_id_type=pl.DeviceIdType.MESH)

    for n, ref in enumerate((wa_ref, wag_ref, wb_ref, wbg_ref)):
        weights[n * heads:(n + 1) * heads] = ref[...].T
    gains[...] = jnp.broadcast_to(go_ref[...].astype(F32), (heads, heads)).T
    gain_in = gi_ref[...].astype(F32)
    mask = m_ref[...].astype(F32)
    low_mask, high_mask = mask[:half], mask[half:]
    for s in range(3):
        keep[s] = jnp.concatenate([m[:, QUART * n:QUART * (n + 1)] for m in (low_mask, high_mask) for n in (s, s + 3)], axis=1)

    flat_turn = turn.reshape(2 * heads * PITCH, LANES)
    flat_out = [ref.reshape(heads, 3, half, LANES) for ref in (a_out, b_out)]

    def project(s, sides, fresh, between=()):
        if fresh:
            def norm(i, carry):
                at = pl.ds(4 * i, 4)
                v = zx[s, :, at].astype(F32).reshape(4 * LANES, heads)
                zx[s, :, at] = layer_norm(v, gain_in).astype(BF16).reshape(2, 4, HALF, heads)
                return carry

            lax.fori_loop(0, half // 4, norm, 0)

        for g in range(half // GROUP):
            def row(i, carry):
                t = PAIR * i
                k = g * GROUP + t
                tall = jnp.concatenate([zx[s, e, k + r] for r in range(PAIR) for e in range(2)], axis=0)
                for side in sides:
                    both = dot(weights[2 * side * heads:2 * (side + 1) * heads], tall, ((1,), (1,)))
                    for r in range(PAIR):
                        at = slice(LANES * r, LANES * (r + 1))
                        act = keep[s, pl.ds(k + r, 1)] * jax.nn.sigmoid(both[heads:, at]) * both[:heads, at]
                        flat_turn[pl.ds(side * heads * PITCH + t + r, heads, stride=PITCH), :] = act
                return carry

            lax.fori_loop(0, GROUP // PAIR, row, 0, unroll=2)

            def pack(h, carry):
                for side in sides:
                    flat_out[side][h, s, g * GROUP:(g + 1) * GROUP] = turn[side * heads + h, 0:GROUP].astype(BF16)
                return carry

            lax.fori_loop(0, heads, pack, 0, unroll=8)
            if g < len(between):
                between[g]()

    sends = []

    def send(*args, **place):
        copy = remote(*args, **place)
        copy.start()
        sends.append(copy)

    def scatter_a(s):
        for q in range(1, row_count):
            send(a_out.at[peers[q], :, s], all_a.at[s, col, me], xa_s.at[s, q], xa_r.at[s, me], row=peers[q])
        all_a[s, col, me] = a_out[me, :, s]

    def scatter_b():
        for q in range(1, row_count):
            send(b_out.at[peers[q]], got_b.at[me], xb_s.at[q], xb_r.at[me], row=peers[q])
        got_b[me] = b_out[me]

    def direct(s, first, last):
        for q in range(first, last):
            src = all_a.at[s, col, peers[q]]
            if q:
                remote(src, src, xa_s.at[s, q], xa_r.at[s, peers[q]], row=peers[q]).wait_recv()
            send(src, src, dir_s.at[s, 0, q], dir_r.at[s, 0, peers[q]], col=up)
            send(src, src, dir_s.at[s, 1, q], dir_r.at[s, 1, peers[q]], col=down)

    def forward(s, first, last):
        for q in range(first, last):
            for way, block in ((0, down), (1, up)):
                ref = all_a.at[s, block, peers[q]]
                remote(ref, ref, dir_s.at[s, way, q], dir_r.at[s, way, peers[q]], col=up).wait_recv()
            away, block = (up, down) if q % 2 == 0 else (down, up)
            src = all_a.at[s, block, peers[q]]
            send(src, src, fwd_s.at[s, q], fwd_r.at[s, peers[q]], col=away)

    def arrived(s):
        for q in range(row_count):
            ref = all_a.at[s, far, peers[q]]
            remote(ref, ref, fwd_s.at[s, q], fwd_r.at[s, peers[q]], col=up).wait_recv()

    lane = lax.broadcasted_iota(jnp.int32, (8, LANES), 1)
    pitch = o_wide.shape[2]
    flat_wide = o_wide.reshape(2 * per * pitch, LANES)
    flat_tail = o_tail.reshape(2 * per * pitch, LANES)

    def swap(v):
        return pltpu.roll(v, HALF, v.ndim - 1)

    def spread():
        for q in range(1, row_count):
            ref = got_b.at[peers[q]]
            remote(ref, ref, xb_s.at[q], xb_r.at[peers[q]], row=peers[q]).wait_recv()

        def channel(h, carry):
            w = [got_b[:, h, s].reshape(depth, LANES) for s in range(3)]
            rhs[h, 0, :, :LANES] = jnp.concatenate([w[0][:, :HALF], w[1][:, :HALF]], axis=1)
            rhs[h, 1, :, :LANES] = jnp.concatenate([w[0][:, HALF:], w[1][:, HALF:]], axis=1)
            rhs[h, 0, :, LANES:] = w[2]
            rhs[h, 1, :, LANES:] = jnp.concatenate([w[2][:, HALF:], w[2][:, :HALF]], axis=1)
            return carry

        lax.fori_loop(0, per, channel, 0, unroll=UNROLL)

    def product(u, s, first, count):
        at = slice(first * HALF, (first + count) * HALF)

        def channel(h, carry):
            turned = [all_a[s, c, :, h].reshape(depth, LANES).T for c in order[first:first + count]]
            res = dot(jnp.concatenate([t[:HALF] for t in turned], axis=0), rhs[h, 0], ((1,), (0,)))
            res += dot(jnp.concatenate([t[HALF:] for t in turned], axis=0), rhs[h, 1], ((1,), (0,)))
            o_wide[s % 2, h, at] = res[:, :LANES]
            o_tail[s % 2, h, at] = res[:, LANES:]
            return carry

        lax.fori_loop(0, per, channel, 0, unroll=UNROLL)

    def partial(u, s, first, count):
        def tile(t, carry):
            at = pl.ds(pl.multiple_of(first * HALF + 8 * t, 8), 8)
            out = []
            for ref in (o_wide, o_tail):
                v = ref[s % 2, :, at]
                mean = jnp.sum(v, axis=0) * (1.0 / per)
                out += [mean, jnp.sum((v - mean) ** 2, axis=0)]
            st_part[s, 0, at] = out[0]
            st_part[s, 1, at] = out[1]
            st_part[s, 2, at] = jnp.where(lane < HALF, out[2], swap(out[3]))
            return carry

        lax.fori_loop(0, count * HALF // 8, tile, 0, unroll=UNROLL)
        own = count * HALF // row_count
        for q in range(1, row_count):
            at = pl.ds(pl.multiple_of(first * HALF + own * peers[q], 8), own)
            send(st_part.at[s, :, at], st_got.at[u, me, :, 0:own], rs_s.at[u, q], rs_r.at[u, me], row=peers[q])

    def combine(u, s, first, count):
        own = count * HALF // row_count
        base = pl.multiple_of(first * HALF + own * me, 8)
        st_got[u, me, :, 0:own] = st_part[s, :, pl.ds(base, own)]
        for q in range(1, row_count):
            ref = st_got.at[u, peers[q], :, 0:own]
            remote(ref, ref, rs_s.at[u, q], rs_r.at[u, peers[q]], row=peers[q]).wait_recv()
        for t in range(own // 8):
            at = slice(8 * t, 8 * t + 8)
            to = pl.ds(pl.multiple_of(base + 8 * t, 8), 8)
            means, squares, both = st_got[u, :, 0, at], st_got[u, :, 1, at], st_got[u, :, 2, at]
            mean = jnp.sum(means, axis=0) * (1.0 / row_count)
            square = jnp.sum(squares, axis=0) + per * jnp.sum((means - mean) ** 2, axis=0)
            st_tot[s, 0, to] = mean
            st_tot[s, 1, to] = lax.rsqrt(square * (1.0 / heads) + LN_EPS)
            total = jnp.sum(both, axis=0)
            mean = total * (1.0 / row_count)
            square = total + swap(per * jnp.sum((both - mean) ** 2, axis=0))
            st_tot[s, 2, to] = jnp.where(lane < HALF, mean, lax.rsqrt(square * (1.0 / heads) + LN_EPS))
        for q in range(1, row_count):
            ref = st_tot.at[s, :, pl.ds(base, own)]
            send(ref, ref, ag_s.at[u, q], ag_r.at[u, me], row=peers[q])

    gain_out = gains[pl.ds(pl.multiple_of(me * per, 8), per), :]
    low = lax.broadcasted_iota(jnp.int32, (per, LANES), 1) < HALF

    def normalize(u, s, first, count):
        own = count * HALF // row_count
        for q in range(1, row_count):
            ref = st_tot.at[s, :, pl.ds(pl.multiple_of(first * HALF + own * peers[q], 8), own)]
            remote(ref, ref, ag_s.at[u, q], ag_r.at[u, peers[q]], row=peers[q]).wait_recv()
        base = (s % 2) * (per * pitch)

        def wide(t, carry):
            for r in range(8):
                i = 8 * t + r
                v = flat_wide[pl.ds(base + i, per, stride=pitch), :]
                v = (v - st_tot[s, 0, pl.ds(i, 1)]) * st_tot[s, 1, pl.ds(i, 1)] * gain_out
                y_out[t // 8, s + 3 * ((t // 4) % 2), 8 * (t % 4) + r] = v.astype(BF16)
            return carry

        def tail(t, carry):
            for r in range(8):
                i = 32 * (t // 2) + 8 * (t % 2) + r
                lo = flat_tail[pl.ds(base + i, per, stride=pitch), :]
                hi = flat_tail[pl.ds(base + i + 16, per, stride=pitch), :]
                one, two = st_tot[s, 2, pl.ds(i, 1)], st_tot[s, 2, pl.ds(i + 16, 1)]
                v = jnp.where(low, lo, swap(hi))
                mean = jnp.where(low[:1], one, swap(two))
                rstd = jnp.where(low[:1], swap(one), two)
                y_out[t // 4, s + 3 * ((t // 2) % 2), 32 + 8 * (t % 2) + r] = ((v - mean) * rstd * gain_out).astype(BF16)
            return carry

        lax.fori_loop(8 * first, 8 * (first + count), wide, 0, unroll=UNROLL)
        lax.fori_loop(4 * first, 4 * (first + count), tail, 0, unroll=UNROLL)

    def back(u, s, first, count, begin=True):
        for n in range(first, first + count):
            for c in range(2):
                dest = order[n] * 2 + c
                src = y_out.at[n, s + 3 * c]
                dst = y_hbm.at[me, s]

                @pl.when(dest != me)
                def _():
                    copy = remote(src, dst, ys_s.at[n, c, s], ys_r.at[me, s], row=dest)
                    copy.start() if begin else copy.wait_send()

                @pl.when(dest == me)
                def _():
                    copy = pltpu.make_async_copy(src, dst, loc.at[s, 3])
                    copy.start() if begin else copy.wait()

    units = [(0, 0, 0, col_count), (1, 1, 0, col_count), (2, 2, 0, col_count - 1), (3, 2, col_count - 1, 1)]

    def nothing():
        pass

    loaded(0)
    project(0, (0,), True)
    pl.semaphore_wait(barrier, row_count + 1)
    scatter_a(0)
    direct(0, 0, 1)
    loaded(1)
    project(1, (0,), True, (nothing, lambda: direct(0, 1, 2)))
    scatter_a(1)
    project(0, (1,), False, (nothing, nothing, lambda: direct(0, 2, 4)))
    project(1, (1,), False, (nothing, nothing, lambda: direct(0, 4, 6)))
    loaded(2)
    project(2, (0, 1), True, (nothing, nothing, lambda: direct(0, 6, row_count)))
    scatter_b()
    scatter_a(2)
    for copy in saves:
        copy.start()
    forward(0, 0, row_count)
    direct(1, 0, row_count)
    forward(1, 0, row_count)
    spread()
    arrived(0)
    product(*units[0])
    partial(*units[0])
    direct(2, 0, row_count)
    combine(*units[0])
    arrived(1)
    product(*units[1])
    partial(*units[1])
    normalize(*units[0])
    combine(*units[1])
    back(*units[0])
    forward(2, 0, row_count // 2)
    normalize(*units[1])
    back(*units[1])
    forward(2, row_count // 2, row_count)
    product(*units[2])
    partial(*units[2])
    combine(*units[2])
    arrived(2)
    product(*units[3])
    partial(*units[3])
    normalize(*units[2])
    combine(*units[3])
    back(*units[2])
    normalize(*units[3])
    back(*units[3])

    for copy in saves:
        copy.wait()
    for copy in sends:
        copy.wait_send()
    for unit in units:
        back(*unit, begin=False)
    for q in range(1, row_count):
        for n in range(3):
            ref = y_hbm.at[peers[q], n]
            remote(y_out.at[0, 0], ref, ys_s.at[0, 0, n], ys_r.at[peers[q], n], row=peers[q]).wait_recv()


def exchange(z, mask, g_in, w_a, w_ag, w_b, w_bg, g_out, row_count, col_count):
    tile_rows, cols, chan = z.shape
    heads = w_a.shape[1]
    half = tile_rows // 2
    per = heads // row_count
    depth = row_count * half
    rows = col_count * HALF
    groups = tile_rows // 32
    wire = (row_count, per, 3, half, LANES)
    dma = pltpu.SemaphoreType.DMA
    hbm = pl.BlockSpec(memory_space=pl.ANY)
    vmem = pl.BlockSpec(memory_space=pltpu.VMEM)
    return pl.pallas_call(
        functools.partial(exchange_kernel, row_count, col_count),
        in_specs=[hbm] + [vmem] * 7,
        out_specs=[hbm, hbm],
        out_shape=[
            jax.ShapeDtypeStruct((row_count, groups, 48, per, LANES), BF16),
            jax.ShapeDtypeStruct((3, 2, half, HALF, chan), BF16),
        ],
        scratch_shapes=[
            pltpu.VMEM((3, 2, half, HALF, chan), BF16),
            pltpu.VMEM((4 * heads, chan), BF16),
            pltpu.VMEM((3, half, LANES), F32),
            pltpu.VMEM((heads, LANES), F32),
            pltpu.VMEM((2 * heads, PITCH, LANES), F32),
            pltpu.VMEM(wire, BF16),
            pltpu.VMEM(wire, BF16),
            pltpu.VMEM((3, col_count, row_count, per, half, LANES), BF16),
            pltpu.VMEM(wire, BF16),
            pltpu.VMEM((per, 2, depth, 2 * LANES), BF16),
            pltpu.VMEM((2, per, rows + 8, LANES), F32),
            pltpu.VMEM((2, per, rows + 8, LANES), F32),
            pltpu.VMEM((3, 3, rows, LANES), F32),
            pltpu.VMEM((4, row_count, 3, rows // row_count, LANES), F32),
            pltpu.VMEM((3, 3, rows, LANES), F32),
            pltpu.VMEM((col_count, 2 * groups, 48, per, LANES), BF16),
            dma((3, row_count)), dma((3, row_count)), dma((row_count,)), dma((row_count,)),
            dma((3, 2, row_count)), dma((3, 2, row_count)), dma((3, row_count)), dma((3, row_count)),
            dma((4, row_count)), dma((4, row_count)), dma((4, row_count)), dma((4, row_count)),
            dma((col_count, 2, 3)), dma((row_count, 3)), dma((3, 4)),
        ],
        compiler_params=pltpu.CompilerParams(collective_id=0, has_side_effects=True, vmem_limit_bytes=67000000),
        cost_estimate=pl.CostEstimate(flops=12 * per * depth * 2 * LANES * rows, bytes_accessed=z.size * 8, transcendentals=0),
    )(z.reshape(2, half, cols, chan), mask, g_in.reshape(1, chan), w_a, w_ag, w_b, w_bg, g_out.reshape(1, heads))


def solution(mesh):
    row_count = mesh.shape['row']
    col_count = mesh.shape['col']
    tile_spec = P(('batch', 'row'), 'col', None)
    mask_spec = P(('batch', 'row'), 'col')

    def local_step(z, mask, g_in, w_a, w_ag, w_b, w_bg, w_g, g_out, w_o):
        y, x = exchange(z, mask, g_in, w_a, w_ag, w_b, w_bg, g_out, row_count, col_count)
        return finish(y, x, z, w_g, w_o)

    return jax.shard_map(local_step, mesh=mesh, in_specs=(tile_spec, mask_spec) + (P(),) * 8, out_specs=tile_spec, check_vma=False)
```

```python
import functools

import jax
import jax.numpy as jnp
from jax import lax
from jax.experimental import pallas as pl
from jax.experimental.pallas import tpu as pltpu
from jax.sharding import PartitionSpec as P

LN_EPS = 0.00001
LANES = 128
HALF = 64
GROUP = 16
PITCH = 24
BATCH = 16
QUART = 32
PAIR = 2
UNROLL = 4
F32 = jnp.float32
BF16 = jnp.bfloat16


def dot(lhs, rhs, dims):
    return lax.dot_general(lhs, rhs, (dims, ((), ())), preferred_element_type=F32)


def layer_norm(values, gain):
    mean = jnp.mean(values, axis=-1, keepdims=True)
    centered = values - mean
    variance = jnp.mean(centered * centered, axis=-1, keepdims=True)
    return centered * lax.rsqrt(variance + LN_EPS) * gain


def finish_kernel(y_ref, x_ref, z_ref, wg_ref, wo_ref, out_ref):
    srcs, _, _, per, _ = y_ref.shape
    heads = srcs * per

    def gated(x, z, upd):
        gate = jax.nn.sigmoid(dot(x, wg_ref[...], ((1,), (0,))))
        return (z.astype(F32) + gate * upd).astype(BF16)

    def wide(i, carry):
        t = BATCH * i
        at = pl.ds(t, BATCH)
        turned = jnp.concatenate([y_ref[:, 0, t + r].reshape(heads, LANES) for r in range(BATCH)], axis=1)
        upd = dot(turned, wo_ref[...], ((0,), (0,)))
        x = jnp.concatenate([x_ref[s, at] for s in range(2)], axis=1).reshape(BATCH * LANES, LANES)
        parts = [slice(QUART * n, QUART * (n + 1)) for n in (0, 3, 1, 4)]
        z = jnp.concatenate([z_ref[at, part] for part in parts], axis=1).reshape(BATCH * LANES, LANES)
        res = gated(x, z, upd).reshape(BATCH, LANES, LANES)
        for e, part in enumerate(parts):
            out_ref[at, part] = res[:, QUART * e:QUART * (e + 1)]
        return carry

    lax.fori_loop(0, 32 // BATCH, wide, 0)
    turned = jnp.concatenate([y_ref[:, 0, 32 + r].reshape(heads, LANES) for r in range(16)], axis=1)
    upd = dot(turned, wo_ref[...], ((0,), (0,)))
    rows = [r + 16 * h for r in range(16) for h in range(2)]
    x = jnp.concatenate([x_ref[2, p] for p in rows], axis=0)
    z = jnp.concatenate([z_ref[p, QUART * n:QUART * (n + 1)] for p in rows for n in (2, 5)], axis=0)
    res = gated(x, z, upd)
    for e, p in enumerate(rows):
        for n in range(2):
            out_ref[p, QUART * (2 + 3 * n):QUART * (3 + 3 * n)] = res[HALF * e + QUART * n:HALF * e + QUART * (n + 1)]


def finish(y, x, z, w_gate, w_out):
    rows, cols, chan = z.shape
    srcs, groups, places, per, _ = y.shape
    tile_spec = pl.BlockSpec((32, cols, chan), lambda t: (t, 0, 0))
    return pl.pallas_call(
        finish_kernel,
        grid=(groups,),
        in_specs=[
            pl.BlockSpec((srcs, 1, places, per, LANES), lambda t: (0, t, 0, 0, 0)),
            pl.BlockSpec((3, 32, HALF, chan), lambda t: (0, t, 0, 0)),
            tile_spec,
            pl.BlockSpec(w_gate.shape, lambda t: (0, 0)),
            pl.BlockSpec(w_out.shape, lambda t: (0, 0)),
        ],
        out_specs=tile_spec,
        out_shape=jax.ShapeDtypeStruct(z.shape, BF16),
        compiler_params=pltpu.CompilerParams(vmem_limit_bytes=60 * 2**20),
        cost_estimate=pl.CostEstimate(flops=4 * rows * cols * chan * chan, bytes_accessed=rows * cols * chan * 8, transcendentals=0),
    )(y, x.reshape(3, rows, HALF, chan), z, w_gate, w_out)


def remote(src, dst, send_sem, recv_sem, **place):
    return pltpu.make_async_remote_copy(
        src_ref=src, dst_ref=dst, send_sem=send_sem, recv_sem=recv_sem, device_id=place, device_id_type=pl.DeviceIdType.MESH
    )


def exchange_kernel(
    row_count, col_count, z_hbm, m_ref, gi_ref, wa_ref, wag_ref, wb_ref, wbg_ref, go_ref, y_hbm, x_hbm,
    zx, weights, keep, gains, turn, a_out, b_out, all_a, got_b, rhs, o_wide, o_tail, st_part, st_pair, st_chip, st_got, st_far, st_tot, y_out,
    xa_s, xa_r, xb_s, xb_r, dir_s, dir_r, fwd_s, fwd_r, pr_s, pr_r, rs_s, rs_r, ag_s, ag_r, sh_s, sh_r, ys_s, ys_r, loc,
):
    me, col = lax.axis_index('row'), lax.axis_index('col')
    per, _, half, _ = a_out.shape[1:]
    heads = per * row_count
    depth = row_count * half
    chip, core = me // 2, me % 2
    chips = row_count // 2
    steps = [(0, 0), (0, 1)]
    for d in range(1, chips // 2 + 1):
        steps += [(d, 0), (-d, 0), (d, 1), (-d, 1)] if 2 * d < chips else [(d, 0), (d, 1)]
    peers = [lax.rem(chip + d + chips, chips) * 2 + lax.rem(core + f, 2) for d, f in steps]
    up, down = lax.rem(col + 1, col_count), lax.rem(col + col_count - 1, col_count)
    far = lax.rem(col + 2, col_count)
    order = (col, down, up, far)
    alike = [q for q, (d, f) in enumerate(steps) if d and not f]

    loads = [
        [
            pltpu.make_async_copy(z_hbm.at[:, :, pl.ds(QUART * (s + 3 * e), QUART)], zx.at[s, :, :, pl.ds(QUART * e, QUART)], loc.at[s, e])
            for e in range(2)
        ]
        for s in range(3)
    ]
    saves = [pltpu.make_async_copy(zx.at[s], x_hbm.at[s], loc.at[s, 2]) for s in range(3)]
    for pair in loads:
        for copy in pair:
            copy.start()

    def loaded(s):
        for copy in loads[s]:
            copy.wait()

    barrier = pltpu.get_barrier_semaphore()
    for p in peers[1:]:
        pl.semaphore_signal(barrier, inc=1, device_id={'row': p}, device_id_type=pl.DeviceIdType.MESH)
    for p in (up, down):
        pl.semaphore_signal(barrier, inc=1, device_id={'col': p}, device_id_type=pl.DeviceIdType.MESH)

    for n, ref in enumerate((wa_ref, wag_ref, wb_ref, wbg_ref)):
        weights[n * heads:(n + 1) * heads] = ref[...].T
    gains[...] = jnp.broadcast_to(go_ref[...].astype(F32), (heads, heads)).T
    gain_in = gi_ref[...].astype(F32)
    mask = m_ref[...].astype(F32)
    low_mask, high_mask = mask[:half], mask[half:]
    for s in range(3):
        keep[s] = jnp.concatenate([m[:, QUART * n:QUART * (n + 1)] for m in (low_mask, high_mask) for n in (s, s + 3)], axis=1)

    flat_turn = turn.reshape(2 * heads * PITCH, LANES)
    flat_out = [ref.reshape(heads, 3, half, LANES) for ref in (a_out, b_out)]

    def project(s, sides, fresh, between=()):
        if fresh:
            def norm(i, carry):
                at = pl.ds(4 * i, 4)
                v = zx[s, :, at].astype(F32).reshape(4 * LANES, heads)
                zx[s, :, at] = layer_norm(v, gain_in).astype(BF16).reshape(2, 4, HALF, heads)
                return carry

            lax.fori_loop(0, half // 4, norm, 0)

        for g in range(half // GROUP):
            def row(i, carry):
                t = PAIR * i
                k = g * GROUP + t
                tall = jnp.concatenate([zx[s, e, k + r] for r in range(PAIR) for e in range(2)], axis=0)
                for side in sides:
                    both = dot(weights[2 * side * heads:2 * (side + 1) * heads], tall, ((1,), (1,)))
                    for r in range(PAIR):
                        at = slice(LANES * r, LANES * (r + 1))
                        act = keep[s, pl.ds(k + r, 1)] * jax.nn.sigmoid(both[heads:, at]) * both[:heads, at]
                        flat_turn[pl.ds(side * heads * PITCH + t + r, heads, stride=PITCH), :] = act
                return carry

            lax.fori_loop(0, GROUP // PAIR, row, 0, unroll=4)

            def pack(h, carry):
                for side in sides:
                    flat_out[side][h, s, g * GROUP:(g + 1) * GROUP] = turn[side * heads + h, 0:GROUP].astype(BF16)
                return carry

            lax.fori_loop(0, heads, pack, 0, unroll=8)
            if g < len(between):
                between[g]()

    sends = []

    def send(*args, **place):
        copy = remote(*args, **place)
        copy.start()
        sends.append(copy)

    def scatter_a(s, first=1, last=row_count):
        for q in range(first, last):
            send(a_out.at[peers[q], :, s], all_a.at[s, col, me], xa_s.at[s, q], xa_r.at[s, me], row=peers[q])
        if first == 1:
            all_a[s, col, me] = a_out[me, :, s]

    def scatter_b():
        for q in range(1, row_count):
            send(b_out.at[peers[q]], got_b.at[me], xb_s.at[q], xb_r.at[me], row=peers[q])
        got_b[me] = b_out[me]

    def direct(s, first, last):
        for q in range(first, last):
            src = all_a.at[s, col, peers[q]]
            if q:
                remote(src, src, xa_s.at[s, q], xa_r.at[s, peers[q]], row=peers[q]).wait_recv()
            send(src, src, dir_s.at[s, 0, q], dir_r.at[s, 0, peers[q]], col=up)
            send(src, src, dir_s.at[s, 1, q], dir_r.at[s, 1, peers[q]], col=down)

    def forward(s, first, last):
        for q in range(first, last):
            for way, block in ((0, down), (1, up)):
                ref = all_a.at[s, block, peers[q]]
                remote(ref, ref, dir_s.at[s, way, q], dir_r.at[s, way, peers[q]], col=up).wait_recv()
            away, block = (up, down) if q % 2 == 0 else (down, up)
            src = all_a.at[s, block, peers[q]]
            send(src, src, fwd_s.at[s, q], fwd_r.at[s, peers[q]], col=away)

    def arrived(s):
        for q in range(row_count):
            ref = all_a.at[s, far, peers[q]]
            remote(ref, ref, fwd_s.at[s, q], fwd_r.at[s, peers[q]], col=up).wait_recv()

    lane = lax.broadcasted_iota(jnp.int32, (8, LANES), 1)
    pitch = o_wide.shape[2]
    flat_wide = o_wide.reshape(2 * per * pitch, LANES)
    flat_tail = o_tail.reshape(2 * per * pitch, LANES)

    def swap(v):
        return pltpu.roll(v, HALF, v.ndim - 1)

    def spread():
        for q in range(1, row_count):
            ref = got_b.at[peers[q]]
            remote(ref, ref, xb_s.at[q], xb_r.at[peers[q]], row=peers[q]).wait_recv()

        def channel(h, carry):
            w = [got_b[:, h, s].reshape(depth, LANES) for s in range(3)]
            rhs[h, 0, :, :LANES] = jnp.concatenate([w[0][:, :HALF], w[1][:, :HALF]], axis=1)
            rhs[h, 1, :, :LANES] = jnp.concatenate([w[0][:, HALF:], w[1][:, HALF:]], axis=1)
            rhs[h, 0, :, LANES:] = w[2]
            rhs[h, 1, :, LANES:] = jnp.concatenate([w[2][:, HALF:], w[2][:, :HALF]], axis=1)
            return carry

        lax.fori_loop(0, per, channel, 0, unroll=UNROLL)

    def product(u, s, first, count):
        at = slice(first * HALF, (first + count) * HALF)

        def channel(h, carry):
            turned = [all_a[s, c, :, h].reshape(depth, LANES).T for c in order[first:first + count]]
            res = dot(jnp.concatenate([t[:HALF] for t in turned], axis=0), rhs[h, 0], ((1,), (0,)))
            res += dot(jnp.concatenate([t[HALF:] for t in turned], axis=0), rhs[h, 1], ((1,), (0,)))
            o_wide[s % 2, h, at] = res[:, :LANES]
            o_tail[s % 2, h, at] = res[:, LANES:]
            return carry

        lax.fori_loop(0, per, channel, 0, unroll=UNROLL)

    def partial(u, s, first, count):
        def tile(t, carry):
            at = pl.ds(pl.multiple_of(first * HALF + 8 * t, 8), 8)
            out = []
            for ref in (o_wide, o_tail):
                v = ref[s % 2, :, at]
                mean = jnp.sum(v, axis=0) * (1.0 / per)
                out += [mean, jnp.sum((v - mean) ** 2, axis=0)]
            st_part[s, 0, at] = out[0]
            st_part[s, 1, at] = out[1]
            st_part[s, 2, at] = jnp.where(lane < HALF, out[2], swap(out[3]))
            return carry

        lax.fori_loop(0, count * HALF // 8, tile, 0, unroll=UNROLL)
        if count == 1:
            for q in range(1, row_count):
                at = pl.ds(pl.multiple_of(first * HALF + 8 * peers[q], 8), 8)
                send(st_part.at[s, :, at], st_far.at[me], rs_s.at[u, q], rs_r.at[u, me], row=peers[q])
            return
        size = count * HALF // 2
        at = pl.ds(pl.multiple_of(first * HALF + size * (1 - core), 8), size)
        send(st_part.at[s, :, at], st_pair.at[u, :, 0:size], pr_s.at[u], pr_r.at[u], row=peers[1])

    def merge(u, s, first, count):
        size = count * HALF // 2
        own = size // chips
        ref = st_pair.at[u, :, 0:size]
        remote(ref, ref, pr_s.at[u], pr_r.at[u], row=peers[1]).wait_recv()

        def tile(t, carry):
            at = pl.ds(pl.multiple_of(8 * t, 8), 8)
            mine = st_part[s, :, pl.ds(pl.multiple_of(first * HALF + size * core + 8 * t, 8), 8)]
            other = st_pair[u, :, at]
            total = mine + other
            gap = (mine - other) ** 2 * (0.5 * per)
            st_chip[u, 0, at] = 0.5 * total[0]
            st_chip[u, 1, at] = total[1] + gap[0]
            st_chip[u, 2, at] = jnp.where(lane < HALF, 0.5 * total[2], total[2] + swap(gap[2]))
            return carry

        lax.fori_loop(0, size // 8, tile, 0, unroll=UNROLL)
        for q in alike:
            at = pl.ds(pl.multiple_of(own * (peers[q] // 2), 8), own)
            send(st_chip.at[u, :, at], st_got.at[u, chip, :, 0:own], rs_s.at[u, q], rs_r.at[u, chip], row=peers[q])

    def settle(s, to, weight, means, squares, both):
        parts = means.shape[0]
        mean = jnp.sum(means, axis=0) * (1.0 / parts)
        square = jnp.sum(squares, axis=0) + weight * jnp.sum((means - mean) ** 2, axis=0)
        st_tot[s, 0, to] = mean
        st_tot[s, 1, to] = lax.rsqrt(square * (1.0 / heads) + LN_EPS)
        total = jnp.sum(both, axis=0)
        mean = total * (1.0 / parts)
        square = total + swap(weight * jnp.sum((both - mean) ** 2, axis=0))
        st_tot[s, 2, to] = jnp.where(lane < HALF, mean, lax.rsqrt(square * (1.0 / heads) + LN_EPS))

    def combine(u, s, first, count):
        size = count * HALF // 2
        own = size // chips
        base = pl.multiple_of(first * HALF + size * core + own * chip, 8)
        st_got[u, chip, :, 0:own] = st_chip[u, :, pl.ds(pl.multiple_of(own * chip, 8), own)]
        for q in alike:
            ref = st_got.at[u, peers[q] // 2, :, 0:own]
            remote(ref, ref, rs_s.at[u, q], rs_r.at[u, peers[q] // 2], row=peers[q]).wait_recv()
        for t in range(own // 8):
            at = slice(8 * t, 8 * t + 8)
            settle(s, pl.ds(pl.multiple_of(base + 8 * t, 8), 8), 2 * per, *(st_got[u, :, n, at] for n in range(3)))
        for q in alike:
            ref = st_tot.at[s, :, pl.ds(base, own)]
            send(ref, ref, ag_s.at[u, q], ag_r.at[u, chip], row=peers[q])

    def combine_far(u, s, first, count):
        base = pl.multiple_of(first * HALF + 8 * me, 8)
        at = pl.ds(base, 8)
        st_far[me] = st_part[s, :, at]
        for q in range(1, row_count):
            ref = st_far.at[peers[q]]
            remote(ref, ref, rs_s.at[u, q], rs_r.at[u, peers[q]], row=peers[q]).wait_recv()
        settle(s, at, per, *(st_far[:, n] for n in range(3)))
        for q in range(1, row_count):
            ref = st_tot.at[s, :, at]
            send(ref, ref, ag_s.at[u, q], ag_r.at[u, me], row=peers[q])

    def share(u, s, first, count):
        size = count * HALF // 2
        own = size // chips
        base = first * HALF + size * core
        for q in alike:
            ref = st_tot.at[s, :, pl.ds(pl.multiple_of(base + own * (peers[q] // 2), 8), own)]
            remote(ref, ref, ag_s.at[u, q], ag_r.at[u, peers[q] // 2], row=peers[q]).wait_recv()
        ref = st_tot.at[s, :, pl.ds(pl.multiple_of(base, 8), size)]
        send(ref, ref, sh_s.at[u], sh_r.at[u], row=peers[1])

    gain_out = gains[pl.ds(pl.multiple_of(me * per, 8), per), :]
    low = lax.broadcasted_iota(jnp.int32, (per, LANES), 1) < HALF

    def normalize(u, s, first, count):
        if count == 1:
            for q in range(1, row_count):
                ref = st_tot.at[s, :, pl.ds(pl.multiple_of(first * HALF + 8 * peers[q], 8), 8)]
                remote(ref, ref, ag_s.at[u, q], ag_r.at[u, peers[q]], row=peers[q]).wait_recv()
        else:
            size = count * HALF // 2
            ref = st_tot.at[s, :, pl.ds(pl.multiple_of(first * HALF + size * (1 - core), 8), size)]
            remote(ref, ref, sh_s.at[u], sh_r.at[u], row=peers[1]).wait_recv()
        base = (s % 2) * (per * pitch)

        def wide(t, carry):
            for r in range(8):
                i = 8 * t + r
                v = flat_wide[pl.ds(base + i, per, stride=pitch), :]
                v = (v - st_tot[s, 0, pl.ds(i, 1)]) * st_tot[s, 1, pl.ds(i, 1)] * gain_out
                y_out[t // 8, s + 3 * ((t // 4) % 2), 8 * (t % 4) + r] = v.astype(BF16)
            return carry

        def tail(t, carry):
            for r in range(8):
                i = 32 * (t // 2) + 8 * (t % 2) + r
                lo = flat_tail[pl.ds(base + i, per, stride=pitch), :]
                hi = flat_tail[pl.ds(base + i + 16, per, stride=pitch), :]
                one, two = st_tot[s, 2, pl.ds(i, 1)], st_tot[s, 2, pl.ds(i + 16, 1)]
                v = jnp.where(low, lo, swap(hi))
                mean = jnp.where(low[:1], one, swap(two))
                rstd = jnp.where(low[:1], swap(one), two)
                y_out[t // 4, s + 3 * ((t // 2) % 2), 32 + 8 * (t % 2) + r] = ((v - mean) * rstd * gain_out).astype(BF16)
            return carry

        lax.fori_loop(8 * first, 8 * (first + count), wide, 0, unroll=UNROLL)
        lax.fori_loop(4 * first, 4 * (first + count), tail, 0, unroll=UNROLL)

    def back(u, s, first, count, begin=True, cores=(0, 1)):
        for c in cores:
            for n in range(first, first + count):
                dest = order[n] * 2 + c
                src = y_out.at[n, s + 3 * c]
                dst = y_hbm.at[me, s]

                @pl.when(dest != me)
                def _():
                    copy = remote(src, dst, ys_s.at[n, c, s], ys_r.at[me, s], row=dest)
                    copy.start() if begin else copy.wait_send()

                @pl.when(dest == me)
                def _():
                    copy = pltpu.make_async_copy(src, dst, loc.at[s, 3])
                    copy.start() if begin else copy.wait()

    units = [(0, 0, 0, col_count), (1, 1, 0, col_count), (2, 2, 0, col_count - 1), (3, 2, col_count - 1, 1)]

    def nothing():
        pass

    loaded(0)
    project(0, (0,), True)
    pl.semaphore_wait(barrier, row_count + 1)
    scatter_a(0)
    direct(0, 0, 1)
    loaded(1)
    project(1, (0,), True, (nothing, lambda: direct(0, 1, 2)))
    scatter_a(1)
    project(0, (1,), False, (nothing, nothing, lambda: direct(0, 2, 4)))
    project(1, (1,), False, (nothing, nothing, lambda: direct(0, 4, 6)))
    loaded(2)
    project(2, (0, 1), True, (nothing, nothing, lambda: direct(0, 6, row_count)))
    scatter_b()
    scatter_a(2, 1, row_count)
    for copy in saves:
        copy.start()
    forward(0, 0, row_count)
    direct(1, 0, row_count)
    forward(1, 0, row_count)
    spread()
    arrived(0)
    product(*units[0])
    partial(*units[0])
    merge(*units[0])
    direct(2, 0, row_count)
    combine(*units[0])
    arrived(1)
    product(*units[1])
    partial(*units[1])
    share(*units[0])
    merge(*units[1])
    normalize(*units[0])
    back(*units[0], cores=(0,))
    combine(*units[1])
    back(*units[0], cores=(1,))
    share(*units[1])
    forward(2, 0, 4)
    normalize(*units[1])
    back(*units[1], cores=(0,))
    forward(2, 4, 8)
    product(*units[2])
    partial(*units[2])
    merge(*units[2])
    combine(*units[2])
    back(*units[1], cores=(1,))
    share(*units[2])
    arrived(2)
    product(*units[3])
    partial(*units[3])
    normalize(*units[2])
    combine_far(*units[3])
    back(*units[2])
    normalize(*units[3])
    back(*units[3])

    for copy in saves:
        copy.wait()
    for copy in sends:
        copy.wait_send()
    for unit in units:
        back(*unit, begin=False)
    for q in range(1, row_count):
        for n in range(3):
            ref = y_hbm.at[peers[q], n]
            remote(y_out.at[0, 0], ref, ys_s.at[0, 0, n], ys_r.at[peers[q], n], row=peers[q]).wait_recv()


def exchange(z, mask, g_in, w_a, w_ag, w_b, w_bg, g_out, row_count, col_count):
    tile_rows, cols, chan = z.shape
    heads = w_a.shape[1]
    half = tile_rows // 2
    per = heads // row_count
    depth = row_count * half
    rows = col_count * HALF
    groups = tile_rows // 32
    wire = (row_count, per, 3, half, LANES)
    dma = pltpu.SemaphoreType.DMA
    hbm = pl.BlockSpec(memory_space=pl.ANY)
    vmem = pl.BlockSpec(memory_space=pltpu.VMEM)
    return pl.pallas_call(
        functools.partial(exchange_kernel, row_count, col_count),
        in_specs=[hbm] + [vmem] * 7,
        out_specs=[hbm, hbm],
        out_shape=[
            jax.ShapeDtypeStruct((row_count, groups, 48, per, LANES), BF16),
            jax.ShapeDtypeStruct((3, 2, half, HALF, chan), BF16),
        ],
        scratch_shapes=[
            pltpu.VMEM((3, 2, half, HALF, chan), BF16),
            pltpu.VMEM((4 * heads, chan), BF16),
            pltpu.VMEM((3, half, LANES), F32),
            pltpu.VMEM((heads, LANES), F32),
            pltpu.VMEM((2 * heads, PITCH, LANES), F32),
            pltpu.VMEM(wire, BF16),
            pltpu.VMEM(wire, BF16),
            pltpu.VMEM((3, col_count, row_count, per, half, LANES), BF16),
            pltpu.VMEM(wire, BF16),
            pltpu.VMEM((per, 2, depth, 2 * LANES), BF16),
            pltpu.VMEM((2, per, rows + 8, LANES), F32),
            pltpu.VMEM((2, per, rows + 8, LANES), F32),
            pltpu.VMEM((3, 3, rows, LANES), F32),
            pltpu.VMEM((3, 3, rows // 2, LANES), F32),
            pltpu.VMEM((3, 3, rows // 2, LANES), F32),
            pltpu.VMEM((3, row_count // 2, 3, rows // row_count, LANES), F32),
            pltpu.VMEM((row_count, 3, 8, LANES), F32),
            pltpu.VMEM((3, 3, rows, LANES), F32),
            pltpu.VMEM((col_count, 2 * groups, 48, per, LANES), BF16),
            dma((3, row_count)), dma((3, row_count)), dma((row_count,)), dma((row_count,)),
            dma((3, 2, row_count)), dma((3, 2, row_count)), dma((3, row_count)), dma((3, row_count)),
            dma((4,)), dma((4,)), dma((4, row_count)), dma((4, row_count)), dma((4, row_count)), dma((4, row_count)), dma((4,)), dma((4,)),
            dma((col_count, 2, 3)), dma((row_count, 3)), dma((3, 4)),
        ],
        compiler_params=pltpu.CompilerParams(collective_id=0, has_side_effects=True, vmem_limit_bytes=67000000),
        cost_estimate=pl.CostEstimate(flops=12 * per * depth * 2 * LANES * rows, bytes_accessed=z.size * 8, transcendentals=0),
    )(z.reshape(2, half, cols, chan), mask, g_in.reshape(1, chan), w_a, w_ag, w_b, w_bg, g_out.reshape(1, heads))


def solution(mesh):
    row_count = mesh.shape['row']
    col_count = mesh.shape['col']
    tile_spec = P(('batch', 'row'), 'col', None)
    mask_spec = P(('batch', 'row'), 'col')

    def local_step(z, mask, g_in, w_a, w_ag, w_b, w_bg, w_g, g_out, w_o):
        y, x = exchange(z, mask, g_in, w_a, w_ag, w_b, w_bg, g_out, row_count, col_count)
        return finish(y, x, z, w_g, w_o)

    return jax.shard_map(local_step, mesh=mesh, in_specs=(tile_spec, mask_spec) + (P(),) * 8, out_specs=tile_spec, check_vma=False)
```

```python
import functools

import jax
import jax.numpy as jnp
from jax import lax
from jax.experimental import pallas as pl
from jax.experimental.pallas import tpu as pltpu
from jax.sharding import PartitionSpec as P

LN_EPS = 0.00001
LANES = 128
HALF = 64
GROUP = 16
PITCH = 24
BATCH = 32
QUART = 32
PAIR = 2
UNROLL = 4
F32 = jnp.float32
BF16 = jnp.bfloat16


def dot(lhs, rhs, dims):
    return lax.dot_general(lhs, rhs, (dims, ((), ())), preferred_element_type=F32)


def layer_norm(values, gain):
    mean = jnp.mean(values, axis=-1, keepdims=True)
    centered = values - mean
    variance = jnp.mean(centered * centered, axis=-1, keepdims=True)
    return centered * lax.rsqrt(variance + LN_EPS) * gain


def finish_kernel(y_ref, x_ref, z_ref, wg_ref, wo_ref, out_ref):
    srcs, _, _, per, _ = y_ref.shape
    heads = srcs * per

    def gated(x, z, upd):
        gate = jax.nn.sigmoid(dot(x, wg_ref[...], ((1,), (0,))))
        return (z.astype(F32) + gate * upd).astype(BF16)

    def wide(i, carry):
        t = BATCH * i
        at = pl.ds(t, BATCH)
        turned = jnp.concatenate([y_ref[:, 0, t + r].reshape(heads, LANES) for r in range(BATCH)], axis=1)
        upd = dot(turned, wo_ref[...], ((0,), (0,)))
        x = jnp.concatenate([x_ref[s, at] for s in range(2)], axis=1).reshape(BATCH * LANES, LANES)
        parts = [slice(QUART * n, QUART * (n + 1)) for n in (0, 3, 1, 4)]
        z = jnp.concatenate([z_ref[at, part] for part in parts], axis=1).reshape(BATCH * LANES, LANES)
        res = gated(x, z, upd).reshape(BATCH, LANES, LANES)
        for e, part in enumerate(parts):
            out_ref[at, part] = res[:, QUART * e:QUART * (e + 1)]
        return carry

    lax.fori_loop(0, 32 // BATCH, wide, 0)
    turned = jnp.concatenate([y_ref[:, 0, 32 + r].reshape(heads, LANES) for r in range(16)], axis=1)
    upd = dot(turned, wo_ref[...], ((0,), (0,)))
    rows = [r + 16 * h for r in range(16) for h in range(2)]
    x = jnp.concatenate([x_ref[2, p] for p in rows], axis=0)
    z = jnp.concatenate([z_ref[p, QUART * n:QUART * (n + 1)] for p in rows for n in (2, 5)], axis=0)
    res = gated(x, z, upd)
    for e, p in enumerate(rows):
        for n in range(2):
            out_ref[p, QUART * (2 + 3 * n):QUART * (3 + 3 * n)] = res[HALF * e + QUART * n:HALF * e + QUART * (n + 1)]


def finish(y, x, z, w_gate, w_out):
    rows, cols, chan = z.shape
    srcs, groups, places, per, _ = y.shape
    tile_spec = pl.BlockSpec((32, cols, chan), lambda t: (t, 0, 0))
    return pl.pallas_call(
        finish_kernel,
        grid=(groups,),
        in_specs=[
            pl.BlockSpec((srcs, 1, places, per, LANES), lambda t: (0, t, 0, 0, 0)),
            pl.BlockSpec((3, 32, HALF, chan), lambda t: (0, t, 0, 0)),
            tile_spec,
            pl.BlockSpec(w_gate.shape, lambda t: (0, 0)),
            pl.BlockSpec(w_out.shape, lambda t: (0, 0)),
        ],
        out_specs=tile_spec,
        out_shape=jax.ShapeDtypeStruct(z.shape, BF16),
        compiler_params=pltpu.CompilerParams(vmem_limit_bytes=60 * 2**20),
        cost_estimate=pl.CostEstimate(flops=4 * rows * cols * chan * chan, bytes_accessed=rows * cols * chan * 8, transcendentals=0),
    )(y, x.reshape(3, rows, HALF, chan), z, w_gate, w_out)


def remote(src, dst, send_sem, recv_sem, **place):
    return pltpu.make_async_remote_copy(
        src_ref=src, dst_ref=dst, send_sem=send_sem, recv_sem=recv_sem, device_id=place, device_id_type=pl.DeviceIdType.MESH
    )


def exchange_kernel(
    row_count, col_count, z_hbm, m_ref, gi_ref, wa_ref, wag_ref, wb_ref, wbg_ref, go_ref, y_hbm, x_hbm,
    zx, weights, keep, gains, turn, a_out, b_out, all_a, got_b, rhs, o_wide, o_tail, st_part, st_pair, st_chip, st_got, st_far, st_tot, y_out,
    xa_s, xa_r, xb_s, xb_r, dir_s, dir_r, fwd_s, fwd_r, pr_s, pr_r, rs_s, rs_r, ag_s, ag_r, sh_s, sh_r, ys_s, ys_r, loc,
):
    me, col = lax.axis_index('row'), lax.axis_index('col')
    per, _, half, _ = a_out.shape[1:]
    heads = per * row_count
    depth = row_count * half
    chip, core = me // 2, me % 2
    chips = row_count // 2
    steps = [(0, 0), (0, 1)]
    for d in range(1, chips // 2 + 1):
        steps += [(d, 0), (-d, 0), (d, 1), (-d, 1)] if 2 * d < chips else [(d, 0), (d, 1)]
    peers = [lax.rem(chip + d + chips, chips) * 2 + lax.rem(core + f, 2) for d, f in steps]
    up, down = lax.rem(col + 1, col_count), lax.rem(col + col_count - 1, col_count)
    far = lax.rem(col + 2, col_count)
    order = (col, down, up, far)
    alike = [q for q, (d, f) in enumerate(steps) if d and not f]

    loads = [
        [
            pltpu.make_async_copy(z_hbm.at[:, :, pl.ds(QUART * (s + 3 * e), QUART)], zx.at[s, :, :, pl.ds(QUART * e, QUART)], loc.at[s, e])
            for e in range(2)
        ]
        for s in range(3)
    ]
    saves = [pltpu.make_async_copy(zx.at[s], x_hbm.at[s], loc.at[s, 2]) for s in range(3)]
    for pair in loads:
        for copy in pair:
            copy.start()

    def loaded(s):
        for copy in loads[s]:
            copy.wait()

    barrier = pltpu.get_barrier_semaphore()
    for p in peers[1:]:
        pl.semaphore_signal(barrier, inc=1, device_id={'row': p}, device_id_type=pl.DeviceIdType.MESH)
    for p in (up, down):
        pl.semaphore_signal(barrier, inc=1, device_id={'col': p}, device_id_type=pl.DeviceIdType.MESH)

    for n, ref in enumerate((wa_ref, wag_ref, wb_ref, wbg_ref)):
        weights[n * heads:(n + 1) * heads] = ref[...].T
    gains[...] = jnp.broadcast_to(go_ref[...].astype(F32), (heads, heads)).T
    gain_in = gi_ref[...].astype(F32)
    mask = m_ref[...].astype(F32)
    low_mask, high_mask = mask[:half], mask[half:]
    for s in range(3):
        keep[s] = jnp.concatenate([m[:, QUART * n:QUART * (n + 1)] for m in (low_mask, high_mask) for n in (s, s + 3)], axis=1)

    flat_turn = turn.reshape(2 * heads * PITCH, LANES)
    flat_out = [ref.reshape(heads, 3, half, LANES) for ref in (a_out, b_out)]

    def project(s, sides, fresh, between=()):
        if fresh:
            def norm(i, carry):
                at = pl.ds(8 * i, 8)
                v = zx[s, :, at].astype(F32).reshape(8 * LANES, heads)
                zx[s, :, at] = layer_norm(v, gain_in).astype(BF16).reshape(2, 8, HALF, heads)
                return carry

            lax.fori_loop(0, half // 8, norm, 0)

        for g in range(half // GROUP):
            def row(i, carry):
                t = PAIR * i
                k = g * GROUP + t
                tall = jnp.concatenate([zx[s, e, k + r] for r in range(PAIR) for e in range(2)], axis=0)
                for side in sides:
                    both = dot(weights[2 * side * heads:2 * (side + 1) * heads], tall, ((1,), (1,)))
                    for r in range(PAIR):
                        at = slice(LANES * r, LANES * (r + 1))
                        act = keep[s, pl.ds(k + r, 1)] * jax.nn.sigmoid(both[heads:, at]) * both[:heads, at]
                        flat_turn[pl.ds(side * heads * PITCH + t + r, heads, stride=PITCH), :] = act
                return carry

            lax.fori_loop(0, GROUP // PAIR, row, 0, unroll=8)

            def pack(h, carry):
                for side in sides:
                    flat_out[side][h, s, g * GROUP:(g + 1) * GROUP] = turn[side * heads + h, 0:GROUP].astype(BF16)
                return carry

            lax.fori_loop(0, heads, pack, 0, unroll=32)
            if g < len(between):
                between[g]()

    sends = []

    def send(*args, **place):
        copy = remote(*args, **place)
        copy.start()
        sends.append(copy)

    def scatter_a(s, first=1, last=row_count):
        for q in range(first, last):
            send(a_out.at[peers[q], :, s], all_a.at[s, col, me], xa_s.at[s, q], xa_r.at[s, me], row=peers[q])
        if first == 1:
            all_a[s, col, me] = a_out[me, :, s]

    def scatter_b():
        for q in range(1, row_count):
            send(b_out.at[peers[q]], got_b.at[me], xb_s.at[q], xb_r.at[me], row=peers[q])
        got_b[me] = b_out[me]

    def direct(s, first, last):
        for q in range(first, last):
            src = all_a.at[s, col, peers[q]]
            if q:
                remote(src, src, xa_s.at[s, q], xa_r.at[s, peers[q]], row=peers[q]).wait_recv()
            send(src, src, dir_s.at[s, 0, q], dir_r.at[s, 0, peers[q]], col=up)
            send(src, src, dir_s.at[s, 1, q], dir_r.at[s, 1, peers[q]], col=down)

    def forward(s, first, last):
        for q in range(first, last):
            for way, block in ((0, down), (1, up)):
                ref = all_a.at[s, block, peers[q]]
                remote(ref, ref, dir_s.at[s, way, q], dir_r.at[s, way, peers[q]], col=up).wait_recv()
            away, block = (up, down) if q % 2 == 0 else (down, up)
            src = all_a.at[s, block, peers[q]]
            send(src, src, fwd_s.at[s, q], fwd_r.at[s, peers[q]], col=away)

    def arrived(s):
        for q in range(row_count):
            ref = all_a.at[s, far, peers[q]]
            remote(ref, ref, fwd_s.at[s, q], fwd_r.at[s, peers[q]], col=up).wait_recv()

    lane = lax.broadcasted_iota(jnp.int32, (8, LANES), 1)
    pitch = o_wide.shape[2]
    flat_wide = o_wide.reshape(2 * per * pitch, LANES)
    flat_tail = o_tail.reshape(2 * per * pitch, LANES)

    def swap(v):
        return pltpu.roll(v, HALF, v.ndim - 1)

    def spread():
        for q in range(1, row_count):
            ref = got_b.at[peers[q]]
            remote(ref, ref, xb_s.at[q], xb_r.at[peers[q]], row=peers[q]).wait_recv()

        def channel(h, carry):
            w = [got_b[:, h, s].reshape(depth, LANES) for s in range(3)]
            rhs[h, 0, :, :LANES] = jnp.concatenate([w[0][:, :HALF], w[1][:, :HALF]], axis=1)
            rhs[h, 1, :, :LANES] = jnp.concatenate([w[0][:, HALF:], w[1][:, HALF:]], axis=1)
            rhs[h, 0, :, LANES:] = w[2]
            rhs[h, 1, :, LANES:] = jnp.concatenate([w[2][:, HALF:], w[2][:, :HALF]], axis=1)
            return carry

        lax.fori_loop(0, per, channel, 0, unroll=UNROLL)

    def product(u, s, first, count):
        at = slice(first * HALF, (first + count) * HALF)

        def channel(h, carry):
            turned = [all_a[s, c, :, h].reshape(depth, LANES).T for c in order[first:first + count]]
            res = dot(jnp.concatenate([t[:HALF] for t in turned], axis=0), rhs[h, 0], ((1,), (0,)))
            res += dot(jnp.concatenate([t[HALF:] for t in turned], axis=0), rhs[h, 1], ((1,), (0,)))
            o_wide[s % 2, h, at] = res[:, :LANES]
            o_tail[s % 2, h, at] = res[:, LANES:]
            return carry

        lax.fori_loop(0, per, channel, 0, unroll=UNROLL)

    def partial(u, s, first, count):
        def tile(t, carry):
            at = pl.ds(pl.multiple_of(first * HALF + 8 * t, 8), 8)
            out = []
            for ref in (o_wide, o_tail):
                v = ref[s % 2, :, at]
                mean = jnp.sum(v, axis=0) * (1.0 / per)
                out += [mean, jnp.sum((v - mean) ** 2, axis=0)]
            st_part[s, 0, at] = out[0]
            st_part[s, 1, at] = out[1]
            st_part[s, 2, at] = jnp.where(lane < HALF, out[2], swap(out[3]))
            return carry

        lax.fori_loop(0, count * HALF // 8, tile, 0, unroll=UNROLL)
        if count == 1:
            for q in range(1, row_count):
                at = pl.ds(pl.multiple_of(first * HALF + 8 * peers[q], 8), 8)
                send(st_part.at[s, :, at], st_far.at[me], rs_s.at[u, q], rs_r.at[u, me], row=peers[q])
            return
        size = count * HALF // 2
        at = pl.ds(pl.multiple_of(first * HALF + size * (1 - core), 8), size)
        send(st_part.at[s, :, at], st_pair.at[u, :, 0:size], pr_s.at[u], pr_r.at[u], row=peers[1])

    def merge(u, s, first, count):
        size = count * HALF // 2
        own = size // chips
        ref = st_pair.at[u, :, 0:size]
        remote(ref, ref, pr_s.at[u], pr_r.at[u], row=peers[1]).wait_recv()

        def tile(t, carry):
            at = pl.ds(pl.multiple_of(8 * t, 8), 8)
            mine = st_part[s, :, pl.ds(pl.multiple_of(first * HALF + size * core + 8 * t, 8), 8)]
            other = st_pair[u, :, at]
            total = mine + other
            gap = (mine - other) ** 2 * (0.5 * per)
            st_chip[u, 0, at] = 0.5 * total[0]
            st_chip[u, 1, at] = total[1] + gap[0]
            st_chip[u, 2, at] = jnp.where(lane < HALF, 0.5 * total[2], total[2] + swap(gap[2]))
            return carry

        lax.fori_loop(0, size // 8, tile, 0, unroll=UNROLL)
        for q in alike:
            at = pl.ds(pl.multiple_of(own * (peers[q] // 2), 8), own)
            send(st_chip.at[u, :, at], st_got.at[u, chip, :, 0:own], rs_s.at[u, q], rs_r.at[u, chip], row=peers[q])

    def settle(s, to, weight, means, squares, both):
        parts = means.shape[0]
        mean = jnp.sum(means, axis=0) * (1.0 / parts)
        square = jnp.sum(squares, axis=0) + weight * jnp.sum((means - mean) ** 2, axis=0)
        st_tot[s, 0, to] = mean
        st_tot[s, 1, to] = lax.rsqrt(square * (1.0 / heads) + LN_EPS)
        total = jnp.sum(both, axis=0)
        mean = total * (1.0 / parts)
        square = total + swap(weight * jnp.sum((both - mean) ** 2, axis=0))
        st_tot[s, 2, to] = jnp.where(lane < HALF, mean, lax.rsqrt(square * (1.0 / heads) + LN_EPS))

    def combine(u, s, first, count):
        size = count * HALF // 2
        own = size // chips
        base = pl.multiple_of(first * HALF + size * core + own * chip, 8)
        st_got[u, chip, :, 0:own] = st_chip[u, :, pl.ds(pl.multiple_of(own * chip, 8), own)]
        for q in alike:
            ref = st_got.at[u, peers[q] // 2, :, 0:own]
            remote(ref, ref, rs_s.at[u, q], rs_r.at[u, peers[q] // 2], row=peers[q]).wait_recv()
        for t in range(own // 8):
            at = slice(8 * t, 8 * t + 8)
            settle(s, pl.ds(pl.multiple_of(base + 8 * t, 8), 8), 2 * per, *(st_got[u, :, n, at] for n in range(3)))
        for q in alike:
            ref = st_tot.at[s, :, pl.ds(base, own)]
            send(ref, ref, ag_s.at[u, q], ag_r.at[u, chip], row=peers[q])

    def combine_far(u, s, first, count):
        base = pl.multiple_of(first * HALF + 8 * me, 8)
        at = pl.ds(base, 8)
        st_far[me] = st_part[s, :, at]
        for q in range(1, row_count):
            ref = st_far.at[peers[q]]
            remote(ref, ref, rs_s.at[u, q], rs_r.at[u, peers[q]], row=peers[q]).wait_recv()
        settle(s, at, per, *(st_far[:, n] for n in range(3)))
        for q in range(1, row_count):
            ref = st_tot.at[s, :, at]
            send(ref, ref, ag_s.at[u, q], ag_r.at[u, me], row=peers[q])

    def share(u, s, first, count):
        size = count * HALF // 2
        own = size // chips
        base = first * HALF + size * core
        for q in alike:
            ref = st_tot.at[s, :, pl.ds(pl.multiple_of(base + own * (peers[q] // 2), 8), own)]
            remote(ref, ref, ag_s.at[u, q], ag_r.at[u, peers[q] // 2], row=peers[q]).wait_recv()
        ref = st_tot.at[s, :, pl.ds(pl.multiple_of(base, 8), size)]
        send(ref, ref, sh_s.at[u], sh_r.at[u], row=peers[1])

    gain_out = gains[pl.ds(pl.multiple_of(me * per, 8), per), :]
    low = lax.broadcasted_iota(jnp.int32, (per, LANES), 1) < HALF

    def normalize(u, s, first, count):
        if count == 1:
            for q in range(1, row_count):
                ref = st_tot.at[s, :, pl.ds(pl.multiple_of(first * HALF + 8 * peers[q], 8), 8)]
                remote(ref, ref, ag_s.at[u, q], ag_r.at[u, peers[q]], row=peers[q]).wait_recv()
        else:
            size = count * HALF // 2
            ref = st_tot.at[s, :, pl.ds(pl.multiple_of(first * HALF + size * (1 - core), 8), size)]
            remote(ref, ref, sh_s.at[u], sh_r.at[u], row=peers[1]).wait_recv()
        base = (s % 2) * (per * pitch)

        def wide(t, carry):
            for r in range(8):
                i = 8 * t + r
                v = flat_wide[pl.ds(base + i, per, stride=pitch), :]
                v = (v - st_tot[s, 0, pl.ds(i, 1)]) * st_tot[s, 1, pl.ds(i, 1)] * gain_out
                y_out[t // 8, s + 3 * ((t // 4) % 2), 8 * (t % 4) + r] = v.astype(BF16)
            return carry

        def tail(t, carry):
            for r in range(8):
                i = 32 * (t // 2) + 8 * (t % 2) + r
                lo = flat_tail[pl.ds(base + i, per, stride=pitch), :]
                hi = flat_tail[pl.ds(base + i + 16, per, stride=pitch), :]
                one, two = st_tot[s, 2, pl.ds(i, 1)], st_tot[s, 2, pl.ds(i + 16, 1)]
                v = jnp.where(low, lo, swap(hi))
                mean = jnp.where(low[:1], one, swap(two))
                rstd = jnp.where(low[:1], swap(one), two)
                y_out[t // 4, s + 3 * ((t // 2) % 2), 32 + 8 * (t % 2) + r] = ((v - mean) * rstd * gain_out).astype(BF16)
            return carry

        lax.fori_loop(8 * first, 8 * (first + count), wide, 0, unroll=UNROLL)
        lax.fori_loop(4 * first, 4 * (first + count), tail, 0, unroll=UNROLL)

    def back(u, s, first, count, begin=True, cores=(0, 1)):
        for c in cores:
            for n in range(first, first + count):
                dest = order[n] * 2 + c
                src = y_out.at[n, s + 3 * c]
                dst = y_hbm.at[me, s]

                @pl.when(dest != me)
                def _():
                    copy = remote(src, dst, ys_s.at[n, c, s], ys_r.at[me, s], row=dest)
                    copy.start() if begin else copy.wait_send()

                @pl.when(dest == me)
                def _():
                    copy = pltpu.make_async_copy(src, dst, loc.at[s, 3])
                    copy.start() if begin else copy.wait()

    units = [(0, 0, 0, col_count), (1, 1, 0, col_count), (2, 2, 0, col_count - 1), (3, 2, col_count - 1, 1)]

    def nothing():
        pass

    loaded(0)
    project(0, (0,), True)
    pl.semaphore_wait(barrier, row_count + 1)
    scatter_a(0)
    direct(0, 0, 1)
    loaded(1)
    project(1, (0,), True, (nothing, lambda: direct(0, 1, 2)))
    scatter_a(1)
    project(0, (1,), False, (nothing, nothing, lambda: direct(0, 2, 4)))
    project(1, (1,), False, (nothing, nothing, lambda: direct(0, 4, 6)))
    loaded(2)
    project(2, (0, 1), True, (nothing, nothing, lambda: direct(0, 6, row_count)))
    scatter_b()
    scatter_a(2, 1, row_count)
    for copy in saves:
        copy.start()
    forward(0, 0, row_count)
    direct(1, 0, row_count)
    forward(1, 0, row_count)
    spread()
    arrived(0)
    product(*units[0])
    partial(*units[0])
    merge(*units[0])
    direct(2, 0, row_count)
    combine(*units[0])
    arrived(1)
    product(*units[1])
    partial(*units[1])
    share(*units[0])
    merge(*units[1])
    normalize(*units[0])
    back(*units[0], cores=(0,))
    combine(*units[1])
    back(*units[0], cores=(1,))
    share(*units[1])
    forward(2, 0, 4)
    normalize(*units[1])
    back(*units[1], cores=(0,))
    forward(2, 4, 8)
    product(*units[2])
    partial(*units[2])
    merge(*units[2])
    combine(*units[2])
    back(*units[1], cores=(1,))
    share(*units[2])
    arrived(2)
    product(*units[3])
    partial(*units[3])
    normalize(*units[2])
    combine_far(*units[3])
    back(*units[2])
    normalize(*units[3])
    back(*units[3])

    for copy in saves:
        copy.wait()
    for copy in sends:
        copy.wait_send()
    for unit in units:
        back(*unit, begin=False)
    for q in range(1, row_count):
        for n in range(3):
            ref = y_hbm.at[peers[q], n]
            remote(y_out.at[0, 0], ref, ys_s.at[0, 0, n], ys_r.at[peers[q], n], row=peers[q]).wait_recv()


def exchange(z, mask, g_in, w_a, w_ag, w_b, w_bg, g_out, row_count, col_count):
    tile_rows, cols, chan = z.shape
    heads = w_a.shape[1]
    half = tile_rows // 2
    per = heads // row_count
    depth = row_count * half
    rows = col_count * HALF
    groups = tile_rows // 32
    wire = (row_count, per, 3, half, LANES)
    dma = pltpu.SemaphoreType.DMA
    hbm = pl.BlockSpec(memory_space=pl.ANY)
    vmem = pl.BlockSpec(memory_space=pltpu.VMEM)
    return pl.pallas_call(
        functools.partial(exchange_kernel, row_count, col_count),
        in_specs=[hbm] + [vmem] * 7,
        out_specs=[hbm, hbm],
        out_shape=[
            jax.ShapeDtypeStruct((row_count, groups, 48, per, LANES), BF16),
            jax.ShapeDtypeStruct((3, 2, half, HALF, chan), BF16),
        ],
        scratch_shapes=[
            pltpu.VMEM((3, 2, half, HALF, chan), BF16),
            pltpu.VMEM((4 * heads, chan), BF16),
            pltpu.VMEM((3, half, LANES), F32),
            pltpu.VMEM((heads, LANES), F32),
            pltpu.VMEM((2 * heads, PITCH, LANES), F32),
            pltpu.VMEM(wire, BF16),
            pltpu.VMEM(wire, BF16),
            pltpu.VMEM((3, col_count, row_count, per, half, LANES), BF16),
            pltpu.VMEM(wire, BF16),
            pltpu.VMEM((per, 2, depth, 2 * LANES), BF16),
            pltpu.VMEM((2, per, rows + 8, LANES), F32),
            pltpu.VMEM((2, per, rows + 8, LANES), F32),
            pltpu.VMEM((3, 3, rows, LANES), F32),
            pltpu.VMEM((3, 3, rows // 2, LANES), F32),
            pltpu.VMEM((3, 3, rows // 2, LANES), F32),
            pltpu.VMEM((3, row_count // 2, 3, rows // row_count, LANES), F32),
            pltpu.VMEM((row_count, 3, 8, LANES), F32),
            pltpu.VMEM((3, 3, rows, LANES), F32),
            pltpu.VMEM((col_count, 2 * groups, 48, per, LANES), BF16),
            dma((3, row_count)), dma((3, row_count)), dma((row_count,)), dma((row_count,)),
            dma((3, 2, row_count)), dma((3, 2, row_count)), dma((3, row_count)), dma((3, row_count)),
            dma((4,)), dma((4,)), dma((4, row_count)), dma((4, row_count)), dma((4, row_count)), dma((4, row_count)), dma((4,)), dma((4,)),
            dma((col_count, 2, 3)), dma((row_count, 3)), dma((3, 4)),
        ],
        compiler_params=pltpu.CompilerParams(collective_id=0, has_side_effects=True, vmem_limit_bytes=67000000),
        cost_estimate=pl.CostEstimate(flops=12 * per * depth * 2 * LANES * rows, bytes_accessed=z.size * 8, transcendentals=0),
    )(z.reshape(2, half, cols, chan), mask, g_in.reshape(1, chan), w_a, w_ag, w_b, w_bg, g_out.reshape(1, heads))


def solution(mesh):
    row_count = mesh.shape['row']
    col_count = mesh.shape['col']
    tile_spec = P(('batch', 'row'), 'col', None)
    mask_spec = P(('batch', 'row'), 'col')

    def local_step(z, mask, g_in, w_a, w_ag, w_b, w_bg, w_g, g_out, w_o):
        y, x = exchange(z, mask, g_in, w_a, w_ag, w_b, w_bg, g_out, row_count, col_count)
        return finish(y, x, z, w_g, w_o)

    return jax.shard_map(local_step, mesh=mesh, in_specs=(tile_spec, mask_spec) + (P(),) * 8, out_specs=tile_spec, check_vma=False)
```

```python
import functools

import jax
import jax.numpy as jnp
from jax import lax
from jax.experimental import pallas as pl
from jax.experimental.pallas import tpu as pltpu
from jax.sharding import PartitionSpec as P

LN_EPS = 0.00001
LANES = 128
HALF = 64
GROUP = 16
PITCH = 24
BATCH = 32
QUART = 32
PAIR = 2
UNROLL = 4
F32 = jnp.float32
BF16 = jnp.bfloat16


def dot(lhs, rhs, dims):
    return lax.dot_general(lhs, rhs, (dims, ((), ())), preferred_element_type=F32)


def loop(count, body, **options):
    lax.fori_loop(0, count, body, 0, **options)


def layer_norm(values, gain):
    mean = jnp.mean(values, axis=-1, keepdims=True)
    centered = values - mean
    variance = jnp.mean(centered * centered, axis=-1, keepdims=True)
    return centered * lax.rsqrt(variance + LN_EPS) * gain


def finish_kernel(y_ref, x_ref, z_ref, wg_ref, wo_ref, out_ref):
    srcs, _, _, per, _ = y_ref.shape
    heads = srcs * per

    def gated(x, z, upd):
        gate = jax.nn.sigmoid(dot(x, wg_ref[...], ((1,), (0,))))
        return (z.astype(F32) + gate * upd).astype(BF16)

    def wide(i, carry):
        t = BATCH * i
        at = pl.ds(t, BATCH)
        turned = jnp.concatenate([y_ref[:, 0, t + r].reshape(heads, LANES) for r in range(BATCH)], axis=1)
        upd = dot(turned, wo_ref[...], ((0,), (0,)))
        x = jnp.concatenate([x_ref[s, at] for s in range(2)], axis=1).reshape(BATCH * LANES, LANES)
        parts = [slice(QUART * n, QUART * (n + 1)) for n in (0, 3, 1, 4)]
        z = jnp.concatenate([z_ref[at, part] for part in parts], axis=1).reshape(BATCH * LANES, LANES)
        res = gated(x, z, upd).reshape(BATCH, LANES, LANES)
        for e, part in enumerate(parts):
            out_ref[at, part] = res[:, QUART * e:QUART * (e + 1)]
        return carry

    loop(32 // BATCH, wide)
    turned = jnp.concatenate([y_ref[:, 0, 32 + r].reshape(heads, LANES) for r in range(16)], axis=1)
    upd = dot(turned, wo_ref[...], ((0,), (0,)))
    rows = [r + 16 * h for r in range(16) for h in range(2)]
    x = jnp.concatenate([x_ref[2, p] for p in rows], axis=0)
    z = jnp.concatenate([z_ref[p, QUART * n:QUART * (n + 1)] for p in rows for n in (2, 5)], axis=0)
    res = gated(x, z, upd)
    for e, p in enumerate(rows):
        for n in range(2):
            out_ref[p, QUART * (2 + 3 * n):QUART * (3 + 3 * n)] = res[HALF * e + QUART * n:HALF * e + QUART * (n + 1)]


def finish(y, x, z, w_gate, w_out):
    rows, cols, chan = z.shape
    srcs, groups, places, per, _ = y.shape
    tile_spec = pl.BlockSpec((32, cols, chan), lambda t: (t, 0, 0))
    return pl.pallas_call(
        finish_kernel,
        grid=(groups,),
        in_specs=[
            pl.BlockSpec((srcs, 1, places, per, LANES), lambda t: (0, t, 0, 0, 0)),
            pl.BlockSpec((3, 32, HALF, chan), lambda t: (0, t, 0, 0)),
            tile_spec,
            pl.BlockSpec(w_gate.shape, lambda t: (0, 0)),
            pl.BlockSpec(w_out.shape, lambda t: (0, 0)),
        ],
        out_specs=tile_spec,
        out_shape=jax.ShapeDtypeStruct(z.shape, BF16),
        compiler_params=pltpu.CompilerParams(vmem_limit_bytes=60 * 2**20),
        cost_estimate=pl.CostEstimate(flops=4 * rows * cols * chan * chan, bytes_accessed=rows * cols * chan * 8, transcendentals=0),
    )(y, x.reshape(3, rows, HALF, chan), z, w_gate, w_out)


def remote(src, dst, send_sem, recv_sem, **place):
    return pltpu.make_async_remote_copy(
        src_ref=src, dst_ref=dst, send_sem=send_sem, recv_sem=recv_sem, device_id=place, device_id_type=pl.DeviceIdType.MESH
    )


def exchange_kernel(
    row_count, col_count, z_hbm, m_ref, gi_ref, wa_ref, wag_ref, wb_ref, wbg_ref, go_ref, y_hbm, x_hbm,
    zx, weights, keep, gains, turn, a_out, b_out, all_a, got_b, rhs, o_wide, o_tail, st_part, st_pair, st_chip, st_got, st_far, st_tot, y_out,
    xa_s, xa_r, xb_s, xb_r, dir_s, dir_r, fwd_s, fwd_r, pr_s, pr_r, rs_s, rs_r, ag_s, ag_r, sh_s, sh_r, ys_s, ys_r, loc,
):
    me, col = lax.axis_index('row'), lax.axis_index('col')
    per, _, half, _ = a_out.shape[1:]
    heads = per * row_count
    depth = row_count * half
    chip, core = me // 2, me % 2
    chips = row_count // 2
    steps = [(0, 0), (0, 1)]
    for d in range(1, chips // 2 + 1):
        steps += [(d, 0), (-d, 0), (d, 1), (-d, 1)] if 2 * d < chips else [(d, 0), (d, 1)]
    peers = [lax.rem(chip + d + chips, chips) * 2 + lax.rem(core + f, 2) for d, f in steps]
    up, down = lax.rem(col + 1, col_count), lax.rem(col + col_count - 1, col_count)
    far = lax.rem(col + 2, col_count)
    order = (col, down, up, far)
    alike = [q for q, (d, f) in enumerate(steps) if d and not f]

    loads = [
        [
            pltpu.make_async_copy(z_hbm.at[:, :, pl.ds(QUART * (s + 3 * e), QUART)], zx.at[s, :, :, pl.ds(QUART * e, QUART)], loc.at[s, e])
            for e in range(2)
        ]
        for s in range(3)
    ]
    saves = [pltpu.make_async_copy(zx.at[s], x_hbm.at[s], loc.at[s, 2]) for s in range(3)]
    for pair in loads:
        for copy in pair:
            copy.start()

    def loaded(s):
        for copy in loads[s]:
            copy.wait()

    barrier = pltpu.get_barrier_semaphore()
    for p in peers[1:]:
        pl.semaphore_signal(barrier, inc=1, device_id={'row': p}, device_id_type=pl.DeviceIdType.MESH)
    for p in (up, down):
        pl.semaphore_signal(barrier, inc=1, device_id={'col': p}, device_id_type=pl.DeviceIdType.MESH)

    for n, ref in enumerate((wa_ref, wag_ref, wb_ref, wbg_ref)):
        weights[n * heads:(n + 1) * heads] = ref[...].T
    gains[...] = jnp.broadcast_to(go_ref[...].astype(F32), (heads, heads)).T
    gain_in = gi_ref[...].astype(F32)
    mask = m_ref[...].astype(F32)
    low_mask, high_mask = mask[:half], mask[half:]
    for s in range(3):
        keep[s] = jnp.concatenate([m[:, QUART * n:QUART * (n + 1)] for m in (low_mask, high_mask) for n in (s, s + 3)], axis=1)

    flat_turn = turn.reshape(2 * heads * PITCH, LANES)
    flat_out = [ref.reshape(heads, 3, half, LANES) for ref in (a_out, b_out)]

    def project(s, sides, fresh, between=()):
        if fresh:
            def norm(i, carry):
                at = pl.ds(8 * i, 8)
                v = zx[s, :, at].astype(F32).reshape(8 * LANES, heads)
                zx[s, :, at] = layer_norm(v, gain_in).astype(BF16).reshape(2, 8, HALF, heads)
                return carry

            loop(half // 8, norm)

        for g in range(half // GROUP):
            def row(i, carry):
                t = PAIR * i
                k = g * GROUP + t
                tall = jnp.concatenate([zx[s, e, k + r] for r in range(PAIR) for e in range(2)], axis=0)
                for side in sides:
                    both = dot(weights[2 * side * heads:2 * (side + 1) * heads], tall, ((1,), (1,)))
                    for r in range(PAIR):
                        at = slice(LANES * r, LANES * (r + 1))
                        act = keep[s, pl.ds(k + r, 1)] * jax.nn.sigmoid(both[heads:, at]) * both[:heads, at]
                        flat_turn[pl.ds(side * heads * PITCH + t + r, heads, stride=PITCH), :] = act
                return carry

            loop(GROUP // PAIR, row, unroll=8)

            def pack(h, carry):
                for side in sides:
                    flat_out[side][h, s, g * GROUP:(g + 1) * GROUP] = turn[side * heads + h, 0:GROUP].astype(BF16)
                return carry

            loop(heads, pack, unroll=32)
            if g < len(between):
                between[g]()

    sends = []

    def send(*args, **place):
        copy = remote(*args, **place)
        copy.start()
        sends.append(copy)

    def scatter_a(s, first=1, last=row_count):
        for q in range(first, last):
            send(a_out.at[peers[q], :, s], all_a.at[s, col, me], xa_s.at[s, q], xa_r.at[s, me], row=peers[q])
        if first == 1:
            all_a[s, col, me] = a_out[me, :, s]

    def scatter_b():
        for q in range(1, row_count):
            send(b_out.at[peers[q]], got_b.at[me], xb_s.at[q], xb_r.at[me], row=peers[q])
        got_b[me] = b_out[me]

    def direct(s, first, last):
        for q in range(first, last):
            src = all_a.at[s, col, peers[q]]
            if q:
                remote(src, src, xa_s.at[s, q], xa_r.at[s, peers[q]], row=peers[q]).wait_recv()
            send(src, src, dir_s.at[s, 0, q], dir_r.at[s, 0, peers[q]], col=up)
            send(src, src, dir_s.at[s, 1, q], dir_r.at[s, 1, peers[q]], col=down)

    def forward(s, first, last):
        for q in range(first, last):
            for way, block in ((0, down), (1, up)):
                ref = all_a.at[s, block, peers[q]]
                remote(ref, ref, dir_s.at[s, way, q], dir_r.at[s, way, peers[q]], col=up).wait_recv()
            away, block = (up, down) if q % 2 == 0 else (down, up)
            src = all_a.at[s, block, peers[q]]
            send(src, src, fwd_s.at[s, q], fwd_r.at[s, peers[q]], col=away)

    def arrived(s):
        for q in range(row_count):
            ref = all_a.at[s, far, peers[q]]
            remote(ref, ref, fwd_s.at[s, q], fwd_r.at[s, peers[q]], col=up).wait_recv()

    lane = lax.broadcasted_iota(jnp.int32, (8, LANES), 1)
    pitch = o_wide.shape[2]
    flat_wide = o_wide.reshape(2 * per * pitch, LANES)
    flat_tail = o_tail.reshape(2 * per * pitch, LANES)

    def swap(v):
        return pltpu.roll(v, HALF, v.ndim - 1)

    def spread():
        for q in range(1, row_count):
            ref = got_b.at[peers[q]]
            remote(ref, ref, xb_s.at[q], xb_r.at[peers[q]], row=peers[q]).wait_recv()

        def channel(h, carry):
            w = [got_b[:, h, s].reshape(depth, LANES) for s in range(3)]
            rhs[h, 0, :, :LANES] = jnp.concatenate([w[0][:, :HALF], w[1][:, :HALF]], axis=1)
            rhs[h, 1, :, :LANES] = jnp.concatenate([w[0][:, HALF:], w[1][:, HALF:]], axis=1)
            rhs[h, 0, :, LANES:] = w[2]
            rhs[h, 1, :, LANES:] = jnp.concatenate([w[2][:, HALF:], w[2][:, :HALF]], axis=1)
            return carry

        loop(per, channel, unroll=UNROLL)

    def product(u, s, first, count):
        at = slice(first * HALF, (first + count) * HALF)

        def channel(h, carry):
            turned = [all_a[s, c, :, h].reshape(depth, LANES).T for c in order[first:first + count]]
            res = dot(jnp.concatenate([t[:HALF] for t in turned], axis=0), rhs[h, 0], ((1,), (0,)))
            res += dot(jnp.concatenate([t[HALF:] for t in turned], axis=0), rhs[h, 1], ((1,), (0,)))
            o_wide[s % 2, h, at] = res[:, :LANES]
            o_tail[s % 2, h, at] = res[:, LANES:]
            return carry

        loop(per, channel, unroll=UNROLL)

    def partial(u, s, first, count):
        def tile(t, carry):
            at = pl.ds(pl.multiple_of(first * HALF + 8 * t, 8), 8)
            out = []
            for ref in (o_wide, o_tail):
                v = ref[s % 2, :, at]
                mean = jnp.sum(v, axis=0) * (1.0 / per)
                out += [mean, jnp.sum((v - mean) ** 2, axis=0)]
            st_part[s, 0, at] = out[0]
            st_part[s, 1, at] = out[1]
            st_part[s, 2, at] = jnp.where(lane < HALF, out[2], swap(out[3]))
            return carry

        loop(count * HALF // 8, tile, unroll=UNROLL)
        if count == 1:
            for q in range(1, row_count):
                at = pl.ds(pl.multiple_of(first * HALF + 8 * peers[q], 8), 8)
                send(st_part.at[s, :, at], st_far.at[me], rs_s.at[u, q], rs_r.at[u, me], row=peers[q])
            return
        size = count * HALF // 2
        at = pl.ds(pl.multiple_of(first * HALF + size * (1 - core), 8), size)
        send(st_part.at[s, :, at], st_pair.at[u, :, 0:size], pr_s.at[u], pr_r.at[u], row=peers[1])

    def merge(u, s, first, count):
        size = count * HALF // 2
        own = size // chips
        ref = st_pair.at[u, :, 0:size]
        remote(ref, ref, pr_s.at[u], pr_r.at[u], row=peers[1]).wait_recv()

        def tile(t, carry):
            at = pl.ds(pl.multiple_of(8 * t, 8), 8)
            mine = st_part[s, :, pl.ds(pl.multiple_of(first * HALF + size * core + 8 * t, 8), 8)]
            other = st_pair[u, :, at]
            total = mine + other
            gap = (mine - other) ** 2 * (0.5 * per)
            st_chip[u, 0, at] = 0.5 * total[0]
            st_chip[u, 1, at] = total[1] + gap[0]
            st_chip[u, 2, at] = jnp.where(lane < HALF, 0.5 * total[2], total[2] + swap(gap[2]))
            return carry

        loop(size // 8, tile, unroll=UNROLL)
        for q in alike:
            at = pl.ds(pl.multiple_of(own * (peers[q] // 2), 8), own)
            send(st_chip.at[u, :, at], st_got.at[u, chip, :, 0:own], rs_s.at[u, q], rs_r.at[u, chip], row=peers[q])

    def settle(s, to, weight, means, squares, both):
        parts = means.shape[0]
        mean = jnp.sum(means, axis=0) * (1.0 / parts)
        square = jnp.sum(squares, axis=0) + weight * jnp.sum((means - mean) ** 2, axis=0)
        st_tot[s, 0, to] = mean
        st_tot[s, 1, to] = lax.rsqrt(square * (1.0 / heads) + LN_EPS)
        total = jnp.sum(both, axis=0)
        mean = total * (1.0 / parts)
        square = total + swap(weight * jnp.sum((both - mean) ** 2, axis=0))
        st_tot[s, 2, to] = jnp.where(lane < HALF, mean, lax.rsqrt(square * (1.0 / heads) + LN_EPS))

    def combine(u, s, first, count):
        size = count * HALF // 2
        own = size // chips
        base = pl.multiple_of(first * HALF + size * core + own * chip, 8)
        st_got[u, chip, :, 0:own] = st_chip[u, :, pl.ds(pl.multiple_of(own * chip, 8), own)]
        for q in alike:
            ref = st_got.at[u, peers[q] // 2, :, 0:own]
            remote(ref, ref, rs_s.at[u, q], rs_r.at[u, peers[q] // 2], row=peers[q]).wait_recv()
        for t in range(own // 8):
            at = slice(8 * t, 8 * t + 8)
            settle(s, pl.ds(pl.multiple_of(base + 8 * t, 8), 8), 2 * per, *(st_got[u, :, n, at] for n in range(3)))
        for q in alike:
            ref = st_tot.at[s, :, pl.ds(base, own)]
            send(ref, ref, ag_s.at[u, q], ag_r.at[u, chip], row=peers[q])

    def combine_far(u, s, first, count):
        base = pl.multiple_of(first * HALF + 8 * me, 8)
        at = pl.ds(base, 8)
        st_far[me] = st_part[s, :, at]
        for q in range(1, row_count):
            ref = st_far.at[peers[q]]
            remote(ref, ref, rs_s.at[u, q], rs_r.at[u, peers[q]], row=peers[q]).wait_recv()
        settle(s, at, per, *(st_far[:, n] for n in range(3)))
        for q in range(1, row_count):
            ref = st_tot.at[s, :, at]
            send(ref, ref, ag_s.at[u, q], ag_r.at[u, me], row=peers[q])

    def share(u, s, first, count):
        size = count * HALF // 2
        own = size // chips
        base = first * HALF + size * core
        for q in alike:
            ref = st_tot.at[s, :, pl.ds(pl.multiple_of(base + own * (peers[q] // 2), 8), own)]
            remote(ref, ref, ag_s.at[u, q], ag_r.at[u, peers[q] // 2], row=peers[q]).wait_recv()
        ref = st_tot.at[s, :, pl.ds(pl.multiple_of(base, 8), size)]
        send(ref, ref, sh_s.at[u], sh_r.at[u], row=peers[1])

    gain_out = gains[pl.ds(pl.multiple_of(me * per, 8), per), :]
    low = lax.broadcasted_iota(jnp.int32, (per, LANES), 1) < HALF

    def normalize(u, s, first, count):
        if count == 1:
            for q in range(1, row_count):
                ref = st_tot.at[s, :, pl.ds(pl.multiple_of(first * HALF + 8 * peers[q], 8), 8)]
                remote(ref, ref, ag_s.at[u, q], ag_r.at[u, peers[q]], row=peers[q]).wait_recv()
        else:
            size = count * HALF // 2
            ref = st_tot.at[s, :, pl.ds(pl.multiple_of(first * HALF + size * (1 - core), 8), size)]
            remote(ref, ref, sh_s.at[u], sh_r.at[u], row=peers[1]).wait_recv()
        base = (s % 2) * (per * pitch)

        def wide(t, carry):
            for r in range(8):
                i = 8 * t + r
                v = flat_wide[pl.ds(base + i, per, stride=pitch), :]
                v = (v - st_tot[s, 0, pl.ds(i, 1)]) * st_tot[s, 1, pl.ds(i, 1)] * gain_out
                y_out[t // 8, s + 3 * ((t // 4) % 2), 8 * (t % 4) + r] = v.astype(BF16)
            return carry

        def tail(t, carry):
            for r in range(8):
                i = 32 * (t // 2) + 8 * (t % 2) + r
                lo = flat_tail[pl.ds(base + i, per, stride=pitch), :]
                hi = flat_tail[pl.ds(base + i + 16, per, stride=pitch), :]
                one, two = st_tot[s, 2, pl.ds(i, 1)], st_tot[s, 2, pl.ds(i + 16, 1)]
                v = jnp.where(low, lo, swap(hi))
                mean = jnp.where(low[:1], one, swap(two))
                rstd = jnp.where(low[:1], swap(one), two)
                y_out[t // 4, s + 3 * ((t // 2) % 2), 32 + 8 * (t % 2) + r] = ((v - mean) * rstd * gain_out).astype(BF16)
            return carry

        lax.fori_loop(8 * first, 8 * (first + count), wide, 0, unroll=UNROLL)
        lax.fori_loop(4 * first, 4 * (first + count), tail, 0, unroll=UNROLL)

    def back(u, s, first, count, begin=True, cores=(0, 1)):
        for c in cores:
            for n in range(first, first + count):
                dest = order[n] * 2 + c
                src = y_out.at[n, s + 3 * c]
                dst = y_hbm.at[me, s]

                @pl.when(dest != me)
                def _():
                    copy = remote(src, dst, ys_s.at[n, c, s], ys_r.at[me, s], row=dest)
                    copy.start() if begin else copy.wait_send()

                @pl.when(dest == me)
                def _():
                    copy = pltpu.make_async_copy(src, dst, loc.at[s, 3])
                    copy.start() if begin else copy.wait()

    units = [(0, 0, 0, col_count), (1, 1, 0, col_count), (2, 2, 0, col_count - 1), (3, 2, col_count - 1, 1)]

    def nothing():
        pass

    loaded(0)
    project(0, (0,), True)
    pl.semaphore_wait(barrier, row_count + 1)
    scatter_a(0)
    direct(0, 0, 1)
    loaded(1)
    project(1, (0,), True, (nothing, lambda: direct(0, 1, 2)))
    scatter_a(1)
    project(0, (1,), False, (nothing, nothing, lambda: direct(0, 2, 4)))
    project(1, (1,), False, (nothing, nothing, lambda: direct(0, 4, 6)))
    loaded(2)
    project(2, (0, 1), True, (nothing, nothing, lambda: direct(0, 6, row_count)))
    scatter_b()
    scatter_a(2, 1, row_count)
    for copy in saves:
        copy.start()
    forward(0, 0, row_count)
    direct(1, 0, row_count)
    forward(1, 0, row_count)
    spread()
    arrived(0)
    product(*units[0])
    partial(*units[0])
    merge(*units[0])
    direct(2, 0, row_count)
    combine(*units[0])
    arrived(1)
    product(*units[1])
    partial(*units[1])
    share(*units[0])
    merge(*units[1])
    normalize(*units[0])
    back(*units[0], cores=(0,))
    combine(*units[1])
    back(*units[0], cores=(1,))
    share(*units[1])
    forward(2, 0, 4)
    normalize(*units[1])
    back(*units[1], cores=(0,))
    forward(2, 4, 8)
    product(*units[2])
    partial(*units[2])
    merge(*units[2])
    combine(*units[2])
    back(*units[1], cores=(1,))
    share(*units[2])
    arrived(2)
    product(*units[3])
    partial(*units[3])
    normalize(*units[2])
    combine_far(*units[3])
    back(*units[2])
    normalize(*units[3])
    back(*units[3])

    for copy in saves:
        copy.wait()
    for copy in sends:
        copy.wait_send()
    for unit in units:
        back(*unit, begin=False)
    for q in range(1, row_count):
        for n in range(3):
            ref = y_hbm.at[peers[q], n]
            remote(y_out.at[0, 0], ref, ys_s.at[0, 0, n], ys_r.at[peers[q], n], row=peers[q]).wait_recv()


def exchange(z, mask, g_in, w_a, w_ag, w_b, w_bg, g_out, row_count, col_count):
    tile_rows, cols, chan = z.shape
    heads = w_a.shape[1]
    half = tile_rows // 2
    per = heads // row_count
    depth = row_count * half
    rows = col_count * HALF
    groups = tile_rows // 32
    wire = (row_count, per, 3, half, LANES)
    dma = pltpu.SemaphoreType.DMA
    chunk_sem, ways_sem, unit_sem, peer_sem = dma((3, row_count)), dma((3, 2, row_count)), dma((4,)), dma((4, row_count))
    o_buffer = pltpu.VMEM((2, per, rows + 8, LANES), F32)
    st_buffer, st_halves = pltpu.VMEM((3, 3, rows, LANES), F32), pltpu.VMEM((3, 3, rows // 2, LANES), F32)
    hbm = pl.BlockSpec(memory_space=pl.ANY)
    vmem = pl.BlockSpec(memory_space=pltpu.VMEM)
    return pl.pallas_call(
        functools.partial(exchange_kernel, row_count, col_count),
        in_specs=[hbm] + [vmem] * 7,
        out_specs=[hbm, hbm],
        out_shape=[
            jax.ShapeDtypeStruct((row_count, groups, 48, per, LANES), BF16),
            jax.ShapeDtypeStruct((3, 2, half, HALF, chan), BF16),
        ],
        scratch_shapes=[
            pltpu.VMEM((3, 2, half, HALF, chan), BF16),
            pltpu.VMEM((4 * heads, chan), BF16),
            pltpu.VMEM((3, half, LANES), F32),
            pltpu.VMEM((heads, LANES), F32),
            pltpu.VMEM((2 * heads, PITCH, LANES), F32),
            pltpu.VMEM(wire, BF16),
            pltpu.VMEM(wire, BF16),
            pltpu.VMEM((3, col_count, row_count, per, half, LANES), BF16),
            pltpu.VMEM(wire, BF16),
            pltpu.VMEM((per, 2, depth, 2 * LANES), BF16),
            o_buffer,
            o_buffer,
            st_buffer,
            st_halves,
            st_halves,
            pltpu.VMEM((3, row_count // 2, 3, rows // row_count, LANES), F32),
            pltpu.VMEM((row_count, 3, 8, LANES), F32),
            st_buffer,
            pltpu.VMEM((col_count, 2 * groups, 48, per, LANES), BF16),
            chunk_sem, chunk_sem, dma((row_count,)), dma((row_count,)),
            ways_sem, ways_sem, chunk_sem, chunk_sem,
            unit_sem, unit_sem, peer_sem, peer_sem, peer_sem, peer_sem, unit_sem, unit_sem,
            dma((col_count, 2, 3)), dma((row_count, 3)), dma((3, 4)),
        ],
        compiler_params=pltpu.CompilerParams(collective_id=0, has_side_effects=True, vmem_limit_bytes=67000000),
        cost_estimate=pl.CostEstimate(flops=12 * per * depth * 2 * LANES * rows, bytes_accessed=z.size * 8, transcendentals=0),
    )(z.reshape(2, half, cols, chan), mask, g_in.reshape(1, chan), w_a, w_ag, w_b, w_bg, g_out.reshape(1, heads))


def solution(mesh):
    row_count = mesh.shape['row']
    col_count = mesh.shape['col']
    tile_spec = P(('batch', 'row'), 'col', None)
    mask_spec = P(('batch', 'row'), 'col')

    def local_step(z, mask, g_in, w_a, w_ag, w_b, w_bg, w_g, g_out, w_o):
        y, x = exchange(z, mask, g_in, w_a, w_ag, w_b, w_bg, g_out, row_count, col_count)
        return finish(y, x, z, w_g, w_o)

    return jax.shard_map(local_step, mesh=mesh, in_specs=(tile_spec, mask_spec) + (P(),) * 8, out_specs=tile_spec, check_vma=False)
```

```python
import functools

import jax
import jax.numpy as jnp
from jax import lax
from jax.experimental import pallas as pl
from jax.experimental.pallas import tpu as pltpu
from jax.sharding import PartitionSpec as P

LN_EPS = 0.00001
LANES = 128
HALF = 64
GROUP = 16
PITCH = 24
BATCH = 32
QUART = 32
PAIR = 2
UNROLL = 4
F32 = jnp.float32
BF16 = jnp.bfloat16


def dot(lhs, rhs, dims):
    return lax.dot_general(lhs, rhs, (dims, ((), ())), preferred_element_type=F32)


def loop(count, body, **options):
    lax.fori_loop(0, count, body, 0, **options)


def layer_norm(values, gain):
    mean = jnp.mean(values, axis=-1, keepdims=True)
    centered = values - mean
    variance = jnp.mean(centered * centered, axis=-1, keepdims=True)
    return centered * lax.rsqrt(variance + LN_EPS) * gain


def finish_kernel(y_ref, x_ref, z_ref, wg_ref, wo_ref, out_ref):
    srcs, _, _, per, _ = y_ref.shape
    heads = srcs * per

    def gated(x, z, upd):
        gate = jax.nn.sigmoid(dot(x, wg_ref[...], ((1,), (0,))))
        return (z.astype(F32) + gate * upd).astype(BF16)

    def wide(i, carry):
        t = BATCH * i
        at = pl.ds(t, BATCH)
        turned = jnp.concatenate([y_ref[:, 0, t + r].reshape(heads, LANES) for r in range(BATCH)], axis=1)
        upd = dot(turned, wo_ref[...], ((0,), (0,)))
        x = jnp.concatenate([x_ref[s, at] for s in range(2)], axis=1).reshape(BATCH * LANES, LANES)
        parts = [slice(QUART * n, QUART * (n + 1)) for n in (0, 3, 1, 4)]
        z = jnp.concatenate([z_ref[at, part] for part in parts], axis=1).reshape(BATCH * LANES, LANES)
        res = gated(x, z, upd).reshape(BATCH, LANES, LANES)
        for e, part in enumerate(parts):
            out_ref[at, part] = res[:, QUART * e:QUART * (e + 1)]
        return carry

    loop(32 // BATCH, wide)
    turned = jnp.concatenate([y_ref[:, 0, 32 + r].reshape(heads, LANES) for r in range(16)], axis=1)
    upd = dot(turned, wo_ref[...], ((0,), (0,)))
    rows = [r + 16 * h for r in range(16) for h in range(2)]
    x = jnp.concatenate([x_ref[2, p] for p in rows], axis=0)
    z = jnp.concatenate([z_ref[p, QUART * n:QUART * (n + 1)] for p in rows for n in (2, 5)], axis=0)
    res = gated(x, z, upd)
    for e, p in enumerate(rows):
        for n in range(2):
            out_ref[p, QUART * (2 + 3 * n):QUART * (3 + 3 * n)] = res[HALF * e + QUART * n:HALF * e + QUART * (n + 1)]


def finish(y, x, z, w_gate, w_out):
    rows, cols, chan = z.shape
    srcs, groups, places, per, _ = y.shape
    tile_spec = pl.BlockSpec((32, cols, chan), lambda t: (t, 0, 0))
    return pl.pallas_call(
        finish_kernel,
        grid=(groups,),
        in_specs=[
            pl.BlockSpec((srcs, 1, places, per, LANES), lambda t: (0, t, 0, 0, 0)),
            pl.BlockSpec((3, 32, HALF, chan), lambda t: (0, t, 0, 0)),
            tile_spec,
            pl.BlockSpec(w_gate.shape, lambda t: (0, 0)),
            pl.BlockSpec(w_out.shape, lambda t: (0, 0)),
        ],
        out_specs=tile_spec,
        out_shape=jax.ShapeDtypeStruct(z.shape, BF16),
        compiler_params=pltpu.CompilerParams(vmem_limit_bytes=60 * 2**20),
        cost_estimate=pl.CostEstimate(flops=4 * rows * cols * chan * chan, bytes_accessed=rows * cols * chan * 8, transcendentals=0),
    )(y, x.reshape(3, rows, HALF, chan), z, w_gate, w_out)


def remote(src, dst, send_sem, recv_sem, **place):
    return pltpu.make_async_remote_copy(
        src_ref=src, dst_ref=dst, send_sem=send_sem, recv_sem=recv_sem, device_id=place, device_id_type=pl.DeviceIdType.MESH
    )


def exchange_kernel(
    row_count, col_count, z_hbm, m_ref, gi_ref, wa_ref, wag_ref, wb_ref, wbg_ref, go_ref, y_hbm, x_hbm,
    zx, weights, keep, gains, turn, a_out, b_out, all_a, got_b, rhs, o_wide, o_tail, st_part, st_pair, st_chip, st_got, st_far, st_tot, y_out,
    xa_s, xa_r, xb_s, xb_r, dir_s, dir_r, fwd_s, fwd_r, pr_s, pr_r, rs_s, rs_r, ag_s, ag_r, sh_s, sh_r, ys_s, ys_r, loc,
):
    me, col = lax.axis_index('row'), lax.axis_index('col')
    per, _, half, _ = a_out.shape[1:]
    heads = per * row_count
    depth = row_count * half
    chip, core = me // 2, me % 2
    chips = row_count // 2
    steps = [(0, 0), (0, 1)]
    for d in range(1, chips // 2 + 1):
        steps += [(d, 0), (-d, 0), (d, 1), (-d, 1)] if 2 * d < chips else [(d, 0), (d, 1)]
    peers = [lax.rem(chip + d + chips, chips) * 2 + lax.rem(core + f, 2) for d, f in steps]
    up, down = lax.rem(col + 1, col_count), lax.rem(col + col_count - 1, col_count)
    far = lax.rem(col + 2, col_count)
    order = (col, up, down, far)
    alike = [q for q, (d, f) in enumerate(steps) if d and not f][::-1]

    loads = [
        [
            pltpu.make_async_copy(z_hbm.at[:, :, pl.ds(QUART * (s + 3 * e), QUART)], zx.at[s, :, :, pl.ds(QUART * e, QUART)], loc.at[s, e])
            for e in range(2)
        ]
        for s in range(3)
    ]
    saves = [pltpu.make_async_copy(zx.at[s], x_hbm.at[s], loc.at[s, 2]) for s in range(3)]
    for pair in loads:
        for copy in pair:
            copy.start()

    def loaded(s):
        for copy in loads[s]:
            copy.wait()

    barrier = pltpu.get_barrier_semaphore()
    for p in peers[1:]:
        pl.semaphore_signal(barrier, inc=1, device_id={'row': p}, device_id_type=pl.DeviceIdType.MESH)
    for p in (up, down):
        pl.semaphore_signal(barrier, inc=1, device_id={'col': p}, device_id_type=pl.DeviceIdType.MESH)

    for n, ref in enumerate((wa_ref, wag_ref, wb_ref, wbg_ref)):
        weights[n * heads:(n + 1) * heads] = ref[...].T
    gains[...] = jnp.broadcast_to(go_ref[...].astype(F32), (heads, heads)).T
    gain_in = gi_ref[...].astype(F32)
    mask = m_ref[...].astype(F32)
    low_mask, high_mask = mask[:half], mask[half:]
    for s in range(3):
        keep[s] = jnp.concatenate([m[:, QUART * n:QUART * (n + 1)] for m in (low_mask, high_mask) for n in (s, s + 3)], axis=1)

    flat_turn = turn.reshape(2 * heads * PITCH, LANES)
    flat_out = [ref.reshape(heads, 3, half, LANES) for ref in (a_out, b_out)]

    def project(s, sides, fresh, between=()):
        if fresh:
            def norm(i, carry):
                at = pl.ds(8 * i, 8)
                v = zx[s, :, at].astype(F32).reshape(8 * LANES, heads)
                zx[s, :, at] = layer_norm(v, gain_in).astype(BF16).reshape(2, 8, HALF, heads)
                return carry

            loop(half // 8, norm)

        for g in range(half // GROUP):
            def row(i, carry):
                t = PAIR * i
                k = g * GROUP + t
                tall = jnp.concatenate([zx[s, e, k + r] for r in range(PAIR) for e in range(2)], axis=0)
                for side in sides:
                    both = dot(weights[2 * side * heads:2 * (side + 1) * heads], tall, ((1,), (1,)))
                    for r in range(PAIR):
                        at = slice(LANES * r, LANES * (r + 1))
                        act = keep[s, pl.ds(k + r, 1)] * jax.nn.sigmoid(both[heads:, at]) * both[:heads, at]
                        flat_turn[pl.ds(side * heads * PITCH + t + r, heads, stride=PITCH), :] = act
                return carry

            loop(GROUP // PAIR, row, unroll=8)

            def pack(h, carry):
                for side in sides:
                    flat_out[side][h, s, g * GROUP:(g + 1) * GROUP] = turn[side * heads + h, 0:GROUP].astype(BF16)
                return carry

            loop(heads, pack, unroll=32)
            if g < len(between):
                between[g]()

    sends = []

    def send(*args, **place):
        copy = remote(*args, **place)
        copy.start()
        sends.append(copy)

    def scatter_a(s, first=1, last=row_count):
        for q in range(first, last):
            send(a_out.at[peers[q], :, s], all_a.at[s, col, me], xa_s.at[s, q], xa_r.at[s, me], row=peers[q])
        if first == 1:
            all_a[s, col, me] = a_out[me, :, s]

    def scatter_b():
        for q in range(1, row_count):
            send(b_out.at[peers[q]], got_b.at[me], xb_s.at[q], xb_r.at[me], row=peers[q])
        got_b[me] = b_out[me]

    def direct(s, first, last):
        for q in range(first, last):
            src = all_a.at[s, col, peers[q]]
            if q:
                remote(src, src, xa_s.at[s, q], xa_r.at[s, peers[q]], row=peers[q]).wait_recv()
            send(src, src, dir_s.at[s, 0, q], dir_r.at[s, 0, peers[q]], col=up)
            send(src, src, dir_s.at[s, 1, q], dir_r.at[s, 1, peers[q]], col=down)

    def forward(s, first, last):
        for q in range(first, last):
            for way, block in ((0, down), (1, up)):
                ref = all_a.at[s, block, peers[q]]
                remote(ref, ref, dir_s.at[s, way, q], dir_r.at[s, way, peers[q]], col=up).wait_recv()
            away, block = (up, down) if q % 2 == 0 else (down, up)
            src = all_a.at[s, block, peers[q]]
            send(src, src, fwd_s.at[s, q], fwd_r.at[s, peers[q]], col=away)

    def arrived(s):
        for q in range(row_count):
            ref = all_a.at[s, far, peers[q]]
            remote(ref, ref, fwd_s.at[s, q], fwd_r.at[s, peers[q]], col=up).wait_recv()

    lane = lax.broadcasted_iota(jnp.int32, (8, LANES), 1)
    pitch = o_wide.shape[2]
    flat_wide = o_wide.reshape(2 * per * pitch, LANES)
    flat_tail = o_tail.reshape(2 * per * pitch, LANES)

    def swap(v):
        return pltpu.roll(v, HALF, v.ndim - 1)

    def spread():
        for q in range(1, row_count):
            ref = got_b.at[peers[q]]
            remote(ref, ref, xb_s.at[q], xb_r.at[peers[q]], row=peers[q]).wait_recv()

        def channel(h, carry):
            w = [got_b[:, h, s].reshape(depth, LANES) for s in range(3)]
            rhs[h, 0, :, :LANES] = jnp.concatenate([w[0][:, :HALF], w[1][:, :HALF]], axis=1)
            rhs[h, 1, :, :LANES] = jnp.concatenate([w[0][:, HALF:], w[1][:, HALF:]], axis=1)
            rhs[h, 0, :, LANES:] = w[2]
            rhs[h, 1, :, LANES:] = jnp.concatenate([w[2][:, HALF:], w[2][:, :HALF]], axis=1)
            return carry

        loop(per, channel, unroll=UNROLL)

    def product(u, s, first, count):
        at = slice(first * HALF, (first + count) * HALF)

        def channel(h, carry):
            turned = [all_a[s, c, :, h].reshape(depth, LANES).T for c in order[first:first + count]]
            res = dot(jnp.concatenate([t[:HALF] for t in turned], axis=0), rhs[h, 0], ((1,), (0,)))
            res += dot(jnp.concatenate([t[HALF:] for t in turned], axis=0), rhs[h, 1], ((1,), (0,)))
            o_wide[s % 2, h, at] = res[:, :LANES]
            o_tail[s % 2, h, at] = res[:, LANES:]
            return carry

        loop(per, channel, unroll=UNROLL)

    def partial(u, s, first, count):
        def tile(t, carry):
            at = pl.ds(pl.multiple_of(first * HALF + 8 * t, 8), 8)
            out = []
            for ref in (o_wide, o_tail):
                v = ref[s % 2, :, at]
                mean = jnp.sum(v, axis=0) * (1.0 / per)
                out += [mean, jnp.sum((v - mean) ** 2, axis=0)]
            st_part[s, 0, at] = out[0]
            st_part[s, 1, at] = out[1]
            st_part[s, 2, at] = jnp.where(lane < HALF, out[2], swap(out[3]))
            return carry

        loop(count * HALF // 8, tile, unroll=UNROLL)
        if count == 1:
            for q in reversed(range(1, row_count)):
                at = pl.ds(pl.multiple_of(first * HALF + 8 * peers[q], 8), 8)
                send(st_part.at[s, :, at], st_far.at[me], rs_s.at[u, q], rs_r.at[u, me], row=peers[q])
            return
        size = count * HALF // 2
        at = pl.ds(pl.multiple_of(first * HALF + size * (1 - core), 8), size)
        send(st_part.at[s, :, at], st_pair.at[u, :, 0:size], pr_s.at[u], pr_r.at[u], row=peers[1])

    def merge(u, s, first, count):
        size = count * HALF // 2
        own = size // chips
        ref = st_pair.at[u, :, 0:size]
        remote(ref, ref, pr_s.at[u], pr_r.at[u], row=peers[1]).wait_recv()

        def tile(t, carry):
            at = pl.ds(pl.multiple_of(8 * t, 8), 8)
            mine = st_part[s, :, pl.ds(pl.multiple_of(first * HALF + size * core + 8 * t, 8), 8)]
            other = st_pair[u, :, at]
            total = mine + other
            gap = (mine - other) ** 2 * (0.5 * per)
            st_chip[u, 0, at] = 0.5 * total[0]
            st_chip[u, 1, at] = total[1] + gap[0]
            st_chip[u, 2, at] = jnp.where(lane < HALF, 0.5 * total[2], total[2] + swap(gap[2]))
            return carry

        loop(size // 8, tile, unroll=UNROLL)
        for q in alike:
            at = pl.ds(pl.multiple_of(own * (peers[q] // 2), 8), own)
            send(st_chip.at[u, :, at], st_got.at[u, chip, :, 0:own], rs_s.at[u, q], rs_r.at[u, chip], row=peers[q])

    def settle(s, to, weight, means, squares, both):
        parts = means.shape[0]
        mean = jnp.sum(means, axis=0) * (1.0 / parts)
        square = jnp.sum(squares, axis=0) + weight * jnp.sum((means - mean) ** 2, axis=0)
        st_tot[s, 0, to] = mean
        st_tot[s, 1, to] = lax.rsqrt(square * (1.0 / heads) + LN_EPS)
        total = jnp.sum(both, axis=0)
        mean = total * (1.0 / parts)
        square = total + swap(weight * jnp.sum((both - mean) ** 2, axis=0))
        st_tot[s, 2, to] = jnp.where(lane < HALF, mean, lax.rsqrt(square * (1.0 / heads) + LN_EPS))

    def combine(u, s, first, count):
        size = count * HALF // 2
        own = size // chips
        base = pl.multiple_of(first * HALF + size * core + own * chip, 8)
        st_got[u, chip, :, 0:own] = st_chip[u, :, pl.ds(pl.multiple_of(own * chip, 8), own)]
        for q in alike:
            ref = st_got.at[u, peers[q] // 2, :, 0:own]
            remote(ref, ref, rs_s.at[u, q], rs_r.at[u, peers[q] // 2], row=peers[q]).wait_recv()
        for t in range(own // 8):
            at = slice(8 * t, 8 * t + 8)
            settle(s, pl.ds(pl.multiple_of(base + 8 * t, 8), 8), 2 * per, *(st_got[u, :, n, at] for n in range(3)))
        for q in alike:
            ref = st_tot.at[s, :, pl.ds(base, own)]
            send(ref, ref, ag_s.at[u, q], ag_r.at[u, chip], row=peers[q])

    def combine_far(u, s, first, count):
        base = pl.multiple_of(first * HALF + 8 * me, 8)
        at = pl.ds(base, 8)
        st_far[me] = st_part[s, :, at]
        for q in range(1, row_count):
            ref = st_far.at[peers[q]]
            remote(ref, ref, rs_s.at[u, q], rs_r.at[u, peers[q]], row=peers[q]).wait_recv()
        settle(s, at, per, *(st_far[:, n] for n in range(3)))
        for q in reversed(range(1, row_count)):
            ref = st_tot.at[s, :, at]
            send(ref, ref, ag_s.at[u, q], ag_r.at[u, me], row=peers[q])

    def share(u, s, first, count):
        size = count * HALF // 2
        own = size // chips
        base = first * HALF + size * core
        for q in alike:
            ref = st_tot.at[s, :, pl.ds(pl.multiple_of(base + own * (peers[q] // 2), 8), own)]
            remote(ref, ref, ag_s.at[u, q], ag_r.at[u, peers[q] // 2], row=peers[q]).wait_recv()
        ref = st_tot.at[s, :, pl.ds(pl.multiple_of(base, 8), size)]
        send(ref, ref, sh_s.at[u], sh_r.at[u], row=peers[1])

    gain_out = gains[pl.ds(pl.multiple_of(me * per, 8), per), :]
    low = lax.broadcasted_iota(jnp.int32, (per, LANES), 1) < HALF

    def normalize(u, s, first, count):
        if count == 1:
            for q in range(1, row_count):
                ref = st_tot.at[s, :, pl.ds(pl.multiple_of(first * HALF + 8 * peers[q], 8), 8)]
                remote(ref, ref, ag_s.at[u, q], ag_r.at[u, peers[q]], row=peers[q]).wait_recv()
        else:
            size = count * HALF // 2
            ref = st_tot.at[s, :, pl.ds(pl.multiple_of(first * HALF + size * (1 - core), 8), size)]
            remote(ref, ref, sh_s.at[u], sh_r.at[u], row=peers[1]).wait_recv()
        base = (s % 2) * (per * pitch)

        def wide(t, carry):
            for r in range(8):
                i = 8 * t + r
                v = flat_wide[pl.ds(base + i, per, stride=pitch), :]
                v = (v - st_tot[s, 0, pl.ds(i, 1)]) * st_tot[s, 1, pl.ds(i, 1)] * gain_out
                y_out[t // 8, s + 3 * ((t // 4) % 2), 8 * (t % 4) + r] = v.astype(BF16)
            return carry

        def tail(t, carry):
            for r in range(8):
                i = 32 * (t // 2) + 8 * (t % 2) + r
                lo = flat_tail[pl.ds(base + i, per, stride=pitch), :]
                hi = flat_tail[pl.ds(base + i + 16, per, stride=pitch), :]
                one, two = st_tot[s, 2, pl.ds(i, 1)], st_tot[s, 2, pl.ds(i + 16, 1)]
                v = jnp.where(low, lo, swap(hi))
                mean = jnp.where(low[:1], one, swap(two))
                rstd = jnp.where(low[:1], swap(one), two)
                y_out[t // 4, s + 3 * ((t // 2) % 2), 32 + 8 * (t % 2) + r] = ((v - mean) * rstd * gain_out).astype(BF16)
            return carry

        lax.fori_loop(8 * first, 8 * (first + count), wide, 0, unroll=UNROLL)
        lax.fori_loop(4 * first, 4 * (first + count), tail, 0, unroll=UNROLL)

    def back(u, s, first, count, begin=True, cores=(0, 1)):
        if count == col_count:
            gaps = [lax.rem(chip + d + col_count - col, col_count) for d in (1, 3, 2, 0)]
            places = [(d + d // 2 - 2 * (d // 3), lax.rem(col + d, col_count)) for d in gaps]
        else:
            places = [(n, order[n]) for n in range(first, first + count)]
        for c in cores:
            for n, block in places:
                dest = block * 2 + c
                src = y_out.at[n, s + 3 * c]
                dst = y_hbm.at[me, s]

                @pl.when(dest != me)
                def _():
                    copy = remote(src, dst, ys_s.at[n, c, s], ys_r.at[me, s], row=dest)
                    copy.start() if begin else copy.wait_send()

                @pl.when(dest == me)
                def _():
                    copy = pltpu.make_async_copy(src, dst, loc.at[s, 3])
                    copy.start() if begin else copy.wait()

    units = [(0, 0, 0, col_count), (1, 1, 0, col_count), (2, 2, 0, col_count - 1), (3, 2, col_count - 1, 1)]

    def nothing():
        pass

    loaded(0)
    project(0, (0,), True)
    pl.semaphore_wait(barrier, row_count + 1)
    scatter_a(0)
    direct(0, 0, 1)
    loaded(1)
    project(1, (0,), True, (nothing, lambda: direct(0, 1, 2)))
    scatter_a(1)
    project(0, (1,), False, (nothing, nothing, lambda: direct(0, 2, 4)))
    project(1, (1,), False, (nothing, nothing, lambda: direct(0, 4, 6)))
    loaded(2)
    project(2, (0, 1), True, (nothing, nothing, lambda: direct(0, 6, row_count)))
    scatter_b()
    scatter_a(2, 1, row_count)
    for copy in saves:
        copy.start()
    forward(0, 0, row_count)
    direct(1, 0, row_count)
    forward(1, 0, row_count)
    spread()
    arrived(0)
    product(*units[0])
    partial(*units[0])
    merge(*units[0])
    direct(2, 0, row_count)
    combine(*units[0])
    arrived(1)
    product(*units[1])
    partial(*units[1])
    share(*units[0])
    merge(*units[1])
    normalize(*units[0])
    back(*units[0], cores=(0,))
    combine(*units[1])
    back(*units[0], cores=(1,))
    share(*units[1])
    forward(2, 0, 4)
    normalize(*units[1])
    back(*units[1], cores=(0,))
    forward(2, 4, 8)
    product(*units[2])
    partial(*units[2])
    merge(*units[2])
    combine(*units[2])
    back(*units[1], cores=(1,))
    share(*units[2])
    arrived(2)
    product(*units[3])
    partial(*units[3])
    normalize(*units[2])
    combine_far(*units[3])
    back(*units[2])
    normalize(*units[3])
    back(*units[3])

    for copy in saves:
        copy.wait()
    for copy in sends:
        copy.wait_send()
    for unit in units:
        back(*unit, begin=False)
    for q in range(1, row_count):
        for n in range(3):
            ref = y_hbm.at[peers[q], n]
            remote(y_out.at[0, 0], ref, ys_s.at[0, 0, n], ys_r.at[peers[q], n], row=peers[q]).wait_recv()


def exchange(z, mask, g_in, w_a, w_ag, w_b, w_bg, g_out, row_count, col_count):
    tile_rows, cols, chan = z.shape
    heads = w_a.shape[1]
    half = tile_rows // 2
    per = heads // row_count
    depth = row_count * half
    rows = col_count * HALF
    groups = tile_rows // 32
    wire = (row_count, per, 3, half, LANES)
    dma = pltpu.SemaphoreType.DMA
    chunk_sem, ways_sem, unit_sem, peer_sem = dma((3, row_count)), dma((3, 2, row_count)), dma((4,)), dma((4, row_count))
    o_buffer = pltpu.VMEM((2, per, rows + 8, LANES), F32)
    st_buffer, st_halves = pltpu.VMEM((3, 3, rows, LANES), F32), pltpu.VMEM((3, 3, rows // 2, LANES), F32)
    hbm = pl.BlockSpec(memory_space=pl.ANY)
    vmem = pl.BlockSpec(memory_space=pltpu.VMEM)
    return pl.pallas_call(
        functools.partial(exchange_kernel, row_count, col_count),
        in_specs=[hbm] + [vmem] * 7,
        out_specs=[hbm, hbm],
        out_shape=[
            jax.ShapeDtypeStruct((row_count, groups, 48, per, LANES), BF16),
            jax.ShapeDtypeStruct((3, 2, half, HALF, chan), BF16),
        ],
        scratch_shapes=[
            pltpu.VMEM((3, 2, half, HALF, chan), BF16),
            pltpu.VMEM((4 * heads, chan), BF16),
            pltpu.VMEM((3, half, LANES), F32),
            pltpu.VMEM((heads, LANES), F32),
            pltpu.VMEM((2 * heads, PITCH, LANES), F32),
            pltpu.VMEM(wire, BF16),
            pltpu.VMEM(wire, BF16),
            pltpu.VMEM((3, col_count, row_count, per, half, LANES), BF16),
            pltpu.VMEM(wire, BF16),
            pltpu.VMEM((per, 2, depth, 2 * LANES), BF16),
            o_buffer,
            o_buffer,
            st_buffer,
            st_halves,
            st_halves,
            pltpu.VMEM((3, row_count // 2, 3, rows // row_count, LANES), F32),
            pltpu.VMEM((row_count, 3, 8, LANES), F32),
            st_buffer,
            pltpu.VMEM((col_count, 2 * groups, 48, per, LANES), BF16),
            chunk_sem, chunk_sem, dma((row_count,)), dma((row_count,)),
            ways_sem, ways_sem, chunk_sem, chunk_sem,
            unit_sem, unit_sem, peer_sem, peer_sem, peer_sem, peer_sem, unit_sem, unit_sem,
            dma((col_count, 2, 3)), dma((row_count, 3)), dma((3, 4)),
        ],
        compiler_params=pltpu.CompilerParams(collective_id=0, has_side_effects=True, vmem_limit_bytes=67000000),
        cost_estimate=pl.CostEstimate(flops=12 * per * depth * 2 * LANES * rows, bytes_accessed=z.size * 8, transcendentals=0),
    )(z.reshape(2, half, cols, chan), mask, g_in.reshape(1, chan), w_a, w_ag, w_b, w_bg, g_out.reshape(1, heads))


def solution(mesh):
    row_count = mesh.shape['row']
    col_count = mesh.shape['col']
    tile_spec = P(('batch', 'row'), 'col', None)
    mask_spec = P(('batch', 'row'), 'col')

    def local_step(z, mask, g_in, w_a, w_ag, w_b, w_bg, w_g, g_out, w_o):
        y, x = exchange(z, mask, g_in, w_a, w_ag, w_b, w_bg, g_out, row_count, col_count)
        return finish(y, x, z, w_g, w_o)

    return jax.shard_map(local_step, mesh=mesh, in_specs=(tile_spec, mask_spec) + (P(),) * 8, out_specs=tile_spec, check_vma=False)
```
